128 devices in a mesh: img: 1, cfg: 2 (over core), patch: 64 (over z, y, x).
Axes of the slice: x: 4, y: 4, z: 4, core: 2. Of those that a mesh axis runs over, the one named last changes fastest.
Arguments:
- latent: bfloat16 [1, 2048, 3072], P('img', 'patch')
- cond_vec: float32 [2, 2, 3072], P(('img', 'cfg'))
- sched_coef: float32 [3, 2], replicated
- w_ada: bfloat16 [2, 3072, 18432], replicated
- w_qkv: bfloat16 [2, 3072, 9216], replicated
- w_out: bfloat16 [2, 24, 128, 3072], replicated
- w_up: bfloat16 [2, 3072, 12288], replicated
- w_down: bfloat16 [2, 12288, 3072], replicated
- w_head: bfloat16 [3072, 3072], replicated
- k_stale: bfloat16 [2, 2, 2048, 3072], P(('img', 'cfg'))
- v_stale: bfloat16 [2, 2, 2048, 3072], P(('img', 'cfg'))
Outputs:
- output 1: float32 [2, 2048, 3072], P(('img', 'cfg'), 'patch')
- output 2: bfloat16 [2, 2, 2048, 3072], P(('img', 'cfg'))
- output 3: bfloat16 [2, 2, 2048, 3072], P(('img', 'cfg'))
All inputs are finite; a program needn't handle non-finite values.
Results may differ from the reference program's by a relative error of at most 0.0132624.
Values are sent between devices in bfloat16 or wider.
A program may use at most 1.5 GiB of HBM per device.

```python
import math
import jax
import jax.numpy as jnp
from jax import lax

D = 3072
HEADS = 24
ROWS = 32
LAYERS = 2
N_PATCH = 64
N_PAIRS = 1
N_STEPS = 2

TOKENS = ROWS * N_PATCH
N_SLOTS = 2 * N_PAIRS
HEAD_DIM = D // HEADS
QK_GAIN = (math.sqrt(math.log(TOKENS / 8.0)) / 1.3) ** 0.5
KEY_STD = QK_GAIN * 1.15


def setup_inputs(seed: int = 0, part: int = 0) -> dict:
    root_key = jax.random.key(seed)
    shared_keys = jax.random.split(root_key, 7)
    local_keys = jax.random.split(jax.random.fold_in(root_key, part), 4)
    inv_width = D ** -0.5
    ada_cols = jnp.repeat(jnp.array([0.7, 0.7, 1.7, 0.7, 0.7, 1.7], jnp.float32), D)
    qkv_cols = jnp.repeat(jnp.array([QK_GAIN, QK_GAIN, 1.0], jnp.float32), D)
    w_ada = jax.random.normal(shared_keys[0], (LAYERS, D, 6 * D), jnp.float32) * (ada_cols * inv_width)
    w_qkv = jax.random.normal(shared_keys[1], (LAYERS, D, 3 * D), jnp.float32) * (qkv_cols * inv_width)
    w_out = jax.random.normal(shared_keys[2], (LAYERS, HEADS, HEAD_DIM, D), jnp.float32) * inv_width
    w_up = jax.random.normal(shared_keys[3], (LAYERS, D, 4 * D), jnp.float32) * inv_width
    w_down = jax.random.normal(shared_keys[4], (LAYERS, 4 * D, D), jnp.float32) * (4 * D) ** -0.5
    w_head = jax.random.normal(shared_keys[5], (D, D), jnp.float32) * inv_width
    low_end = jnp.array([0.75, 0.2, 1.5], jnp.float32)[:, None]
    high_end = jnp.array([0.95, 0.4, 3.5], jnp.float32)[:, None]
    sched_coef = low_end + (high_end - low_end) * jax.random.uniform(shared_keys[6], (3, N_STEPS), jnp.float32)
    latent = jax.random.normal(local_keys[0], (N_PAIRS, TOKENS, D), jnp.float32)
    cond_vec = jax.random.normal(local_keys[1], (N_SLOTS, N_STEPS, D), jnp.float32)
    k_stale = jax.random.normal(local_keys[2], (N_SLOTS, LAYERS, TOKENS, D), jnp.float32) * KEY_STD
    v_stale = jax.random.normal(local_keys[3], (N_SLOTS, LAYERS, TOKENS, D), jnp.float32)
    return {
        "latent": latent.astype(jnp.bfloat16),
        "cond_vec": cond_vec,
        "sched_coef": sched_coef,
        "w_ada": w_ada.astype(jnp.bfloat16),
        "w_qkv": w_qkv.astype(jnp.bfloat16),
        "w_out": w_out.astype(jnp.bfloat16),
        "w_up": w_up.astype(jnp.bfloat16),
        "w_down": w_down.astype(jnp.bfloat16),
        "w_head": w_head.astype(jnp.bfloat16),
        "k_stale": k_stale.astype(jnp.bfloat16),
        "v_stale": v_stale.astype(jnp.bfloat16),
    }


def layer_norm(values):
    row_mean = jnp.mean(values, -1, keepdims=True)
    centered = values - row_mean
    row_var = jnp.mean(centered * centered, -1, keepdims=True)
    return centered * lax.rsqrt(row_var + 1e-6)


def attend(queries, key_set, value_set):
    q_blk = min(ROWS, 128)
    blocks = queries.reshape(ROWS // q_blk, q_blk, HEADS, HEAD_DIM).astype(jnp.float32)
    key_h = key_set.reshape(TOKENS, HEADS, HEAD_DIM).astype(jnp.float32)
    val_h = value_set.reshape(TOKENS, HEADS, HEAD_DIM).astype(jnp.float32)
    score_scale = HEAD_DIM ** -0.5

    def one_block(q_part):
        scores = jnp.einsum("qhe,khe->hqk", q_part, key_h) * score_scale
        row_max = jnp.max(scores, -1, keepdims=True)
        weights = jnp.exp(scores - row_max)
        row_sum = jnp.sum(weights, -1)
        mixed_out = jnp.einsum("hqk,khe->qhe", weights.astype(jnp.bfloat16).astype(jnp.float32), val_h)
        return (mixed_out / row_sum.T[:, :, None]).astype(jnp.bfloat16)

    return lax.map(one_block, blocks).reshape(ROWS, HEADS, HEAD_DIM)


def dit_block(resid_now, mod_now, qkv_layer, out_layer, up_layer, down_layer, k_old, v_old):
    shift_attn, scale_attn, gate_attn, shift_mlp, scale_mlp, gate_mlp = jnp.split(mod_now, 6)
    norm_attn = (layer_norm(resid_now) * (1.0 + scale_attn) + shift_attn).astype(jnp.bfloat16)
    qkv_all = jnp.dot(norm_attn, qkv_layer, preferred_element_type=jnp.float32).astype(jnp.bfloat16)
    q_new, k_new, v_new = jnp.split(qkv_all, 3, axis=-1)

    def per_patch(patch_pos):
        row_start = patch_pos * ROWS
        key_set = lax.dynamic_update_slice(k_old, lax.dynamic_slice_in_dim(k_new, row_start, ROWS), (row_start, 0))
        value_set = lax.dynamic_update_slice(v_old, lax.dynamic_slice_in_dim(v_new, row_start, ROWS), (row_start, 0))
        return attend(lax.dynamic_slice_in_dim(q_new, row_start, ROWS), key_set, value_set)

    heads_out = lax.map(per_patch, jnp.arange(N_PATCH)).reshape(TOKENS, HEADS, HEAD_DIM)
    attn_out = jnp.einsum("nhe,hed->nd", heads_out.astype(jnp.float32), out_layer.astype(jnp.float32))
    resid_now = resid_now + gate_attn * attn_out
    norm_mlp = (layer_norm(resid_now) * (1.0 + scale_mlp) + shift_mlp).astype(jnp.bfloat16)
    mlp_up = jnp.dot(norm_mlp, up_layer, preferred_element_type=jnp.float32)
    mlp_act = jax.nn.gelu(mlp_up, approximate=True).astype(jnp.bfloat16)
    mlp_down = jnp.dot(mlp_act, down_layer, preferred_element_type=jnp.float32)
    resid_now = resid_now + gate_mlp * mlp_down
    return resid_now, k_new, v_new


def reference(latent, cond_vec, sched_coef, w_ada, w_qkv, w_out, w_up, w_down, w_head, k_stale, v_stale):
    def one_slot(slot_in):
        img_latent, silu_slot, k_slot, v_slot = slot_in

        def layer_body(resid_now, layer_in):
            ada_layer, qkv_layer, out_layer, up_layer, down_layer, k_old, v_old = layer_in
            mod_now = jnp.dot(silu_slot, ada_layer, preferred_element_type=jnp.float32)
            resid_now, k_new, v_new = dit_block(resid_now, mod_now, qkv_layer, out_layer, up_layer, down_layer, k_old, v_old)
            return resid_now, (k_new, v_new)

        resid_now, fresh_kv = lax.scan(layer_body, img_latent, (w_ada, w_qkv, w_out, w_up, w_down, k_slot, v_slot))
        eps_own = jnp.dot(layer_norm(resid_now).astype(jnp.bfloat16), w_head, preferred_element_type=jnp.float32).astype(jnp.bfloat16)
        return eps_own, fresh_kv[0], fresh_kv[1]

    latent_now = latent.astype(jnp.float32)
    silu_all = jax.nn.silu(cond_vec).astype(jnp.bfloat16)
    k_cache = k_stale
    v_cache = v_stale
    for step_idx in range(N_STEPS):
        slot_in = (jnp.repeat(latent_now, 2, axis=0), silu_all[:, step_idx], k_cache, v_cache)
        eps_own, k_cache, v_cache = lax.map(one_slot, slot_in)
        eps_pairs = eps_own.astype(jnp.float32).reshape(N_PAIRS, 2, TOKENS, D)
        eps_cond = eps_pairs[:, 0]
        eps_unc = eps_pairs[:, 1]
        guided = eps_unc + sched_coef[2, step_idx] * (eps_cond - eps_unc)
        latent_now = sched_coef[0, step_idx] * latent_now + sched_coef[1, step_idx] * guided
    return jnp.repeat(latent_now, 2, axis=0), k_cache, v_cache
```

```python
import jax
import jax.numpy as jnp
from jax import lax
from jax.experimental import pallas as pl
from jax.experimental.pallas import tpu as pltpu
from jax.sharding import PartitionSpec as P

RING = 4
AXES = ("z", "y", "x")
COLOR_ORDERS = (("x", "y", "z"), ("y", "z", "x"), ("z", "x", "y"))
MESH = pl.DeviceIdType.MESH


def layer_norm(values):
    row_mean = jnp.mean(values, -1, keepdims=True)
    centered = values - row_mean
    row_var = jnp.mean(centered * centered, -1, keepdims=True)
    return centered * lax.rsqrt(row_var + 1e-6)


def attend(queries, key_set, value_set, n_heads, head_dim):
    local_rows = queries.shape[0]
    tokens = key_set.shape[0]
    q_blk = min(local_rows, 128)
    blocks = queries.reshape(local_rows // q_blk, q_blk, n_heads, head_dim)
    key_h = key_set.reshape(tokens, n_heads, head_dim)
    val_h = value_set.reshape(tokens, n_heads, head_dim)
    score_scale = head_dim ** -0.5

    def one_block(q_part):
        scores = jnp.einsum("qhe,khe->hqk", q_part, key_h, preferred_element_type=jnp.float32) * score_scale
        row_max = jnp.max(scores, -1, keepdims=True)
        weights = jnp.exp(scores - row_max)
        row_sum = jnp.sum(weights, -1)
        mixed_out = jnp.einsum("hqk,khe->qhe", weights.astype(jnp.bfloat16), val_h, preferred_element_type=jnp.float32)
        return (mixed_out / row_sum.T[:, :, None]).astype(jnp.bfloat16)

    return lax.map(one_block, blocks).reshape(local_rows, n_heads, head_dim)


def torus_position():
    patch = lax.axis_index("patch")
    return {"z": patch // (RING * RING), "y": (patch // RING) % RING, "x": patch % RING}


def patch_at(pos):
    return (pos["z"] * RING + pos["y"]) * RING + pos["x"]


def shifted(pos, axis, by):
    return {**pos, axis: lax.rem(pos[axis] + (by % RING), RING)}


def device_of(pos):
    return {"patch": patch_at(pos)}


def ring_copies(ref, color, stage, pos, send_sem, recv_sem):
    order = COLOR_ORDERS[color]
    axis = order[stage]
    width = ref.shape[4] // 3
    base = color * width
    half = width // 2

    def region(coord, start, size):
        index = []
        for name in AXES:
            if name == axis:
                index.append(coord)
            elif name in order[:stage]:
                index.append(slice(None))
            else:
                index.append(pos[name])
        return ref.at[(*index, slice(None), pl.ds(start, size))]

    def copy(coord, start, size, to, slot):
        part = region(coord, start, size)
        return pltpu.make_async_remote_copy(
            src_ref=part,
            dst_ref=part,
            send_sem=send_sem.at[slot],
            recv_sem=recv_sem.at[slot],
            device_id=device_of(shifted(pos, axis, to)),
            device_id_type=MESH,
        )

    me = pos[axis]
    prev = lax.rem(me + RING - 1, RING)
    succ = lax.rem(me + 1, RING)
    return (
        copy(me, base, width, 1, 0),
        copy(me, base, width, -1, 1),
        copy(prev, base, half, 1, 2),
        copy(succ, base + half, half, -1, 3),
    )


def gather_kernel(own_k, own_v, all_k, all_v, local_sem, send_sem, recv_sem):
    pos = torus_position()
    barrier = pltpu.get_barrier_semaphore()
    for axis in AXES:
        for by in (1, -1):
            pl.semaphore_signal(barrier, inc=1, device_id=device_of(shifted(pos, axis, by)), device_id_type=MESH)
    n_layers = own_k.shape[0]
    placed = []
    for src, dst in ((own_k, all_k), (own_v, all_v)):
        for layer in range(n_layers):
            mine = dst.at[layer, pos["z"], pos["y"], pos["x"]]
            put = pltpu.make_async_copy(src.at[layer], mine, local_sem.at[len(placed)])
            put.start()
            placed.append(put)
    pl.semaphore_wait(barrier, 6)
    for put in placed:
        put.wait()
    whole = [dst.at[layer] for layer in range(n_layers) for dst in (all_k, all_v)]
    jobs = [(t, color) for t in range(len(whole)) for color in range(3)]
    sent = []
    ready = {}
    for stage in range(3):
        copies = {
            (t, color): ring_copies(whole[t], color, stage, pos, send_sem.at[t, color, stage], recv_sem.at[t, color, stage])
            for t, color in jobs
        }
        for job in jobs:
            for done in ready.get(job, ()):
                done.wait_recv()
            for first in copies[job][:2]:
                first.start()
        for job in jobs:
            copies[job][0].wait_recv()
            copies[job][2].start()
            copies[job][1].wait_recv()
            copies[job][3].start()
            ready[job] = copies[job][2:]
            sent.extend(copies[job])
    for job in jobs:
        for done in ready[job]:
            done.wait_recv()
    for one in sent:
        one.wait_send()


def gather_patches(own_k, own_v):
    n_layers, rows, width = own_k.shape
    full = jax.ShapeDtypeStruct((n_layers, RING, RING, RING, rows, width), own_k.dtype)
    out_k, out_v = pl.pallas_call(
        gather_kernel,
        out_shape=(full, full),
        in_specs=[pl.BlockSpec(memory_space=pltpu.VMEM)] * 2,
        out_specs=[pl.BlockSpec(memory_space=pl.ANY)] * 2,
        scratch_shapes=[
            pltpu.SemaphoreType.DMA((2 * n_layers,)),
            pltpu.SemaphoreType.DMA((2 * n_layers, 3, 3, 4)),
            pltpu.SemaphoreType.DMA((2 * n_layers, 3, 3, 4)),
        ],
        compiler_params=pltpu.CompilerParams(collective_id=0, has_side_effects=True),
        name="torus_gather",
    )(own_k, own_v)
    tokens = RING * RING * RING * rows
    return out_k.reshape(n_layers, tokens, width), out_v.reshape(n_layers, tokens, width)


def solution(mesh):
    n_cfg = mesh.shape["cfg"]
    partner = [(dev_pos, dev_pos ^ 1) for dev_pos in range(n_cfg)]
    slot_spec = P(("img", "cfg"), None, None)
    cache_spec = P(("img", "cfg"), None, None, None)
    rep_spec = P()

    def local_step(latent, cond_vec, sched_coef, w_ada, w_qkv, w_out, w_up, w_down, w_head, k_stale, v_stale):
        n_layers = k_stale.shape[1]
        local_rows = latent.shape[1]
        n_heads = w_out.shape[1]
        head_dim = w_out.shape[2]
        n_steps = sched_coef.shape[1]
        cfg_slot = lax.axis_index("cfg")
        row_start = lax.axis_index("patch") * local_rows
        is_cond = cfg_slot % 2 == 0
        latent_now = lax.dynamic_index_in_dim(latent, cfg_slot // 2, axis=0, keepdims=False).astype(jnp.float32)
        mod_all = jnp.einsum("td,lde->tle", jax.nn.silu(cond_vec[0]).astype(jnp.bfloat16), w_ada, preferred_element_type=jnp.float32)
        k_cache = [k_stale[0, layer_idx] for layer_idx in range(n_layers)]
        v_cache = [v_stale[0, layer_idx] for layer_idx in range(n_layers)]
        for step_idx in range(n_steps):
            resid_now = latent_now
            k_next = []
            v_next = []
            for layer_idx in range(n_layers):
                shift_attn, scale_attn, gate_attn, shift_mlp, scale_mlp, gate_mlp = jnp.split(mod_all[step_idx, layer_idx], 6)
                norm_attn = (layer_norm(resid_now) * (1.0 + scale_attn) + shift_attn).astype(jnp.bfloat16)
                qkv_all = jnp.dot(norm_attn, w_qkv[layer_idx], preferred_element_type=jnp.float32).astype(jnp.bfloat16)
                q_new, k_new, v_new = jnp.split(qkv_all, 3, axis=-1)
                if step_idx < n_steps - 1:
                    k_next.append(lax.all_gather(k_new, "patch", axis=0, tiled=True))
                    v_next.append(lax.all_gather(v_new, "patch", axis=0, tiled=True))
                else:
                    k_next.append(k_new)
                    v_next.append(v_new)
                key_set = lax.dynamic_update_slice(k_cache[layer_idx], k_new, (row_start, 0))
                value_set = lax.dynamic_update_slice(v_cache[layer_idx], v_new, (row_start, 0))
                heads_out = attend(q_new, key_set, value_set, n_heads, head_dim)
                attn_out = jnp.einsum("qhe,hed->qd", heads_out, w_out[layer_idx], preferred_element_type=jnp.float32)
                resid_now = resid_now + gate_attn * attn_out
                norm_mlp = (layer_norm(resid_now) * (1.0 + scale_mlp) + shift_mlp).astype(jnp.bfloat16)
                mlp_up = jnp.dot(norm_mlp, w_up[layer_idx], preferred_element_type=jnp.float32)
                mlp_act = jax.nn.gelu(mlp_up, approximate=True).astype(jnp.bfloat16)
                mlp_down = jnp.dot(mlp_act, w_down[layer_idx], preferred_element_type=jnp.float32)
                resid_now = resid_now + gate_mlp * mlp_down
            k_cache = k_next
            v_cache = v_next
            eps_own = jnp.dot(layer_norm(resid_now).astype(jnp.bfloat16), w_head, preferred_element_type=jnp.float32).astype(jnp.bfloat16)
            eps_peer = lax.ppermute(eps_own, "cfg", partner)
            eps_cond = jnp.where(is_cond, eps_own, eps_peer).astype(jnp.float32)
            eps_unc = jnp.where(is_cond, eps_peer, eps_own).astype(jnp.float32)
            guided = eps_unc + sched_coef[2, step_idx] * (eps_cond - eps_unc)
            latent_now = sched_coef[0, step_idx] * latent_now + sched_coef[1, step_idx] * guided
        k_last, v_last = gather_patches(jnp.stack(k_cache), jnp.stack(v_cache))
        return latent_now[None], k_last[None], v_last[None]

    return jax.shard_map(
        local_step,
        mesh=mesh,
        in_specs=(P("img", "patch", None), slot_spec, rep_spec, rep_spec, rep_spec, rep_spec, rep_spec, rep_spec, rep_spec, cache_spec, cache_spec),
        out_specs=(P(("img", "cfg"), "patch", None), cache_spec, cache_spec),
        check_vma=False,
    )
```

```python
import functools

import jax
import jax.numpy as jnp
from jax import lax
from jax.experimental import pallas as pl
from jax.experimental.pallas import tpu as pltpu
from jax.sharding import PartitionSpec as P

RING = 4
AXES = ("z", "y", "x")
COLOR_ORDERS = (("x", "y", "z"), ("y", "z", "x"), ("z", "x", "y"))
SHARE_ORDERS = (("y", "x"), ("x", "y"))
MESH = pl.DeviceIdType.MESH
F32 = jnp.float32
BF16 = jnp.bfloat16
HEAD = 128
TILE = 512
SUB = 256
WIDE = 2 * TILE
BUFFERS = 11
STEPS = 2
LAYERS = 2
K, V, Q = 0, 1, 2


def dot(lhs, rhs):
    return jnp.dot(lhs, rhs, preferred_element_type=F32)


def torus_position():
    patch = lax.axis_index("patch")
    return {"z": lax.div(patch, RING * RING), "y": lax.rem(lax.div(patch, RING), RING), "x": lax.rem(patch, RING)}


def patch_at(pos):
    return (pos["z"] * RING + pos["y"]) * RING + pos["x"]


class Torus:
    def __init__(self):
        self.pos = torus_position()
        self.coord, self.patch = {}, {}
        for axis in AXES:
            for by in range(1, RING):
                coord = lax.rem(self.pos[axis] + by, RING)
                self.coord[axis, by] = coord
                self.patch[axis, by] = patch_at({**self.pos, axis: coord})


def remote(src, dst, send_sem, recv_sem, **device_id):
    return pltpu.make_async_remote_copy(
        src_ref=src, dst_ref=dst, send_sem=send_sem, recv_sem=recv_sem, device_id=device_id, device_id_type=MESH
    )


class Ring:
    def __init__(self, torus, axis, view, send_sem, recv_sem):
        me, succ, prev = torus.pos[axis], torus.coord[axis, 1], torus.coord[axis, RING - 1]
        ahead, behind = torus.patch[axis, 1], torus.patch[axis, RING - 1]
        self.sends = ((me, None, ahead), (me, None, behind), (prev, 0, ahead), (succ, 1, behind))
        self.parts = (view, send_sem, recv_sem)

    def copy(self, slot):
        view, send_sem, recv_sem = self.parts
        coord, half, patch = self.sends[slot]
        part = view(coord, half)
        return remote(part, part, send_sem(slot), recv_sem(slot), patch=patch)

    def first(self):
        for slot in (0, 1):
            self.copy(slot).start()

    def relay(self):
        for slot in (0, 1):
            self.copy(slot).wait_recv()
            self.copy(slot + 2).start()

    def settle(self):
        for slot in (2, 3):
            self.copy(slot).wait_recv()

    def drain(self):
        for slot in range(4):
            self.copy(slot).wait_send()


def full_rings(ref, color, torus, send_sem, recv_sem):
    width = ref.shape[4]
    cut = [0, width // 3 // SUB * SUB, width // 3 // SUB * SUB * 2, width]
    base, size = cut[color], cut[color + 1] - cut[color]
    order = COLOR_ORDERS[color]

    def stage(k):
        axis = order[k]

        def view(coord, half):
            index = []
            for name in AXES:
                index.append(coord if name == axis else slice(None) if name in order[:k] else torus.pos[name])
            columns = pl.ds(base, size) if half is None else pl.ds(base + half * (size // 2), size // 2)
            return ref.at[(*index, slice(None), columns)]

        return Ring(torus, axis, view, lambda slot: send_sem.at[k, slot], lambda slot: recv_sem.at[k, slot])

    return [stage(k) for k in range(3)]


def share_rings(ref, color, torus, send_sem, recv_sem):
    size = ref.shape[4] // 2
    order = SHARE_ORDERS[color]
    columns = pl.ds(color * size, size)

    def stage(k):
        axis = order[k]

        def view(coord, half):
            planes = slice(None) if half is None else pl.ds(half * (RING // 2), RING // 2)
            index = [coord if name == axis else slice(None) if name in order[:k] else torus.pos[name] for name in ("y", "x")]
            return ref.at[(planes, *index, slice(None), columns)]

        return Ring(torus, axis, view, lambda slot: send_sem.at[k, slot], lambda slot: recv_sem.at[k, slot])

    return [stage(k) for k in range(2)]


def denoise_kernel(
    lat, cond, sched, w_ada, w_qkv, w_out, w_up, w_down, w_head, k_old, v_old,
    lat_out, all_k, all_v, shared,
    wbuf, kbuf, vbuf, xs, r, h, act, out_own, out_peer, down_own, down_peer, sb, rb, o_own, ob, mod, cond_peer, scores,
    w_sem, kv_sem, cond_sem, mod_send, mod_recv, qkv_send, qkv_recv, o_send, o_recv, out_send, out_recv, down_send, down_recv,
    x_sem, share_put, share_send, share_recv, own_put, own_send, own_recv, full_send, full_recv,
):
    rows, width = lat.shape
    half = width // 2
    group = width // RING
    chunk = width // 8
    hidden = w_up.shape[2] // 2
    n_qkv = half // TILE
    n_out = width // WIDE
    n_up = hidden // TILE
    n_deep = hidden // half
    n_down = n_out * n_deep
    n_head = half // TILE
    n_block = 3 * n_qkv + n_out + n_up + n_down
    n_step = LAYERS * n_block + n_head
    n_ada = 3
    n_tiles = n_ada + STEPS * n_step
    n_buf = wbuf.shape[0]
    scale = HEAD**-0.5

    c = lax.axis_index("cfg")
    other = 1 - c
    torus = Torus()
    z, y, x = (torus.pos[axis] for axis in AXES)
    z_core = lax.div(z, 2)
    z_odd = lax.rem(z, 2)
    z_patch = [(v * RING + y) * RING + x for v in range(RING)]
    pair_patch = [((2 * c + g) * RING + y) * RING + x for g in range(2)]

    def put(src, dst, slot):
        pltpu.make_async_copy(src, dst, w_sem.at[slot]).start()

    def put_deep(ref, col, slot):
        col = pl.multiple_of(col, TILE)
        for k in range(2):
            put(ref.at[pl.ds(k * half, half), pl.ds(col, TILE)], wbuf.at[slot, :, pl.ds(k * TILE, TILE)], slot)

    def put_wide(ref, row, col, slot):
        row = pl.multiple_of(row, half)
        col = pl.multiple_of(col, WIDE)
        put(ref.at[pl.ds(row, half), pl.ds(col, WIDE)], wbuf.at[slot], slot)

    def issue_ada(i):
        col = pl.multiple_of(((y * RING + x) * n_ada + i) * chunk, chunk)
        for k in range(2):
            put(w_ada.at[c, pl.ds(k * half, half), pl.ds(col, chunk)], wbuf.at[i, :, pl.ds(k * chunk, chunk)], i)

    def issue(n):
        slot = lax.rem(n, n_buf)
        inside = lax.rem(n - n_ada, n_step)
        layer = lax.div(inside, n_block)
        u = lax.rem(inside, n_block)
        live = n < n_tiles
        block = live & (inside < LAYERS * n_block)
        at_out, at_up, at_down = 3 * n_qkv, 3 * n_qkv + n_out, 3 * n_qkv + n_out + n_up

        @pl.when(block & (u < at_out))
        def _():
            part = lax.rem(lax.div(u, n_qkv) + 1, 3)
            put_deep(w_qkv.at[layer], part * width + c * half + lax.rem(u, n_qkv) * TILE, slot)

        @pl.when(block & (u >= at_out) & (u < at_up))
        def _():
            put_wide(w_out.at[layer], c * half, (u - at_out) * WIDE, slot)

        @pl.when(block & (u >= at_up) & (u < at_down))
        def _():
            put_deep(w_up.at[layer], c * hidden + (u - at_up) * TILE, slot)

        @pl.when(block & (u >= at_down))
        def _():
            d = u - at_down
            put_wide(w_down.at[layer], c * hidden + lax.rem(d, n_deep) * half, lax.div(d, n_deep) * WIDE, slot)

        @pl.when(live & (inside >= LAYERS * n_block))
        def _():
            put_deep(w_head, c * half + (inside - LAYERS * n_block) * TILE, slot)

    def tile_loop(base, count, body, hooks=()):
        def one(t, carry):
            n = base + t
            slot = lax.rem(n, n_buf)
            tile = wbuf.at[slot]
            pltpu.make_async_copy(tile, tile, w_sem.at[slot]).wait()
            body(t, tile)
            issue(n + n_buf)
            for at, when, hook in hooks:
                pl.when((t == at) & when)(hook)
            return carry

        lax.fori_loop(0, count, one, 0)

    def deep_dot(tile):
        return dot(h[:, :half], tile[:, :TILE]) + dot(h[:, half:], tile[:, TILE:])

    def load_kv(old_k, old_v):
        for i, src in ((K, old_k), (V, old_v)):
            pltpu.make_async_copy(src, (kbuf, vbuf)[i], kv_sem.at[i]).start()

    def load_stale(b):
        columns = pl.ds(pl.multiple_of(z * group, group), group)
        load_kv(k_old.at[b, :, :, :, :, columns], v_old.at[b, :, :, :, :, columns])

    def load_shared(b):
        load_kv(shared.at[b, K], shared.at[b, V])

    share = [
        [share_rings(shared.at[b, i], color, torus, share_send.at[b, i, color], share_recv.at[b, i, color]) for i in (K, V) for color in range(2)]
        for b in range(LAYERS)
    ]
    full = [
        [
            [full_rings((all_k, all_v)[i].at[b], color, torus, full_send.at[b, i, color], full_recv.at[b, i, color]) for color in range(3)]
            for i in (K, V)
        ]
        for b in range(LAYERS)
    ]

    def first(rings, k):
        for ring in rings:
            if k:
                ring[k - 1].settle()
            ring[k].first()

    def relay(rings, k):
        for ring in rings:
            ring[k].relay()

    def settle(rings, k):
        for ring in rings:
            ring[k].settle()

    barrier = pltpu.get_barrier_semaphore()

    def announce(**device_id):
        pl.semaphore_signal(barrier, inc=1, device_id=device_id, device_id_type=MESH)

    for i in range(n_ada):
        issue_ada(i)
    announce(cfg=other)
    for by in range(1, RING):
        for core in range(2):
            announce(patch=torus.patch["z", by], cfg=core)
        announce(patch=torus.patch["y", by])
        announce(patch=torus.patch["x", by])
    pl.semaphore_wait(barrier, 1 + 4 * (RING - 1))

    cond_swap = remote(cond, cond_peer, cond_sem.at[0], cond_sem.at[1], cfg=other)
    cond_swap.start()
    xs[0] = lat[...].astype(F32)
    cond_swap.wait()
    mine, theirs = cond[...], cond_peer[...]
    both = jnp.concatenate([jnp.where(c == 0, mine, theirs), jnp.where(c == 0, theirs, mine)], axis=0)
    silu = (both * jax.nn.sigmoid(both)).astype(BF16)
    for i in range(n_ada):
        filled = wbuf.at[i, :, pl.ds(0, 2 * chunk)]
        pltpu.make_async_copy(filled, filled, w_sem.at[i]).wait()
    for n in range(n_ada, n_buf):
        issue(jnp.int32(n))
    load_stale(0)
    for i in range(n_ada):
        tile = wbuf.at[i]
        mod[c, y, x, :, pl.ds(i * chunk, chunk)] = dot(silu[:, :half], tile[:, :chunk]) + dot(silu[:, half:], tile[:, chunk : 2 * chunk])
        issue(jnp.int32(n_buf + i))
    mod_copies = []
    for axis, part in (("y", mod.at[c, y, x]), ("x", mod.at[c, :, x])):
        stage = []
        for by in range(1, RING):
            slot = len(mod_copies) + len(stage)
            stage.append(remote(part, part, mod_send.at[slot], mod_recv.at[slot], patch=torus.patch[axis, by]))
        for one in stage:
            one.start()
        for one in stage:
            one.wait_recv()
        mod_copies += stage
    mod_swap = remote(mod.at[c], mod.at[c], mod_send.at[len(mod_copies)], mod_recv.at[len(mod_copies)], cfg=other)
    mod_swap.start()
    mod_swap.wait_recv()
    mod_copies.append(mod_swap)

    def mod_row(b, step, which, i, s):
        piece = which * 8 + i
        at = piece // n_ada
        columns = slice((piece % n_ada) * chunk, (piece % n_ada + 1) * chunk)
        both = mod[b, at // RING, at % RING, s * STEPS : (s + 1) * STEPS, columns]
        return jnp.where(step == 0, both[0:1], both[1:2])

    def normed(s):
        values = r[s * rows : (s + 1) * rows, :]
        centered = values - jnp.mean(values, -1, keepdims=True)
        return centered * lax.rsqrt(jnp.mean(centered * centered, -1, keepdims=True) + 1e-6)

    def modulate(b, step, shift, gain):
        for s in range(2):
            values = normed(s)
            for i in range(8):
                at = slice(i * chunk, (i + 1) * chunk)
                part = values[:, at] * (1.0 + mod_row(b, step, gain, i, s)) + mod_row(b, step, shift, i, s)
                h[s * rows : (s + 1) * rows, at] = part.astype(BF16)

    def add_gated(b, step, gate, own, peer):
        for s in range(2):
            for i in range(8):
                at = (slice(s * rows, (s + 1) * rows), slice(i * chunk, (i + 1) * chunk))
                r[at] = r[at] + mod_row(b, step, gate, i, s) * (own[at] + peer[at])

    def chunk_swap(own, peer, t, send_sem, recv_sem):
        columns = pl.ds(pl.multiple_of(t * WIDE, WIDE), WIDE)
        return remote(own.at[:, columns], peer.at[:, columns], send_sem.at[t], recv_sem.at[t], cfg=other)

    def qkv_copy(p, s, g):
        return remote(sb.at[s, g, p], rb.at[p, z], qkv_send.at[p, s, g], qkv_recv.at[p, z], patch=pair_patch[g], cfg=s)

    def qkv_out(p, do_send):
        for s in range(2):
            for g in range(2):
                here = (2 * c + g == z) & (c == s)
                away = (2 * c + g != z) | (c != s)
                if do_send:

                    @pl.when(here)
                    def _():
                        rb[p, z] = sb[s, g, p]

                    @pl.when(away)
                    def _():
                        qkv_copy(p, s, g).start()
                else:

                    @pl.when(away)
                    def _():
                        qkv_copy(p, s, g).wait_send()

    def qkv_in(p):
        for src in range(RING):

            @pl.when((z != src) | (c != z_core))
            def _():
                part = rb.at[p, src]
                remote(part, part, qkv_send.at[p, 0, 0], qkv_recv.at[p, src], cfg=other).wait_recv()

    def qkv_part(p, base):
        def body(t, tile):
            part = deep_dot(tile).astype(BF16)
            for k in range(TILE // SUB):
                col = t * TILE + k * SUB
                g = lax.div(col, group)
                columns = pl.ds(pl.multiple_of(col - g * group, SUB), SUB)
                for s in range(2):
                    sb[s, g, p, :, columns] = part[s * rows : (s + 1) * rows, k * SUB : (k + 1) * SUB]

        tile_loop(base + p * n_qkv, n_qkv, body)
        qkv_out(p, True)

    def own_copies(b, i):
        local, swap = [], []
        for g in range(2):
            columns = pl.ds(pl.multiple_of(c * half + g * group, group), group)
            place = (all_k, all_v)[i].at[b, z, y, x, :, columns]
            local.append(pltpu.make_async_copy(sb.at[c, g, i], place, own_put.at[i, g]))
            swap.append(remote(sb.at[other, g, i], place, own_send.at[i, g], own_recv.at[i, g], cfg=other))
        return local, swap

    def own_start(b, i):
        local, swap = own_copies(b, i)
        for one in local + swap:
            one.start()

    def own_wait(b, i):
        local, swap = own_copies(b, i)
        for one in local + swap:
            one.wait()

    def share_copy(b, i):
        return pltpu.make_async_copy(rb.at[i], shared.at[b, i, :, y, x], share_put.at[i])

    tokens_z = RING * RING * rows
    n_rows = RING * rows

    def attention(hooks):
        def patch_of(index):
            return lax.div(index, jnp.full_like(index, rows))

        row_z = patch_of(lax.broadcasted_iota(jnp.int32, (n_rows, tokens_z), 0))
        col_p = patch_of(lax.broadcasted_iota(jnp.int32, (n_rows, tokens_z), 1))
        row_f = patch_of(lax.broadcasted_iota(jnp.int32, (n_rows, n_rows), 0))
        col_f = patch_of(lax.broadcasted_iota(jnp.int32, (n_rows, n_rows), 1))

        def scored(queries, keys):
            return lax.dot_general(queries, keys, (((1,), (1,)), ((), ())), preferred_element_type=F32)

        def one(head, carry):
            at = pl.ds(pl.multiple_of(head * HEAD, HEAD), HEAD)
            queries = rb[Q, :, :, at].reshape(n_rows, HEAD)
            fresh = scored(queries, rb[K, :, :, at].reshape(n_rows, HEAD))
            fresh = jnp.where(row_f == col_f, fresh, -jnp.inf)
            top = jnp.max(fresh, -1, keepdims=True)
            for plane in range(RING):
                part = scored(queries, kbuf[plane, :, :, :, at].reshape(tokens_z, HEAD))
                part = jnp.where((row_z == plane) & (col_p == y * RING + x), -jnp.inf, part)
                scores[:, plane * tokens_z : (plane + 1) * tokens_z] = part
                top = jnp.maximum(top, jnp.max(part, -1, keepdims=True))
            weights = jnp.exp((fresh - top) * scale)
            total = jnp.sum(weights, -1, keepdims=True)
            mixed = dot(weights.astype(BF16), rb[V, :, :, at].reshape(n_rows, HEAD))
            for plane in range(RING):
                weights = jnp.exp((scores[:, plane * tokens_z : (plane + 1) * tokens_z] - top) * scale)
                total = total + jnp.sum(weights, -1, keepdims=True)
                mixed = mixed + dot(weights.astype(BF16), vbuf[plane, :, :, :, at].reshape(tokens_z, HEAD))
            o_own[:, :, at] = (mixed / total).astype(BF16).reshape(RING, rows, HEAD)
            for at, when, hook in hooks:
                pl.when((head == at) & when)(hook)
            return carry

        for i in (K, V):
            buf = (kbuf, vbuf)[i]
            pltpu.make_async_copy(buf, buf, kv_sem.at[i]).wait()
        lax.fori_loop(0, group // HEAD, one, 0)

    def o_copy(dst):
        return remote(o_own.at[dst], ob.at[c, z_odd], o_send.at[dst], o_recv.at[c, z_odd], patch=z_patch[dst], cfg=z_core)

    def o_out(do_send):
        for dst in range(RING):
            if do_send:

                @pl.when((z == dst) & (c == z_core))
                def _():
                    ob[c, z_odd] = o_own[dst]

            @pl.when((z != dst) | (c != z_core))
            def _():
                if do_send:
                    o_copy(dst).start()
                else:
                    o_copy(dst).wait_send()

    def o_in():
        for s in range(2):
            for g in range(2):

                @pl.when((2 * c + g != z) | (c != s))
                def _():
                    part = ob.at[s, g]
                    remote(part, part, o_send.at[0], o_recv.at[s, g], cfg=other).wait_recv()

    def block(step, b):
        base = n_ada + step * n_step + b * n_block
        begin = step == 0
        last = step == STEPS - 1
        heads = group // HEAD
        no_hooks = ()

        def unless_first(action):
            if b:
                action()
            else:
                pl.when(step > 0)(action)

        if b == 0:
            for s in range(2):
                r[s * rows : (s + 1) * rows, :] = xs[step]
        modulate(b, step, 0, 1)

        @unless_first
        def _():
            for p in (K, V, Q):
                qkv_out(p, False)

        qkv_part(K, base)

        @pl.when(last)
        def _():
            own_start(b, K)

        qkv_part(V, base)

        @pl.when(last)
        def _():
            own_start(b, V)
            own_wait(b, K)
            first(full[b][K], 0)

        @pl.when(begin if b else last)
        def _():
            relay(share[1 - b], 1)

        qkv_part(Q, base)

        @pl.when(last)
        def _():
            own_wait(b, V)
            first(full[b][V], 0)
            if b:
                first(full[0][V], 2)

        for p in (K, V, Q):
            qkv_in(p)

        @pl.when(begin)
        def _():
            for p in (K, V):
                share_copy(b, p).start()

        @unless_first
        def _():
            o_out(False)

        if b:
            hooks = ((heads - 1, last, lambda: relay(full[0][K], 2)),)
        else:
            hooks = ((heads // 3, last, lambda: relay(full[0][K], 0)), (heads - 1, last, lambda: relay(full[0][V], 0)))
        attention(hooks)

        @pl.when(begin)
        def _():
            for p in (K, V):
                share_copy(b, p).wait()

        o_out(True)

        @pl.when(begin)
        def _():
            if b == 0:
                load_stale(1)
            first(share[b], 0)

        @pl.when(last)
        def _():
            if b == 0:
                first(full[0][K], 1)
            else:
                relay(full[1][K], 0)
                relay(full[1][V], 0)

        o_in()

        def out_body(t, tile):
            columns = pl.ds(pl.multiple_of(t * WIDE, WIDE), WIDE)
            part = [ob[:, g].reshape(2 * rows, group) for g in range(2)]
            out_own[:, columns] = dot(part[0], tile[:group]) + dot(part[1], tile[group:])
            chunk_swap(out_own, out_peer, t, out_send, out_recv).start()

        @unless_first
        def _():
            for t in range(n_out):
                chunk_swap(out_own, out_peer, t, out_send, out_recv).wait_send()

        tile_loop(base + 3 * n_qkv, n_out, out_body)
        if b == 0:

            @pl.when(last)
            def _():
                first(full[0][V], 1)

        for t in range(n_out):
            chunk_swap(out_own, out_peer, t, out_send, out_recv).wait_recv()
        add_gated(b, step, 2, out_own, out_peer)
        modulate(b, step, 3, 4)

        def up_body(t, tile):
            act[:, pl.ds(pl.multiple_of(t * TILE, TILE), TILE)] = jax.nn.gelu(deep_dot(tile), approximate=True).astype(BF16)

        def refill(share_in, then):
            settle(share_in, 1)
            load_shared(1 - b)
            then()

        if b:
            hooks = (
                (1, begin, lambda: refill(share[0], lambda: relay(share[1], 0))),
                (n_up // 2, begin, lambda: first(share[1], 1)),
            )
        else:
            hooks = (
                (1, begin, lambda: relay(share[0], 0)),
                (n_up // 2, begin, lambda: first(share[0], 1)),
                (1, last, lambda: refill(share[1], lambda: None)),
                (n_up // 2 - 1, last, lambda: relay(full[0][K], 1)),
                (n_up * 3 // 4, last, lambda: relay(full[0][V], 1)),
            )
        tile_loop(base + 3 * n_qkv + n_out, n_up, up_body, hooks)

        def down_body(t, tile):
            n = lax.div(t, n_deep)
            deep = lax.rem(t, n_deep)
            columns = pl.ds(pl.multiple_of(n * WIDE, WIDE), WIDE)
            part = dot(act[:, pl.ds(pl.multiple_of(deep * half, half), half)], tile[...])

            @pl.when(deep == 0)
            def _():
                down_own[:, columns] = part

            @pl.when(deep != 0)
            def _():
                down_own[:, columns] = down_own[:, columns] + part

            @pl.when(deep == n_deep - 1)
            def _():
                chunk_swap(down_own, down_peer, n, down_send, down_recv).start()

        @unless_first
        def _():
            for t in range(n_out):
                chunk_swap(down_own, down_peer, t, down_send, down_recv).wait_send()

        if b:
            hooks = (
                (n_down // 2, last, lambda: first(full[1][K] + full[1][V], 1)),
                (n_down - 1, last, lambda: relay(full[0][V], 2)),
            )
        else:
            hooks = ((0, last, lambda: first(full[0][K], 2)),)
        tile_loop(base + 3 * n_qkv + n_out + n_up, n_down, down_body, hooks)
        for t in range(n_out):
            chunk_swap(down_own, down_peer, t, down_send, down_recv).wait_recv()
        add_gated(b, step, 5, down_own, down_peer)

    def one_step(step, carry):
        for b in range(LAYERS):
            block(step, b)
        for s in range(2):
            h[s * rows : (s + 1) * rows, :] = normed(s).astype(BF16)
        later = lax.rem(step + 1, STEPS)

        def head_body(t, tile):
            eps = deep_dot(tile).astype(BF16).astype(F32)
            with_cond, without = eps[:rows], eps[rows:]
            guided = without + sched[2, step] * (with_cond - without)
            columns = pl.ds(pl.multiple_of(c * half + t * TILE, TILE), TILE)
            xs[later, :, columns] = sched[0, step] * xs[step, :, columns] + sched[1, step] * guided

        @pl.when(step > 0)
        def _():
            x_half(xs, step, c, half, x_sem, other).wait_send()

        tile_loop(n_ada + step * n_step + LAYERS * n_block, n_head, head_body)
        swap = x_half(xs, later, c, half, x_sem, other)
        swap.start()
        swap.wait_recv()
        return carry

    lax.fori_loop(0, STEPS, one_step, 0)
    lat_out[...] = xs[0]

    for i in (K, V):
        relay(full[1][i], 1)
    for i in (K, V):
        first(full[1][i], 2)
    for i in (K, V):
        relay(full[1][i], 2)
    for b in range(LAYERS):
        for i in (K, V):
            settle(full[b][i], 2)
    x_half(xs, 0, c, half, x_sem, other).wait_send()
    for p in (K, V, Q):
        qkv_out(p, False)
    o_out(False)
    for t in range(n_out):
        chunk_swap(out_own, out_peer, t, out_send, out_recv).wait_send()
        chunk_swap(down_own, down_peer, t, down_send, down_recv).wait_send()
    for one in mod_copies:
        one.wait_send()
    for b in range(LAYERS):
        for ring in share[b] + full[b][K] + full[b][V]:
            for stage in ring:
                stage.drain()


def x_half(xs, at, c, half, x_sem, other):
    part = xs.at[at, :, pl.ds(pl.multiple_of(c * half, half), half)]
    return remote(part, part, x_sem.at[0], x_sem.at[1], cfg=other)


def denoise(lat, cond, sched, w_ada, w_qkv, w_out, w_up, w_down, w_head, k_old, v_old):
    rows, width = lat.shape
    group = width // RING
    hidden = w_up.shape[2] // 2
    torus = (RING, RING, RING)
    cache = jax.ShapeDtypeStruct((LAYERS, *torus, rows, width), BF16)
    k_old = k_old.reshape(cache.shape)
    v_old = v_old.reshape(cache.shape)
    w_out = w_out.reshape(LAYERS, width, width)
    n_out = width // WIDE
    anywhere = pl.BlockSpec(memory_space=pl.ANY)
    vmem = pl.BlockSpec(memory_space=pltpu.VMEM)
    dma = pltpu.SemaphoreType.DMA
    lat_out, all_k, all_v, _ = pl.pallas_call(
        denoise_kernel,
        out_shape=(
            jax.ShapeDtypeStruct((rows, width), F32),
            cache,
            cache,
            jax.ShapeDtypeStruct((LAYERS, 2, *torus, rows, group), BF16),
        ),
        in_specs=[vmem, vmem, pl.BlockSpec(memory_space=pltpu.SMEM)] + [anywhere] * 8,
        out_specs=[vmem, anywhere, anywhere, anywhere],
        scratch_shapes=[
            pltpu.VMEM((BUFFERS, width // 2, WIDE), BF16),
            pltpu.VMEM((*torus, rows, group), BF16),
            pltpu.VMEM((*torus, rows, group), BF16),
            pltpu.VMEM((STEPS, rows, width), F32),
            pltpu.VMEM((2 * rows, width), F32),
            pltpu.VMEM((2 * rows, width), BF16),
            pltpu.VMEM((2 * rows, hidden), BF16),
            pltpu.VMEM((2 * rows, width), F32),
            pltpu.VMEM((2 * rows, width), F32),
            pltpu.VMEM((2 * rows, width), F32),
            pltpu.VMEM((2 * rows, width), F32),
            pltpu.VMEM((2, 2, 3, rows, group), BF16),
            pltpu.VMEM((3, RING, rows, group), BF16),
            pltpu.VMEM((RING, rows, group), BF16),
            pltpu.VMEM((2, 2, rows, group), BF16),
            pltpu.VMEM((LAYERS, RING, RING, 2 * STEPS, 3 * width // 8), F32),
            pltpu.VMEM((STEPS, width), F32),
            pltpu.VMEM((RING * rows, RING**3 * rows), F32),
            dma((BUFFERS,)),
            dma((2,)),
            dma((2,)),
            dma((2 * RING - 1,)),
            dma((2 * RING - 1,)),
            dma((3, 2, 2)),
            dma((3, RING)),
            dma((RING,)),
            dma((2, 2)),
            dma((n_out,)),
            dma((n_out,)),
            dma((n_out,)),
            dma((n_out,)),
            dma((2,)),
            dma((2,)),
            dma((LAYERS, 2, 2, 2, 4)),
            dma((LAYERS, 2, 2, 2, 4)),
            dma((2, 2)),
            dma((2, 2)),
            dma((2, 2)),
            dma((LAYERS, 2, 3, 3, 4)),
            dma((LAYERS, 2, 3, 3, 4)),
        ],
        compiler_params=pltpu.CompilerParams(collective_id=0, has_side_effects=True, vmem_limit_bytes=63 * 2**20),
        name="denoise",
    )(lat, cond, sched, w_ada, w_qkv, w_out, w_up, w_down, w_head, k_old, v_old)
    tokens = RING**3 * rows
    return lat_out, all_k.reshape(LAYERS, tokens, width), all_v.reshape(LAYERS, tokens, width)


def solution(mesh):
    slot_spec = P(("img", "cfg"), None, None)
    cache_spec = P(("img", "cfg"), None, None, None)
    rep_spec = P()

    def local_step(latent, cond_vec, sched_coef, w_ada, w_qkv, w_out, w_up, w_down, w_head, k_stale, v_stale):
        lat_out, k_new, v_new = denoise(
            latent[0], cond_vec[0], sched_coef, w_ada, w_qkv, w_out, w_up, w_down, w_head, k_stale[0], v_stale[0]
        )
        return lat_out[None], k_new[None], v_new[None]

    return jax.shard_map(
        local_step,
        mesh=mesh,
        in_specs=(P("img", "patch", None), slot_spec, rep_spec, rep_spec, rep_spec, rep_spec, rep_spec, rep_spec, rep_spec, cache_spec, cache_spec),
        out_specs=(P(("img", "cfg"), "patch", None), cache_spec, cache_spec),
        check_vma=False,
    )
```

```python
import functools

import jax
import jax.numpy as jnp
from jax import lax
from jax.experimental import pallas as pl
from jax.experimental.pallas import tpu as pltpu
from jax.sharding import PartitionSpec as P

RING = 4
AXES = ("z", "y", "x")
COLOR_ORDERS = (("x", "y", "z"), ("y", "z", "x"), ("z", "x", "y"))
SHARE_ORDERS = (("y", "x"), ("x", "y"))
MESH = pl.DeviceIdType.MESH
F32 = jnp.float32
BF16 = jnp.bfloat16
HEAD = 128
TILE = 512
SUB = 256
WIDE = 2 * TILE
BUFFERS = 12
STEPS = 2
LAYERS = 2
Q, K, V = 0, 1, 2
KV = (K, V)


def dot(lhs, rhs):
    return jnp.dot(lhs, rhs, preferred_element_type=F32)


def scoped(name, action):
    def inside():
        with jax.named_scope(name):
            action()

    return inside


def torus_position():
    patch = lax.axis_index("patch")
    return {"z": lax.div(patch, RING * RING), "y": lax.rem(lax.div(patch, RING), RING), "x": lax.rem(patch, RING)}


def patch_at(pos):
    return (pos["z"] * RING + pos["y"]) * RING + pos["x"]


class Torus:
    def __init__(self):
        self.pos = torus_position()
        self.coord, self.patch = {}, {}
        for axis in AXES:
            for by in range(1, RING):
                coord = lax.rem(self.pos[axis] + by, RING)
                self.coord[axis, by] = coord
                self.patch[axis, by] = patch_at({**self.pos, axis: coord})


def remote(src, dst, send_sem, recv_sem, **device_id):
    return pltpu.make_async_remote_copy(
        src_ref=src, dst_ref=dst, send_sem=send_sem, recv_sem=recv_sem, device_id=device_id, device_id_type=MESH
    )


class Ring:
    def __init__(self, torus, axis, view, send_sem, recv_sem):
        me, succ, prev = torus.pos[axis], torus.coord[axis, 1], torus.coord[axis, RING - 1]
        ahead, behind = torus.patch[axis, 1], torus.patch[axis, RING - 1]
        self.sends = ((me, None, ahead), (me, None, behind), (prev, 0, ahead), (succ, 1, behind))
        self.parts = (view, send_sem, recv_sem)

    def copy(self, slot):
        view, send_sem, recv_sem = self.parts
        coord, half, patch = self.sends[slot]
        part = view(coord, half)
        return remote(part, part, send_sem(slot), recv_sem(slot), patch=patch)

    def first(self):
        for slot in (0, 1):
            self.copy(slot).start()

    def relay(self):
        for slot in (0, 1):
            self.copy(slot).wait_recv()
            self.copy(slot + 2).start()

    def settle(self):
        for slot in (2, 3):
            self.copy(slot).wait_recv()

    def drain(self):
        for slot in range(4):
            self.copy(slot).wait_send()


def full_rings(ref, color, torus, send_sem, recv_sem):
    width = ref.shape[4]
    cut = [0, width // 3 // SUB * SUB, width // 3 // SUB * SUB * 2, width]
    base, size = cut[color], cut[color + 1] - cut[color]
    order = COLOR_ORDERS[color]

    def stage(k):
        axis = order[k]

        def view(coord, half):
            index = []
            for name in AXES:
                index.append(coord if name == axis else slice(None) if name in order[:k] else torus.pos[name])
            columns = pl.ds(base, size) if half is None else pl.ds(base + half * (size // 2), size // 2)
            return ref.at[(*index, slice(None), columns)]

        return Ring(torus, axis, view, lambda slot: send_sem.at[k, slot], lambda slot: recv_sem.at[k, slot])

    return [stage(k) for k in range(3)]


def share_rings(ref, color, torus, send_sem, recv_sem):
    size = ref.shape[4] // 2
    order = SHARE_ORDERS[color]
    columns = pl.ds(color * size, size)

    def stage(k):
        axis = order[k]

        def view(coord, half):
            planes = slice(None) if half is None else pl.ds(half * (RING // 2), RING // 2)
            index = [coord if name == axis else slice(None) if name in order[:k] else torus.pos[name] for name in ("y", "x")]
            return ref.at[(planes, *index, slice(None), columns)]

        return Ring(torus, axis, view, lambda slot: send_sem.at[k, slot], lambda slot: recv_sem.at[k, slot])

    return [stage(k) for k in range(2)]


def denoise_kernel(
    lat, cond, sched, w_ada, w_qkv, w_out, w_up, w_down, w_head, k_old, v_old,
    lat_out, all_k, all_v, shared,
    wbuf, kbuf, vbuf, lat_own, cond_own, xs, r, h, act, out_own, out_peer, down_own, down_peer, sb, rb, o_sum, o_top, o_total, o_own, ob, mod,
    cond_peer, scores,
    w_sem, in_sem, kv_sem, cond_sem, mod_send, mod_recv, qkv_send, qkv_recv, o_send, o_recv, out_send, out_recv, down_send, down_recv,
    x_sem, share_put, share_send, share_recv, own_put, own_send, own_recv, full_send, full_recv,
):
    rows, width = lat.shape
    half = width // 2
    group = width // RING
    chunk = width // 8
    hidden = w_up.shape[2] // 2
    n_qkv = half // TILE
    n_out = width // WIDE
    n_up = hidden // TILE
    n_deep = hidden // half
    n_down = n_out * n_deep
    n_head = half // TILE
    n_block = 3 * n_qkv + n_out + n_up + n_down
    n_step = LAYERS * n_block + n_head
    n_ada = 3
    n_tiles = n_ada + STEPS * n_step
    n_buf = wbuf.shape[0]
    scale = HEAD**-0.5

    c = lax.axis_index("cfg")
    other = 1 - c
    torus = Torus()
    z, y, x = (torus.pos[axis] for axis in AXES)
    z_core = lax.div(z, 2)
    z_odd = lax.rem(z, 2)
    z_patch = [(v * RING + y) * RING + x for v in range(RING)]
    pair_patch = [((2 * c + g) * RING + y) * RING + x for g in range(2)]

    def put(src, dst, slot):
        pltpu.make_async_copy(src, dst, w_sem.at[slot]).start()

    def put_deep(ref, col, slot):
        col = pl.multiple_of(col, TILE)
        for k in range(2):
            put(ref.at[pl.ds(k * half, half), pl.ds(col, TILE)], wbuf.at[slot, :, pl.ds(k * TILE, TILE)], slot)

    def put_wide(ref, row, col, slot):
        row = pl.multiple_of(row, half)
        col = pl.multiple_of(col, WIDE)
        put(ref.at[pl.ds(row, half), pl.ds(col, WIDE)], wbuf.at[slot], slot)

    def issue_ada(i):
        col = pl.multiple_of(i * 2 * width + (y * RING + x) * chunk, chunk)
        for k in range(2):
            put(w_ada.at[c, pl.ds(k * half, half), pl.ds(col, chunk)], wbuf.at[i, :, pl.ds(k * chunk, chunk)], i)

    def issue(n):
        slot = lax.rem(n, n_buf)
        inside = lax.rem(n - n_ada, n_step)
        layer = lax.div(inside, n_block)
        u = lax.rem(inside, n_block)
        live = n < n_tiles
        block = live & (inside < LAYERS * n_block)
        at_out, at_up, at_down = 3 * n_qkv, 3 * n_qkv + n_out, 3 * n_qkv + n_out + n_up

        @pl.when(block & (u < at_out))
        def _():
            put_deep(w_qkv.at[layer], lax.div(u, n_qkv) * width + c * half + lax.rem(u, n_qkv) * TILE, slot)

        @pl.when(block & (u >= at_out) & (u < at_up))
        def _():
            put_wide(w_out.at[layer], c * half, (u - at_out) * WIDE, slot)

        @pl.when(block & (u >= at_up) & (u < at_down))
        def _():
            put_deep(w_up.at[layer], c * hidden + (u - at_up) * TILE, slot)

        @pl.when(block & (u >= at_down))
        def _():
            d = u - at_down
            put_wide(w_down.at[layer], c * hidden + lax.rem(d, n_deep) * half, lax.div(d, n_deep) * WIDE, slot)

        @pl.when(live & (inside >= LAYERS * n_block))
        def _():
            put_deep(w_head, c * half + (inside - LAYERS * n_block) * TILE, slot)

    def tile_loop(base, count, body, hooks=()):
        def one(t, carry):
            n = base + t
            slot = lax.rem(n, n_buf)
            tile = wbuf.at[slot]
            pltpu.make_async_copy(tile, tile, w_sem.at[slot]).wait()
            body(t, tile)
            issue(n + n_buf)
            for at, when, hook in hooks:
                pl.when((t == at) & when)(scoped("hook", hook))
            return carry

        lax.fori_loop(0, count, one, 0)

    def deep_dot(tile):
        return dot(h[:, :half], tile[:, :TILE]) + dot(h[:, half:], tile[:, TILE:])

    def load_kv(old_k, old_v):
        pltpu.make_async_copy(old_k, kbuf, kv_sem.at[0]).start()
        pltpu.make_async_copy(old_v, vbuf, kv_sem.at[1]).start()

    def load_stale(b):
        columns = pl.ds(pl.multiple_of(z * group, group), group)
        load_kv(k_old.at[b, :, :, :, :, columns], v_old.at[b, :, :, :, :, columns])

    def load_shared(b):
        load_kv(shared.at[b, 0], shared.at[b, 1])

    share = [
        [share_rings(shared.at[b, i], color, torus, share_send.at[b, i, color], share_recv.at[b, i, color]) for i in range(2) for color in range(2)]
        for b in range(LAYERS)
    ]
    full = [
        {
            p: [full_rings(ref.at[b], color, torus, full_send.at[b, p - K, color], full_recv.at[b, p - K, color]) for color in range(3)]
            for p, ref in ((K, all_k), (V, all_v))
        }
        for b in range(LAYERS)
    ]

    def first(rings, k):
        for ring in rings:
            if k:
                ring[k - 1].settle()
            ring[k].first()

    def relay(rings, k):
        for ring in rings:
            ring[k].relay()

    def settle(rings, k):
        for ring in rings:
            ring[k].settle()

    barrier = pltpu.get_barrier_semaphore()

    def announce(**device_id):
        pl.semaphore_signal(barrier, inc=1, device_id=device_id, device_id_type=MESH)

    announce(cfg=other)
    for by in range(1, RING):
        for core in range(2):
            announce(patch=torus.patch["z", by], cfg=core)
        announce(patch=torus.patch["y", by])
        announce(patch=torus.patch["x", by])
    cond_in = pltpu.make_async_copy(cond, cond_own, in_sem.at[0])
    cond_in.start()
    for i in range(n_ada):
        issue_ada(i)
    lat_in = pltpu.make_async_copy(lat, lat_own, in_sem.at[1])
    lat_in.start()
    cond_in.wait()
    with jax.named_scope("barrier"):
        pl.semaphore_wait(barrier, 1 + 4 * (RING - 1))

    cond_swap = remote(cond_own, cond_peer, cond_sem.at[0], cond_sem.at[1], cfg=other)
    cond_swap.start()
    lat_in.wait()
    xs[0] = lat_own[...].astype(F32)
    with jax.named_scope("cond_swap"):
        cond_swap.wait()
    mine, theirs = cond_own[...], cond_peer[...]
    both = jnp.concatenate([jnp.where(c == 0, mine, theirs), jnp.where(c == 0, theirs, mine)], axis=0)
    silu = (both * jax.nn.sigmoid(both)).astype(BF16)

    def mod_ring(i, axis):
        part, base = (mod.at[c, i, y, x], 0) if axis == "y" else (mod.at[c, i, :, x], RING - 1)
        return [
            remote(part, part, mod_send.at[i, base + by - 1], mod_recv.at[i, base + by - 1], patch=torus.patch[axis, by]) for by in range(1, RING)
        ]

    def mod_swap(i):
        return remote(mod.at[c, i], mod.at[c, i], mod_send.at[i, 2 * RING - 2], mod_recv.at[i, 2 * RING - 2], cfg=other)

    def mod_go(i, axis):
        for one in mod_ring(i, axis):
            one.start()

    def mod_wait(i, axis):
        for one in mod_ring(i, axis):
            one.wait_recv()

    for i in range(n_ada):
        with jax.named_scope("ada_wait"):
            filled = wbuf.at[i, :, pl.ds(0, 2 * chunk)]
            pltpu.make_async_copy(filled, filled, w_sem.at[i]).wait()
        if i == 0:
            for n in range(n_ada, n_buf):
                issue(jnp.int32(n))
            load_stale(0)
        tile = wbuf.at[i]
        mod[c, i, y, x] = dot(silu[:, :half], tile[:, :chunk]) + dot(silu[:, half:], tile[:, chunk : 2 * chunk])
        mod_go(i, "y")
        issue(jnp.int32(n_buf + i))
    with jax.named_scope("mod_y"):
        for i in range(n_ada):
            mod_wait(i, "y")
            mod_go(i, "x")
    with jax.named_scope("mod_x"):
        mod_wait(0, "x")
    mod_swap(0).start()
    with jax.named_scope("mod_swap"):
        mod_swap(0).wait_recv()

    def mod_rest():
        for i in range(1, n_ada):
            mod_wait(i, "x")
            mod_swap(i).start()
        for i in range(1, n_ada):
            mod_swap(i).wait_recv()

    def mod_row(b, step, which, i, s):
        at = which % 2 * 8 + i
        both = mod[b, which // 2, at // RING, at % RING, s * STEPS : (s + 1) * STEPS, :]
        return jnp.where(step == 0, both[0:1], both[1:2])

    def normed(s):
        values = r[s * rows : (s + 1) * rows, :]
        centered = values - jnp.mean(values, -1, keepdims=True)
        return centered * lax.rsqrt(jnp.mean(centered * centered, -1, keepdims=True) + 1e-6)

    def modulate(b, step, shift, gain):
        for s in range(2):
            values = normed(s)
            for i in range(8):
                at = slice(i * chunk, (i + 1) * chunk)
                part = values[:, at] * (1.0 + mod_row(b, step, gain, i, s)) + mod_row(b, step, shift, i, s)
                h[s * rows : (s + 1) * rows, at] = part.astype(BF16)

    def add_gated(b, step, gate, own, peer):
        for s in range(2):
            for i in range(8):
                at = (slice(s * rows, (s + 1) * rows), slice(i * chunk, (i + 1) * chunk))
                r[at] = r[at] + mod_row(b, step, gate, i, s) * (own[at] + peer[at])

    def chunk_swap(own, peer, t, send_sem, recv_sem):
        columns = pl.ds(pl.multiple_of(t * WIDE, WIDE), WIDE)
        return remote(own.at[:, columns], peer.at[:, columns], send_sem.at[t], recv_sem.at[t], cfg=other)

    def qkv_copy(p, s, g):
        return remote(sb.at[s, g, p], rb.at[p, z], qkv_send.at[p, s, g], qkv_recv.at[p, z], patch=pair_patch[g], cfg=s)

    def qkv_out(p, do_send):
        for s in range(2):
            for g in range(2):
                here = (2 * c + g == z) & (c == s)
                away = (2 * c + g != z) | (c != s)
                if do_send:

                    @pl.when(here)
                    def _():
                        rb[p, z] = sb[s, g, p]

                    @pl.when(away)
                    def _():
                        qkv_copy(p, s, g).start()
                else:

                    @pl.when(away)
                    def _():
                        qkv_copy(p, s, g).wait_send()

    def qkv_in(p):
        for src in range(RING):

            @pl.when((z != src) | (c != z_core))
            def _():
                part = rb.at[p, src]
                remote(part, part, qkv_send.at[p, 0, 0], qkv_recv.at[p, src], cfg=other).wait_recv()

    def qkv_part(p, base, hooks=()):
        def body(t, tile):
            part = deep_dot(tile).astype(BF16)
            for k in range(TILE // SUB):
                col = t * TILE + k * SUB
                g = lax.div(col, group)
                columns = pl.ds(pl.multiple_of(col - g * group, SUB), SUB)
                for s in range(2):
                    sb[s, g, p, :, columns] = part[s * rows : (s + 1) * rows, k * SUB : (k + 1) * SUB]

        tile_loop(base + p * n_qkv, n_qkv, body, hooks)
        qkv_out(p, True)

    def own_copies(b, p):
        local, swap = [], []
        for g in range(2):
            columns = pl.ds(pl.multiple_of(c * half + g * group, group), group)
            place = (all_k if p == K else all_v).at[b, z, y, x, :, columns]
            local.append(pltpu.make_async_copy(sb.at[c, g, p], place, own_put.at[p - K, g]))
            swap.append(remote(sb.at[other, g, p], place, own_send.at[p - K, g], own_recv.at[p - K, g], cfg=other))
        return local + swap

    def own_start(b, p):
        for one in own_copies(b, p):
            one.start()

    def own_wait(b, p):
        for one in own_copies(b, p):
            one.wait()

    def share_copy(b, p):
        return pltpu.make_async_copy(rb.at[p], shared.at[b, p - K, :, y, x], share_put.at[p - K])

    tokens_z = RING * RING * rows
    n_rows = RING * rows

    n_heads = group // HEAD

    def scored(queries, keys):
        return lax.dot_general(queries, keys, (((1,), (1,)), ((), ())), preferred_element_type=F32)

    def patch_of(shape, axis):
        index = lax.broadcasted_iota(jnp.int32, shape, axis)
        return lax.div(index, jnp.full_like(index, rows))

    def attend_cache(hooks):
        own_patch = patch_of((n_rows, tokens_z), 0) * (RING * RING) + y * RING + x
        key_patch = patch_of((n_rows, tokens_z), 1)

        def one(head, carry):
            at = pl.ds(pl.multiple_of(head * HEAD, HEAD), HEAD)
            queries = rb[Q, :, :, at].reshape(n_rows, HEAD)
            top = None
            for plane in range(RING):
                part = scored(queries, kbuf[plane, :, :, :, at].reshape(tokens_z, HEAD))
                part = jnp.where(key_patch + plane * RING * RING == own_patch, -jnp.inf, part)
                scores[:, plane * tokens_z : (plane + 1) * tokens_z] = part
                best = jnp.max(part, -1, keepdims=True)
                top = best if top is None else jnp.maximum(top, best)
            total = mixed = None
            for plane in range(RING):
                weights = jnp.exp((scores[:, plane * tokens_z : (plane + 1) * tokens_z] - top) * scale)
                add = jnp.sum(weights, -1, keepdims=True)
                more = dot(weights.astype(BF16), vbuf[plane, :, :, :, at].reshape(tokens_z, HEAD))
                total = add if total is None else total + add
                mixed = more if mixed is None else mixed + more
            o_sum[:, at] = mixed
            o_top[head] = jnp.broadcast_to(top, (n_rows, HEAD))
            o_total[head] = jnp.broadcast_to(total, (n_rows, HEAD))
            for when_at, when, hook in hooks:
                pl.when((head == when_at) & when)(scoped("hook", hook))
            return carry

        for i in range(2):
            buf = (kbuf, vbuf)[i]
            pltpu.make_async_copy(buf, buf, kv_sem.at[i]).wait()
        lax.fori_loop(0, n_heads, one, 0)

    def attend_fresh():
        same = patch_of((n_rows, n_rows), 0) == patch_of((n_rows, n_rows), 1)
        for head in range(n_heads):
            at = slice(head * HEAD, (head + 1) * HEAD)
            part = scored(rb[Q, :, :, at].reshape(n_rows, HEAD), rb[K, :, :, at].reshape(n_rows, HEAD))
            part = jnp.where(same, part, -jnp.inf)
            before = o_top[head]
            top = jnp.maximum(before, jnp.max(part, -1, keepdims=True))
            shrink = jnp.exp((before - top) * scale)
            weights = jnp.exp((part - top) * scale)
            total = o_total[head] * shrink + jnp.sum(weights, -1, keepdims=True)
            mixed = o_sum[:, at] * shrink + dot(weights.astype(BF16), rb[V, :, :, at].reshape(n_rows, HEAD))
            o_own[:, :, at] = (mixed / total).astype(BF16).reshape(RING, rows, HEAD)

    def o_copy(dst):
        return remote(o_own.at[dst], ob.at[c, z_odd], o_send.at[dst], o_recv.at[c, z_odd], patch=z_patch[dst], cfg=z_core)

    def o_out(do_send):
        for dst in range(RING):
            if do_send:

                @pl.when((z == dst) & (c == z_core))
                def _():
                    ob[c, z_odd] = o_own[dst]

            @pl.when((z != dst) | (c != z_core))
            def _():
                if do_send:
                    o_copy(dst).start()
                else:
                    o_copy(dst).wait_send()

    def o_in():
        for s in range(2):
            for g in range(2):

                @pl.when((2 * c + g != z) | (c != s))
                def _():
                    part = ob.at[s, g]
                    remote(part, part, o_send.at[0], o_recv.at[s, g], cfg=other).wait_recv()

    def block(step, b):
        base = n_ada + step * n_step + b * n_block
        begin = step == 0
        last = step == STEPS - 1

        def unless_first(action):
            if b:
                action()
            else:
                pl.when(step > 0)(action)

        def gather_own(p):
            own_wait(b, p)
            first(full[b][p], 0)

        if b == 0:
            for s in range(2):
                r[s * rows : (s + 1) * rows, :] = xs[step]
        with jax.named_scope("ln1"):
            modulate(b, step, 0, 1)

        @unless_first
        def _():
            for p in (Q, K, V):
                qkv_out(p, False)

        with jax.named_scope("qkv_q"):
            qkv_part(Q, base)
        with jax.named_scope("qkv_k"):
            qkv_part(K, base)

        @pl.when(last)
        def _():
            own_start(b, K)

        @pl.when(begin if b else last)
        def _():
            with jax.named_scope("relay_share"):
                relay(share[1 - b], 1)

        with jax.named_scope("qkv_v"):
            qkv_part(V, base, ((n_qkv - 1, last, lambda: gather_own(K)),))

        @pl.when(last)
        def _():
            own_start(b, V)
            if b:
                with jax.named_scope("full_1a"):
                    gather_own(V)
                    first(full[0][V], 2)
                    relay(full[1][K], 0)
                    relay(full[1][V], 0)

        with jax.named_scope("q_in"):
            qkv_in(Q)

        @unless_first
        def _():
            o_out(False)

        hooks = ()
        if b == 0:
            hooks = (
                (min(1, n_heads - 2), last, lambda: gather_own(V)),
                (max(n_heads - 2, 1), last, lambda: relay(full[0][K], 0)),
            )
        with jax.named_scope("attend_cache"):
            attend_cache(hooks)
        if b == 0:
            pl.when(begin)(lambda: load_stale(1))
        with jax.named_scope("kv_in"):
            for p in KV:
                qkv_in(p)

        @pl.when(begin)
        def _():
            for p in KV:
                share_copy(b, p).start()

        with jax.named_scope("attend_fresh"):
            attend_fresh()

        @pl.when(begin)
        def _():
            for p in KV:
                share_copy(b, p).wait()

        o_out(True)

        @pl.when(begin)
        def _():
            first(share[b], 0)
            if b == 0:
                with jax.named_scope("mod_rest"):
                    mod_rest()

        @pl.when(last)
        def _():
            with jax.named_scope("full_2"):
                if b == 0:
                    relay(full[0][V], 0)
                    first(full[0][K], 1)
                else:
                    relay(full[0][K], 2)
                    first(full[1][K], 1)
                    first(full[1][V], 1)
                    relay(full[0][V], 2)

        with jax.named_scope("o_in"):
            o_in()

        def out_body(t, tile):
            columns = pl.ds(pl.multiple_of(t * WIDE, WIDE), WIDE)
            part = [ob[:, g].reshape(2 * rows, group) for g in range(2)]
            out_own[:, columns] = dot(part[0], tile[:group]) + dot(part[1], tile[group:])
            chunk_swap(out_own, out_peer, t, out_send, out_recv).start()

        @unless_first
        def _():
            for t in range(n_out):
                chunk_swap(out_own, out_peer, t, out_send, out_recv).wait_send()

        with jax.named_scope("out"):
            tile_loop(base + 3 * n_qkv, n_out, out_body)
        if b == 0:

            @pl.when(last)
            def _():
                first(full[0][V], 1)

        with jax.named_scope("out_swap"):
            for t in range(n_out):
                chunk_swap(out_own, out_peer, t, out_send, out_recv).wait_recv()
        with jax.named_scope("ln2"):
            add_gated(b, step, 2, out_own, out_peer)
            modulate(b, step, 3, 4)

        def up_body(t, tile):
            act[:, pl.ds(pl.multiple_of(t * TILE, TILE), TILE)] = jax.nn.gelu(deep_dot(tile), approximate=True).astype(BF16)

        def refill(share_in, then):
            settle(share_in, 1)
            load_shared(1 - b)
            then()

        if b:
            hooks = (
                (1, begin, lambda: refill(share[0], lambda: relay(share[1], 0))),
                (n_up // 2, begin, lambda: first(share[1], 1)),
            )
        else:
            hooks = (
                (1, begin, lambda: relay(share[0], 0)),
                (n_up // 2, begin, lambda: first(share[0], 1)),
                (1, last, lambda: refill(share[1], lambda: None)),
                (n_up // 3, last, lambda: relay(full[0][K], 1)),
                (n_up - 1, last, lambda: relay(full[0][V], 1)),
            )
        with jax.named_scope("up"):
            tile_loop(base + 3 * n_qkv + n_out, n_up, up_body, hooks)

        def down_body(t, tile):
            n = lax.div(t, n_deep)
            deep = lax.rem(t, n_deep)
            columns = pl.ds(pl.multiple_of(n * WIDE, WIDE), WIDE)
            part = dot(act[:, pl.ds(pl.multiple_of(deep * half, half), half)], tile[...])

            @pl.when(deep == 0)
            def _():
                down_own[:, columns] = part

            @pl.when(deep != 0)
            def _():
                down_own[:, columns] = down_own[:, columns] + part

            @pl.when(deep == n_deep - 1)
            def _():
                chunk_swap(down_own, down_peer, n, down_send, down_recv).start()

        @unless_first
        def _():
            for t in range(n_out):
                chunk_swap(down_own, down_peer, t, down_send, down_recv).wait_send()

        hooks = () if b else ((n_down // 4, last, lambda: first(full[0][K], 2)),)
        with jax.named_scope("down"):
            tile_loop(base + 3 * n_qkv + n_out + n_up, n_down, down_body, hooks)
        with jax.named_scope("down_swap"):
            for t in range(n_out):
                chunk_swap(down_own, down_peer, t, down_send, down_recv).wait_recv()
        with jax.named_scope("gate2"):
            add_gated(b, step, 5, down_own, down_peer)
        if b:

            @pl.when(last)
            def _():
                with jax.named_scope("full_3"):
                    for p in KV:
                        relay(full[1][p], 1)


    def one_step(step, carry):
        for b in range(LAYERS):
            block(step, b)
        for s in range(2):
            h[s * rows : (s + 1) * rows, :] = normed(s).astype(BF16)
        later = lax.rem(step + 1, STEPS)

        def head_body(t, tile):
            eps = deep_dot(tile).astype(BF16).astype(F32)
            with_cond, without = eps[:rows], eps[rows:]
            guided = without + sched[step, 2] * (with_cond - without)
            columns = pl.ds(pl.multiple_of(c * half + t * TILE, TILE), TILE)
            xs[later, :, columns] = sched[step, 0] * xs[step, :, columns] + sched[step, 1] * guided

        @pl.when(step > 0)
        def _():
            x_half(xs, step, c, half, x_sem, other).wait_send()

        with jax.named_scope("head"):
            tile_loop(n_ada + step * n_step + LAYERS * n_block, n_head, head_body)
        swap = x_half(xs, later, c, half, x_sem, other)
        swap.start()
        with jax.named_scope("x_swap"):
            swap.wait_recv()
        return carry

    lax.fori_loop(0, STEPS, one_step, 0)
    lat_out[...] = xs[0]

    with jax.named_scope("tail_c1"):
        for p in KV:
            first(full[1][p], 2)
    with jax.named_scope("tail_c2k"):
        relay(full[1][K], 2)
    with jax.named_scope("tail_c2v"):
        relay(full[1][V], 2)
    with jax.named_scope("tail_end"):
        for b in range(LAYERS):
            for p in KV:
                settle(full[b][p], 2)
    x_half(xs, 0, c, half, x_sem, other).wait_send()
    for p in (Q, K, V):
        qkv_out(p, False)
    o_out(False)
    for t in range(n_out):
        chunk_swap(out_own, out_peer, t, out_send, out_recv).wait_send()
        chunk_swap(down_own, down_peer, t, down_send, down_recv).wait_send()
    for i in range(n_ada):
        for one in (*mod_ring(i, "y"), *mod_ring(i, "x"), mod_swap(i)):
            one.wait_send()
    for b in range(LAYERS):
        for ring in share[b] + full[b][K] + full[b][V]:
            for stage in ring:
                stage.drain()


def x_half(xs, at, c, half, x_sem, other):
    part = xs.at[at, :, pl.ds(pl.multiple_of(c * half, half), half)]
    return remote(part, part, x_sem.at[0], x_sem.at[1], cfg=other)


def denoise(lat, cond, sched, w_ada, w_qkv, w_out, w_up, w_down, w_head, k_old, v_old):
    rows, width = lat.shape
    group = width // RING
    hidden = w_up.shape[2] // 2
    torus = (RING, RING, RING)
    cache = jax.ShapeDtypeStruct((LAYERS, *torus, rows, width), BF16)
    k_old = k_old.reshape(cache.shape)
    v_old = v_old.reshape(cache.shape)
    w_out = w_out.reshape(LAYERS, width, width)
    n_out = width // WIDE
    anywhere = pl.BlockSpec(memory_space=pl.ANY)
    vmem = pl.BlockSpec(memory_space=pltpu.VMEM)
    dma = pltpu.SemaphoreType.DMA
    n_heads = group // HEAD
    n_ada = 3
    lat_out, all_k, all_v, _ = pl.pallas_call(
        denoise_kernel,
        out_shape=(
            jax.ShapeDtypeStruct((rows, width), F32),
            cache,
            cache,
            jax.ShapeDtypeStruct((LAYERS, 2, *torus, rows, group), BF16),
        ),
        in_specs=[anywhere, anywhere, pl.BlockSpec(memory_space=pltpu.SMEM)] + [anywhere] * 8,
        out_specs=[vmem, anywhere, anywhere, anywhere],
        scratch_shapes=[
            pltpu.VMEM((BUFFERS, width // 2, WIDE), BF16),
            pltpu.VMEM((*torus, rows, group), BF16),
            pltpu.VMEM((*torus, rows, group), BF16),
            pltpu.VMEM((rows, width), BF16),
            pltpu.VMEM((STEPS, width), F32),
            pltpu.VMEM((STEPS, rows, width), F32),
            pltpu.VMEM((2 * rows, width), F32),
            pltpu.VMEM((2 * rows, width), BF16),
            pltpu.VMEM((2 * rows, hidden), BF16),
            pltpu.VMEM((2 * rows, width), F32),
            pltpu.VMEM((2 * rows, width), F32),
            pltpu.VMEM((2 * rows, width), F32),
            pltpu.VMEM((2 * rows, width), F32),
            pltpu.VMEM((2, 2, 3, rows, group), BF16),
            pltpu.VMEM((3, RING, rows, group), BF16),
            pltpu.VMEM((RING * rows, group), F32),
            pltpu.VMEM((n_heads, RING * rows, HEAD), F32),
            pltpu.VMEM((n_heads, RING * rows, HEAD), F32),
            pltpu.VMEM((RING, rows, group), BF16),
            pltpu.VMEM((2, 2, rows, group), BF16),
            pltpu.VMEM((LAYERS, n_ada, RING, RING, 2 * STEPS, width // 8), F32),
            pltpu.VMEM((STEPS, width), F32),
            pltpu.VMEM((RING * rows, RING**3 * rows), F32),
            dma((BUFFERS,)),
            dma((2,)),
            dma((2,)),
            dma((2,)),
            dma((n_ada, 2 * RING - 1)),
            dma((n_ada, 2 * RING - 1)),
            dma((3, 2, 2)),
            dma((3, RING)),
            dma((RING,)),
            dma((2, 2)),
            dma((n_out,)),
            dma((n_out,)),
            dma((n_out,)),
            dma((n_out,)),
            dma((2,)),
            dma((2,)),
            dma((LAYERS, 2, 2, 2, 4)),
            dma((LAYERS, 2, 2, 2, 4)),
            dma((2, 2)),
            dma((2, 2)),
            dma((2, 2)),
            dma((LAYERS, 2, 3, 3, 4)),
            dma((LAYERS, 2, 3, 3, 4)),
        ],
        compiler_params=pltpu.CompilerParams(collective_id=0, has_side_effects=True, vmem_limit_bytes=63 * 2**20),
        name="denoise",
    )(lat, cond, sched.T, w_ada, w_qkv, w_out, w_up, w_down, w_head, k_old, v_old)
    tokens = RING**3 * rows
    return lat_out, all_k.reshape(LAYERS, tokens, width), all_v.reshape(LAYERS, tokens, width)


def solution(mesh):
    slot_spec = P(("img", "cfg"), None, None)
    cache_spec = P(("img", "cfg"), None, None, None)
    rep_spec = P()

    def local_step(latent, cond_vec, sched_coef, w_ada, w_qkv, w_out, w_up, w_down, w_head, k_stale, v_stale):
        lat_out, k_new, v_new = denoise(
            latent[0], cond_vec[0], sched_coef, w_ada, w_qkv, w_out, w_up, w_down, w_head, k_stale[0], v_stale[0]
        )
        return lat_out[None], k_new[None], v_new[None]

    return jax.shard_map(
        local_step,
        mesh=mesh,
        in_specs=(P("img", "patch", None), slot_spec, rep_spec, rep_spec, rep_spec, rep_spec, rep_spec, rep_spec, rep_spec, cache_spec, cache_spec),
        out_specs=(P(("img", "cfg"), "patch", None), cache_spec, cache_spec),
        check_vma=False,
    )
```

```python
import functools

import jax
import jax.numpy as jnp
from jax import lax
from jax.experimental import pallas as pl
from jax.experimental.pallas import tpu as pltpu
from jax.sharding import PartitionSpec as P

RING = 4
AXES = ("z", "y", "x")
COLOR_ORDERS = (("x", "y", "z"), ("y", "z", "x"), ("z", "x", "y"))
HEAD_AXES = ("z", "y")
MESH = pl.DeviceIdType.MESH
F32 = jnp.float32
BF16 = jnp.bfloat16
HEAD = 128
TILE = 512
SUB = 256
WIDE = 2 * TILE
BUFFERS = 12
STEPS = 2
LAYERS = 2
Q, K, V = 0, 1, 2
KV = (K, V)


def dot(lhs, rhs):
    return jnp.dot(lhs, rhs, preferred_element_type=F32)


def scoped(name, action):
    def inside():
        with jax.named_scope(name):
            action()

    return inside


def torus_position():
    patch = lax.axis_index("patch")
    return {"z": lax.div(patch, RING * RING), "y": lax.rem(lax.div(patch, RING), RING), "x": lax.rem(patch, RING)}


def patch_at(pos):
    return (pos["z"] * RING + pos["y"]) * RING + pos["x"]


class Torus:
    def __init__(self):
        self.pos = torus_position()
        self.coord, self.patch = {}, {}
        for axis in AXES:
            for by in range(1, RING):
                coord = lax.rem(self.pos[axis] + by, RING)
                self.coord[axis, by] = coord
                self.patch[axis, by] = patch_at({**self.pos, axis: coord})


def remote(src, dst, send_sem, recv_sem, **device_id):
    return pltpu.make_async_remote_copy(
        src_ref=src, dst_ref=dst, send_sem=send_sem, recv_sem=recv_sem, device_id=device_id, device_id_type=MESH
    )


class Ring:
    def __init__(self, torus, axis, view, send_sem, recv_sem):
        me, succ, prev = torus.pos[axis], torus.coord[axis, 1], torus.coord[axis, RING - 1]
        ahead, behind = torus.patch[axis, 1], torus.patch[axis, RING - 1]
        self.sends = ((me, None, ahead), (me, None, behind), (prev, 0, ahead), (succ, 1, behind))
        self.parts = (view, send_sem, recv_sem)

    def copy(self, slot):
        view, send_sem, recv_sem = self.parts
        coord, half, patch = self.sends[slot]
        part = view(coord, half)
        return remote(part, part, send_sem(slot), recv_sem(slot), patch=patch)

    def first(self):
        for slot in (0, 1):
            self.copy(slot).start()

    def relay(self):
        for slot in (0, 1):
            self.copy(slot).wait_recv()
            self.copy(slot + 2).start()

    def settle(self):
        for slot in (2, 3):
            self.copy(slot).wait_recv()

    def drain(self):
        for slot in range(4):
            self.copy(slot).wait_send()


def full_rings(ref, color, torus, send_sem, recv_sem):
    width = ref.shape[4]
    cut = [0, width // 3 // SUB * SUB, width // 3 // SUB * SUB * 2, width]
    base, size = cut[color], cut[color + 1] - cut[color]
    order = COLOR_ORDERS[color]

    def stage(k):
        axis = order[k]

        def view(coord, half):
            index = []
            for name in AXES:
                index.append(coord if name == axis else slice(None) if name in order[:k] else torus.pos[name])
            columns = pl.ds(base, size) if half is None else pl.ds(base + half * (size // 2), size // 2)
            return ref.at[(*index, slice(None), columns)]

        return Ring(torus, axis, view, lambda slot: send_sem.at[k, slot], lambda slot: recv_sem.at[k, slot])

    return [stage(k) for k in range(3)]


def share_rings(ref, head_axis, color, torus, send_sem, recv_sem):
    size = ref.shape[4] // 2
    rest = [axis for axis in AXES if axis != head_axis]
    order = rest if color else rest[::-1]
    columns = pl.ds(color * size, size)

    def stage(k):
        axis = order[k]

        def view(coord, half):
            index = []
            for name in AXES:
                if name == head_axis:
                    index.append(slice(None) if half is None else pl.ds(half * (RING // 2), RING // 2))
                else:
                    index.append(coord if name == axis else slice(None) if name in order[:k] else torus.pos[name])
            return ref.at[(*index, slice(None), columns)]

        return Ring(torus, axis, view, lambda slot: send_sem.at[k, slot], lambda slot: recv_sem.at[k, slot])

    return [stage(k) for k in range(2)]


def denoise_kernel(
    lat, cond, sched, w_ada, w_qkv, w_out, w_up, w_down, w_head, k_old, v_old,
    lat_out, all_k, all_v, shared,
    wbuf, kbuf, vbuf, lat_own, cond_own, xs, r, h, act, out_own, out_peer, down_own, down_peer, sb, rb, o_sum, o_top, o_total, o_own, ob, mod,
    cond_peer, scores,
    w_sem, in_sem, kv_sem, cond_sem, mod_send, mod_recv, qkv_send, qkv_recv, o_send, o_recv, out_send, out_recv, down_send, down_recv,
    x_sem, share_put, share_send, share_recv, own_put, own_send, own_recv, full_send, full_recv,
):
    rows, width = lat.shape
    half = width // 2
    group = width // RING
    chunk = width // 8
    hidden = w_up.shape[2] // 2
    n_qkv = half // TILE
    n_out = width // WIDE
    n_up = hidden // TILE
    n_deep = hidden // half
    n_down = n_out * n_deep
    n_head = half // TILE
    n_block = 3 * n_qkv + n_out + n_up + n_down
    n_step = LAYERS * n_block + n_head
    n_ada = 3
    n_tiles = n_ada + STEPS * n_step
    n_buf = wbuf.shape[0]
    scale = HEAD**-0.5

    c = lax.axis_index("cfg")
    other = 1 - c
    mod_block = other
    torus = Torus()
    z, y, x = (torus.pos[axis] for axis in AXES)
    line = [torus.pos[axis] for axis in HEAD_AXES]
    line_core = [lax.div(at, 2) for at in line]
    line_odd = [lax.rem(at, 2) for at in line]

    def line_patch(b, at):
        return patch_at({**torus.pos, HEAD_AXES[b]: at})

    def line_rows(ref, b):
        return ref.at[tuple(slice(None) if axis == HEAD_AXES[b] else torus.pos[axis] for axis in AXES)]


    def put(src, dst, slot):
        pltpu.make_async_copy(src, dst, w_sem.at[slot]).start()

    def put_deep(ref, col, slot):
        col = pl.multiple_of(col, TILE)
        for k in range(2):
            put(ref.at[pl.ds(k * half, half), pl.ds(col, TILE)], wbuf.at[slot, :, pl.ds(k * TILE, TILE)], slot)

    def put_wide(ref, row, col, slot):
        row = pl.multiple_of(row, half)
        col = pl.multiple_of(col, WIDE)
        put(ref.at[pl.ds(row, half), pl.ds(col, WIDE)], wbuf.at[slot], slot)

    def issue_ada(i):
        col = pl.multiple_of(i * 2 * width + (y * RING + x) * chunk, chunk)
        for k in range(2):
            put(w_ada.at[mod_block, pl.ds(k * half, half), pl.ds(col, chunk)], wbuf.at[i, :, pl.ds(k * chunk, chunk)], i)

    def issue(n):
        slot = lax.rem(n, n_buf)
        inside = lax.rem(n - n_ada, n_step)
        layer = lax.div(inside, n_block)
        u = lax.rem(inside, n_block)
        live = n < n_tiles
        block = live & (inside < LAYERS * n_block)
        at_out, at_up, at_down = 3 * n_qkv, 3 * n_qkv + n_out, 3 * n_qkv + n_out + n_up

        @pl.when(block & (u < at_out))
        def _():
            put_deep(w_qkv.at[layer], lax.div(u, n_qkv) * width + c * half + lax.rem(u, n_qkv) * TILE, slot)

        @pl.when(block & (u >= at_out) & (u < at_up))
        def _():
            put_wide(w_out.at[layer], c * half, (u - at_out) * WIDE, slot)

        @pl.when(block & (u >= at_up) & (u < at_down))
        def _():
            put_deep(w_up.at[layer], c * hidden + (u - at_up) * TILE, slot)

        @pl.when(block & (u >= at_down))
        def _():
            d = u - at_down
            put_wide(w_down.at[layer], c * hidden + lax.rem(d, n_deep) * half, lax.div(d, n_deep) * WIDE, slot)

        @pl.when(live & (inside >= LAYERS * n_block))
        def _():
            put_deep(w_head, c * half + (inside - LAYERS * n_block) * TILE, slot)

    def tile_loop(base, count, body, hooks=()):
        def one(t, carry):
            n = base + t
            slot = lax.rem(n, n_buf)
            tile = wbuf.at[slot]
            pltpu.make_async_copy(tile, tile, w_sem.at[slot]).wait()
            body(t, tile)
            issue(n + n_buf)
            for at, when, hook in hooks:
                pl.when((t == at) & when)(scoped("hook", hook))
            return carry

        lax.fori_loop(0, count, one, 0)

    def deep_dot(tile):
        return dot(h[:, :half], tile[:, :TILE]) + dot(h[:, half:], tile[:, TILE:])

    def load_kv(old_k, old_v):
        pltpu.make_async_copy(old_k, kbuf, kv_sem.at[0]).start()
        pltpu.make_async_copy(old_v, vbuf, kv_sem.at[1]).start()

    def load_stale(b):
        columns = pl.ds(pl.multiple_of(line[b] * group, group), group)
        load_kv(k_old.at[b, :, :, :, :, columns], v_old.at[b, :, :, :, :, columns])

    def load_shared(b):
        load_kv(shared.at[b, 0], shared.at[b, 1])

    share = [
        [share_rings(shared.at[b, i], HEAD_AXES[b], color, torus, share_send.at[b, i, color], share_recv.at[b, i, color]) for i in range(2) for color in range(2)]
        for b in range(LAYERS)
    ]
    full = [
        {
            p: [full_rings(ref.at[b], color, torus, full_send.at[b, p - K, color], full_recv.at[b, p - K, color]) for color in (2, 1, 0)]
            for p, ref in ((K, all_k), (V, all_v))
        }
        for b in range(LAYERS)
    ]

    def first(rings, k):
        for ring in rings:
            if k:
                ring[k - 1].settle()
            ring[k].first()

    def relay(rings, k):
        for ring in rings:
            ring[k].relay()

    def settle(rings, k):
        for ring in rings:
            ring[k].settle()

    barrier = pltpu.get_barrier_semaphore()

    def announce(**device_id):
        pl.semaphore_signal(barrier, inc=1, device_id=device_id, device_id_type=MESH)

    announce(cfg=other)
    for by in range(1, RING):
        for axis in HEAD_AXES:
            for core in range(2):
                announce(patch=torus.patch[axis, by], cfg=core)
        announce(patch=torus.patch["x", by])
    cond_in = pltpu.make_async_copy(cond, cond_own, in_sem.at[0])
    cond_in.start()
    for i in range(n_ada):
        issue_ada(i)
    lat_in = pltpu.make_async_copy(lat, lat_own, in_sem.at[1])
    lat_in.start()
    cond_in.wait()
    with jax.named_scope("barrier"):
        pl.semaphore_wait(barrier, 1 + 5 * (RING - 1))

    cond_swap = remote(cond_own, cond_peer, cond_sem.at[0], cond_sem.at[1], cfg=other)
    cond_swap.start()
    lat_in.wait()
    xs[0] = lat_own[...].astype(F32)
    with jax.named_scope("cond_swap"):
        cond_swap.wait()
    mine, theirs = cond_own[...], cond_peer[...]
    both = jnp.concatenate([jnp.where(c == 0, mine, theirs), jnp.where(c == 0, theirs, mine)], axis=0)
    silu = (both * jax.nn.sigmoid(both)).astype(BF16)

    def mod_ring(i, axis):
        part, base = (mod.at[mod_block, i, y, x], 0) if axis == "y" else (mod.at[mod_block, i, :, x], RING - 1)
        return [
            remote(part, part, mod_send.at[i, base + by - 1], mod_recv.at[i, base + by - 1], patch=torus.patch[axis, by]) for by in range(1, RING)
        ]

    def mod_swap(i):
        return remote(mod.at[mod_block, i], mod.at[mod_block, i], mod_send.at[i, 2 * RING - 2], mod_recv.at[i, 2 * RING - 2], cfg=other)

    def mod_go(i, axis):
        for one in mod_ring(i, axis):
            one.start()

    def mod_wait(i, axis):
        for one in mod_ring(i, axis):
            one.wait_recv()

    for i in range(n_ada):
        with jax.named_scope("ada_wait"):
            filled = wbuf.at[i, :, pl.ds(0, 2 * chunk)]
            pltpu.make_async_copy(filled, filled, w_sem.at[i]).wait()
        if i == 0:
            for n in range(n_ada, n_buf):
                issue(jnp.int32(n))
            load_stale(0)
        tile = wbuf.at[i]
        mod[mod_block, i, y, x] = dot(silu[:, :half], tile[:, :chunk]) + dot(silu[:, half:], tile[:, chunk : 2 * chunk])
        mod_go(i, "y")
        issue(jnp.int32(n_buf + i))
    with jax.named_scope("mod_y"):
        for i in range(n_ada):
            mod_wait(i, "y")
            mod_go(i, "x")
    with jax.named_scope("mod_x"):
        mod_wait(0, "x")
    mod_swap(0).start()
    with jax.named_scope("mod_swap"):
        mod_swap(0).wait_recv()

    def mod_rest():
        for i in range(1, n_ada):
            mod_wait(i, "x")
            mod_swap(i).start()
        for i in range(1, n_ada):
            mod_swap(i).wait_recv()

    def mod_row(b, step, which, i, s):
        at = which % 2 * 8 + i
        both = mod[b, which // 2, at // RING, at % RING, s * STEPS : (s + 1) * STEPS, :]
        return jnp.where(step == 0, both[0:1], both[1:2])

    def normed(s):
        values = r[s * rows : (s + 1) * rows, :]
        centered = values - jnp.mean(values, -1, keepdims=True)
        return centered * lax.rsqrt(jnp.mean(centered * centered, -1, keepdims=True) + 1e-6)

    def modulate(b, step, shift, gain):
        for s in range(2):
            values = normed(s)
            for i in range(8):
                at = slice(i * chunk, (i + 1) * chunk)
                part = values[:, at] * (1.0 + mod_row(b, step, gain, i, s)) + mod_row(b, step, shift, i, s)
                h[s * rows : (s + 1) * rows, at] = part.astype(BF16)

    def add_gated(b, step, gate, own, peer):
        for s in range(2):
            for i in range(8):
                at = (slice(s * rows, (s + 1) * rows), slice(i * chunk, (i + 1) * chunk))
                r[at] = r[at] + mod_row(b, step, gate, i, s) * (own[at] + peer[at])

    def chunk_swap(own, peer, t, send_sem, recv_sem):
        columns = pl.ds(pl.multiple_of(t * WIDE, WIDE), WIDE)
        return remote(own.at[:, columns], peer.at[:, columns], send_sem.at[t], recv_sem.at[t], cfg=other)

    def qkv_copy(b, p, s, g):
        return remote(sb.at[s, g, p], rb.at[b, p, line[b]], qkv_send.at[p, s, g], qkv_recv.at[b, p, line[b]], patch=line_patch(b, 2 * c + g), cfg=s)

    def qkv_out(b, p, do_send):
        for s in range(2):
            for g in range(2):
                if do_send:

                    @pl.when((2 * c + g == line[b]) & (c == s))
                    def _():
                        rb[b, p, line[b]] = sb[s, g, p]

                @pl.when((2 * c + g != line[b]) | (c != s))
                def _():
                    if do_send:
                        qkv_copy(b, p, s, g).start()
                    else:
                        qkv_copy(b, p, s, g).wait_send()

    def qkv_in(b, p):
        for src in range(RING):

            @pl.when((line[b] != src) | (c != line_core[b]))
            def _():
                part = rb.at[b, p, src]
                remote(part, part, qkv_send.at[p, 0, 0], qkv_recv.at[b, p, src], cfg=other).wait_recv()

    def qkv_part(p, base, hooks=()):
        def body(t, tile):
            part = deep_dot(tile).astype(BF16)
            for k in range(TILE // SUB):
                col = t * TILE + k * SUB
                g = lax.div(col, group)
                columns = pl.ds(pl.multiple_of(col - g * group, SUB), SUB)
                for s in range(2):
                    sb[s, g, p, :, columns] = part[s * rows : (s + 1) * rows, k * SUB : (k + 1) * SUB]

        tile_loop(base + p * n_qkv, n_qkv, body, hooks)

    def own_copies(b, p):
        local, swap = [], []
        for g in range(2):
            columns = pl.ds(pl.multiple_of(c * half + g * group, group), group)
            place = (all_k if p == K else all_v).at[b, z, y, x, :, columns]
            local.append(pltpu.make_async_copy(sb.at[c, g, p], place, own_put.at[p - K, g]))
            swap.append(remote(sb.at[other, g, p], place, own_send.at[p - K, g], own_recv.at[p - K, g], cfg=other))
        return local + swap

    def own_start(b, p):
        for one in own_copies(b, p):
            one.start()

    def own_wait(b, p):
        for one in own_copies(b, p):
            one.wait()

    def share_copy(b, p):
        return pltpu.make_async_copy(rb.at[b, p], line_rows(shared.at[b, p - K], b), share_put.at[p - K])

    tokens_z = RING * RING * rows
    n_rows = RING * rows

    n_heads = group // HEAD

    def scored(queries, keys):
        return lax.dot_general(queries, keys, (((1,), (1,)), ((), ())), preferred_element_type=F32)

    def patch_of(shape, axis):
        index = lax.broadcasted_iota(jnp.int32, shape, axis)
        return lax.div(index, jnp.full_like(index, rows))

    def attend_cache(b, hooks):
        own_patch = line_patch(b, patch_of((n_rows, tokens_z), 0))
        key_patch = patch_of((n_rows, tokens_z), 1)

        together = 2

        def one(step, carry):
            heads = [step * together + j for j in range(together)]
            columns = [pl.ds(pl.multiple_of(head * HEAD, HEAD), HEAD) for head in heads]
            queries = [rb[b, Q, :, :, at].reshape(n_rows, HEAD) for at in columns]
            tops, totals, mixed = [None] * together, [None] * together, [None] * together
            for plane in range(RING):
                planes = slice(plane * tokens_z, (plane + 1) * tokens_z)
                hidden_keys = key_patch + plane * RING * RING == own_patch
                for j, at in enumerate(columns):
                    part = scored(queries[j], kbuf[plane, :, :, :, at].reshape(tokens_z, HEAD))
                    part = jnp.where(hidden_keys, -jnp.inf, part)
                    scores[j, :, planes] = part
                    best = jnp.max(part, -1, keepdims=True)
                    tops[j] = best if plane == 0 else jnp.maximum(tops[j], best)
            for plane in range(RING):
                planes = slice(plane * tokens_z, (plane + 1) * tokens_z)
                for j, at in enumerate(columns):
                    weights = jnp.exp((scores[j, :, planes] - tops[j]) * scale)
                    add = jnp.sum(weights, -1, keepdims=True)
                    more = dot(weights.astype(BF16), vbuf[plane, :, :, :, at].reshape(tokens_z, HEAD))
                    totals[j] = add if plane == 0 else totals[j] + add
                    mixed[j] = more if plane == 0 else mixed[j] + more
            for j, (head, at) in enumerate(zip(heads, columns)):
                o_sum[:, at] = mixed[j]
                o_top[head] = jnp.broadcast_to(tops[j], (n_rows, HEAD))
                o_total[head] = jnp.broadcast_to(totals[j], (n_rows, HEAD))
            for when_at, when, hook in hooks:
                pl.when((step == when_at // together) & when)(scoped("hook", hook))
            return carry

        for i in range(2):
            buf = (kbuf, vbuf)[i]
            pltpu.make_async_copy(buf, buf, kv_sem.at[i]).wait()
        lax.fori_loop(0, n_heads // together, one, 0)

    def attend_fresh(b):
        same = patch_of((n_rows, n_rows), 0) == patch_of((n_rows, n_rows), 1)
        for start in range(0, n_heads, 3):
            heads = range(start, min(start + 3, n_heads))
            columns = [slice(head * HEAD, (head + 1) * HEAD) for head in heads]
            parts = [scored(rb[b, Q, :, :, at].reshape(n_rows, HEAD), rb[b, K, :, :, at].reshape(n_rows, HEAD)) for at in columns]
            parts = [jnp.where(same, part, -jnp.inf) for part in parts]
            tops = [jnp.maximum(o_top[head], jnp.max(part, -1, keepdims=True)) for head, part in zip(heads, parts)]
            weights = [jnp.exp((part - top) * scale) for part, top in zip(parts, tops)]
            fresh = [dot(weight.astype(BF16), rb[b, V, :, :, at].reshape(n_rows, HEAD)) for weight, at in zip(weights, columns)]
            shrink = [jnp.exp((o_top[head] - top) * scale) for head, top in zip(heads, tops)]
            totals = [o_total[head] * less + jnp.sum(weight, -1, keepdims=True) for head, less, weight in zip(heads, shrink, weights)]
            for at, less, more, total in zip(columns, shrink, fresh, totals):
                o_own[:, :, at] = ((o_sum[:, at] * less + more) / total).astype(BF16).reshape(RING, rows, HEAD)

    def o_copy(b, dst):
        return remote(
            o_own.at[dst], ob.at[c, line_odd[b]], o_send.at[dst], o_recv.at[c, line_odd[b]], patch=line_patch(b, dst), cfg=line_core[b]
        )

    def o_out(b, do_send):
        for dst in range(RING):
            if do_send:

                @pl.when((line[b] == dst) & (c == line_core[b]))
                def _():
                    ob[c, line_odd[b]] = o_own[dst]

            @pl.when((line[b] != dst) | (c != line_core[b]))
            def _():
                if do_send:
                    o_copy(b, dst).start()
                else:
                    o_copy(b, dst).wait_send()

    def o_in(b):
        for s in range(2):
            for g in range(2):

                @pl.when((2 * c + g != line[b]) | (c != s))
                def _():
                    part = ob.at[s, g]
                    remote(part, part, o_send.at[0], o_recv.at[s, g], cfg=other).wait_recv()

    def block(step, b):
        base = n_ada + step * n_step + b * n_block
        begin = step == 0
        last = step == STEPS - 1

        def unless_first(action):
            if b:
                action()
            else:
                pl.when(step > 0)(action)

        def gather_own(p):
            own_wait(b, p)
            first(full[b][p], 0)

        def send_late():
            gather_own(V)
            for p in KV:
                qkv_out(b, p, True)

        if b == 0:
            for s in range(2):
                r[s * rows : (s + 1) * rows, :] = xs[step]
        with jax.named_scope("ln1"):
            modulate(b, step, 0, 1)

        @unless_first
        def _():
            for p in (Q, K, V):
                qkv_out(1 - b, p, False)

        with jax.named_scope("qkv_q"):
            qkv_part(Q, base)
        qkv_out(b, Q, True)
        with jax.named_scope("qkv_k"):
            qkv_part(K, base)
        pl.when(begin)(lambda: qkv_out(b, K, True))

        @pl.when(last)
        def _():
            own_start(b, K)
            if b == 0:
                with jax.named_scope("relay_share"):
                    relay(share[1], 1)

        with jax.named_scope("qkv_v"):
            qkv_part(V, base, ((n_qkv - 1, last, lambda: gather_own(K)),))

        pl.when(begin)(lambda: qkv_out(b, V, True))

        @pl.when(last)
        def _():
            own_start(b, V)
            if b:
                with jax.named_scope("full_1a"):
                    send_late()
                    first(full[0][V], 2)
                    relay(full[1][K], 0)
                    relay(full[1][V], 0)

        with jax.named_scope("q_in"):
            qkv_in(b, Q)

        @unless_first
        def _():
            o_out(1 - b, False)

        if b:
            hooks = ((n_heads // 2, begin, lambda: relay(share[0], 1)),)
        else:
            hooks = (
                (min(1, n_heads - 2), last, send_late),
                (max(n_heads - 2, 1), last, lambda: relay(full[0][K], 0)),
            )
        with jax.named_scope("attend_cache"):
            attend_cache(b, hooks)
        if b == 0:
            pl.when(begin)(lambda: load_stale(1))
        with jax.named_scope("kv_in"):
            for p in KV:
                qkv_in(b, p)

        @pl.when(begin)
        def _():
            for p in KV:
                share_copy(b, p).start()

        with jax.named_scope("attend_fresh"):
            attend_fresh(b)

        @pl.when(begin)
        def _():
            for p in KV:
                share_copy(b, p).wait()

        o_out(b, True)

        @pl.when(begin)
        def _():
            first(share[b], 0)
            if b == 0:
                with jax.named_scope("mod_rest"):
                    mod_rest()

        @pl.when(last)
        def _():
            with jax.named_scope("full_2"):
                if b == 0:
                    relay(full[0][V], 0)
                    first(full[0][K], 1)
                else:
                    relay(full[0][K], 2)
                    first(full[1][K], 1)
                    first(full[1][V], 1)
                    relay(full[0][V], 2)

        with jax.named_scope("o_in"):
            o_in(b)

        def out_body(t, tile):
            columns = pl.ds(pl.multiple_of(t * WIDE, WIDE), WIDE)
            part = [ob[:, g].reshape(2 * rows, group) for g in range(2)]
            out_own[:, columns] = dot(part[0], tile[:group]) + dot(part[1], tile[group:])
            chunk_swap(out_own, out_peer, t, out_send, out_recv).start()

        @unless_first
        def _():
            for t in range(n_out):
                chunk_swap(out_own, out_peer, t, out_send, out_recv).wait_send()

        with jax.named_scope("out"):
            tile_loop(base + 3 * n_qkv, n_out, out_body)
        if b == 0:

            @pl.when(last)
            def _():
                first(full[0][V], 1)

        with jax.named_scope("out_swap"):
            for t in range(n_out):
                chunk_swap(out_own, out_peer, t, out_send, out_recv).wait_recv()
        with jax.named_scope("ln2"):
            add_gated(b, step, 2, out_own, out_peer)
            modulate(b, step, 3, 4)

        def up_body(t, tile):
            act[:, pl.ds(pl.multiple_of(t * TILE, TILE), TILE)] = jax.nn.gelu(deep_dot(tile), approximate=True).astype(BF16)

        def refill(share_in, then):
            settle(share_in, 1)
            load_shared(1 - b)
            then()

        if b:
            hooks = (
                (n_up // 4, begin, lambda: refill(share[0], lambda: relay(share[1], 0))),
                (n_up * 2 // 3, begin, lambda: first(share[1], 1)),
            )
        else:
            hooks = (
                (n_up // 4, begin, lambda: relay(share[0], 0)),
                (n_up * 2 // 3, begin, lambda: first(share[0], 1)),
                (1, last, lambda: refill(share[1], lambda: None)),
                (n_up // 6, last, lambda: relay(full[0][K], 1)),
                (n_up * 3 // 4, last, lambda: relay(full[0][V], 1)),
            )
        with jax.named_scope("up"):
            tile_loop(base + 3 * n_qkv + n_out, n_up, up_body, hooks)

        def down_body(t, tile):
            n = lax.div(t, n_deep)
            deep = lax.rem(t, n_deep)
            columns = pl.ds(pl.multiple_of(n * WIDE, WIDE), WIDE)
            part = dot(act[:, pl.ds(pl.multiple_of(deep * half, half), half)], tile[...])

            @pl.when(deep == 0)
            def _():
                down_own[:, columns] = part

            @pl.when(deep != 0)
            def _():
                down_own[:, columns] = down_own[:, columns] + part

            @pl.when(deep == n_deep - 1)
            def _():
                chunk_swap(down_own, down_peer, n, down_send, down_recv).start()

        @unless_first
        def _():
            for t in range(n_out):
                chunk_swap(down_own, down_peer, t, down_send, down_recv).wait_send()

        hooks = () if b else ((n_down // 12, last, lambda: first(full[0][K], 2)),)
        with jax.named_scope("down"):
            tile_loop(base + 3 * n_qkv + n_out + n_up, n_down, down_body, hooks)
        with jax.named_scope("down_swap"):
            for t in range(n_out):
                chunk_swap(down_own, down_peer, t, down_send, down_recv).wait_recv()
        with jax.named_scope("gate2"):
            add_gated(b, step, 5, down_own, down_peer)
        if b:

            @pl.when(last)
            def _():
                with jax.named_scope("full_3"):
                    for p in KV:
                        relay(full[1][p], 1)


    def one_step(step, carry):
        for b in range(LAYERS):
            block(step, b)
        for s in range(2):
            h[s * rows : (s + 1) * rows, :] = normed(s).astype(BF16)
        later = lax.rem(step + 1, STEPS)

        def head_body(t, tile):
            eps = deep_dot(tile).astype(BF16).astype(F32)
            with_cond, without = eps[:rows], eps[rows:]
            guided = without + sched[step, 2] * (with_cond - without)
            columns = pl.ds(pl.multiple_of(c * half + t * TILE, TILE), TILE)
            xs[later, :, columns] = sched[step, 0] * xs[step, :, columns] + sched[step, 1] * guided

        @pl.when(step > 0)
        def _():
            x_half(xs, step, c, half, x_sem, other).wait_send()

        with jax.named_scope("head"):
            tile_loop(n_ada + step * n_step + LAYERS * n_block, n_head, head_body)
        swap = x_half(xs, later, c, half, x_sem, other)
        swap.start()
        with jax.named_scope("x_swap"):
            swap.wait_recv()
        return carry

    lax.fori_loop(0, STEPS, one_step, 0)
    lat_out[...] = xs[0]

    with jax.named_scope("tail_c1"):
        for p in KV:
            first(full[1][p], 2)
    with jax.named_scope("tail_c2k"):
        relay(full[1][K], 2)
    with jax.named_scope("tail_c2v"):
        relay(full[1][V], 2)
    with jax.named_scope("tail_end"):
        for b in range(LAYERS):
            for p in KV:
                settle(full[b][p], 2)
    x_half(xs, 0, c, half, x_sem, other).wait_send()
    for p in (Q, K, V):
        qkv_out(LAYERS - 1, p, False)
    o_out(LAYERS - 1, False)
    for t in range(n_out):
        chunk_swap(out_own, out_peer, t, out_send, out_recv).wait_send()
        chunk_swap(down_own, down_peer, t, down_send, down_recv).wait_send()
    for i in range(n_ada):
        for one in (*mod_ring(i, "y"), *mod_ring(i, "x"), mod_swap(i)):
            one.wait_send()
    for b in range(LAYERS):
        for ring in share[b] + full[b][K] + full[b][V]:
            for stage in ring:
                stage.drain()


def x_half(xs, at, c, half, x_sem, other):
    part = xs.at[at, :, pl.ds(pl.multiple_of(c * half, half), half)]
    return remote(part, part, x_sem.at[0], x_sem.at[1], cfg=other)


def denoise(lat, cond, sched, w_ada, w_qkv, w_out, w_up, w_down, w_head, k_old, v_old):
    rows, width = lat.shape
    group = width // RING
    hidden = w_up.shape[2] // 2
    torus = (RING, RING, RING)
    cache = jax.ShapeDtypeStruct((LAYERS, *torus, rows, width), BF16)
    k_old = k_old.reshape(cache.shape)
    v_old = v_old.reshape(cache.shape)
    w_out = w_out.reshape(LAYERS, width, width)
    n_out = width // WIDE
    anywhere = pl.BlockSpec(memory_space=pl.ANY)
    vmem = pl.BlockSpec(memory_space=pltpu.VMEM)
    dma = pltpu.SemaphoreType.DMA
    n_heads = group // HEAD
    n_ada = 3
    lat_out, all_k, all_v, _ = pl.pallas_call(
        denoise_kernel,
        out_shape=(
            jax.ShapeDtypeStruct((rows, width), F32),
            cache,
            cache,
            jax.ShapeDtypeStruct((LAYERS, 2, *torus, rows, group), BF16),
        ),
        in_specs=[anywhere, anywhere, pl.BlockSpec(memory_space=pltpu.SMEM)] + [anywhere] * 8,
        out_specs=[vmem, anywhere, anywhere, anywhere],
        scratch_shapes=[
            pltpu.VMEM((BUFFERS, width // 2, WIDE), BF16),
            pltpu.VMEM((*torus, rows, group), BF16),
            pltpu.VMEM((*torus, rows, group), BF16),
            pltpu.VMEM((rows, width), BF16),
            pltpu.VMEM((STEPS, width), F32),
            pltpu.VMEM((STEPS, rows, width), F32),
            pltpu.VMEM((2 * rows, width), F32),
            pltpu.VMEM((2 * rows, width), BF16),
            pltpu.VMEM((2 * rows, hidden), BF16),
            pltpu.VMEM((2 * rows, width), F32),
            pltpu.VMEM((2 * rows, width), F32),
            pltpu.VMEM((2 * rows, width), F32),
            pltpu.VMEM((2 * rows, width), F32),
            pltpu.VMEM((2, 2, 3, rows, group), BF16),
            pltpu.VMEM((LAYERS, 3, RING, rows, group), BF16),
            pltpu.VMEM((RING * rows, group), F32),
            pltpu.VMEM((n_heads, RING * rows, HEAD), F32),
            pltpu.VMEM((n_heads, RING * rows, HEAD), F32),
            pltpu.VMEM((RING, rows, group), BF16),
            pltpu.VMEM((2, 2, rows, group), BF16),
            pltpu.VMEM((LAYERS, n_ada, RING, RING, 2 * STEPS, width // 8), F32),
            pltpu.VMEM((STEPS, width), F32),
            pltpu.VMEM((2, RING * rows, RING**3 * rows), F32),
            dma((BUFFERS,)),
            dma((2,)),
            dma((2,)),
            dma((2,)),
            dma((n_ada, 2 * RING - 1)),
            dma((n_ada, 2 * RING - 1)),
            dma((3, 2, 2)),
            dma((LAYERS, 3, RING)),
            dma((RING,)),
            dma((2, 2)),
            dma((n_out,)),
            dma((n_out,)),
            dma((n_out,)),
            dma((n_out,)),
            dma((2,)),
            dma((2,)),
            dma((LAYERS, 2, 2, 2, 4)),
            dma((LAYERS, 2, 2, 2, 4)),
            dma((2, 2)),
            dma((2, 2)),
            dma((2, 2)),
            dma((LAYERS, 2, 3, 3, 4)),
            dma((LAYERS, 2, 3, 3, 4)),
        ],
        compiler_params=pltpu.CompilerParams(collective_id=0, has_side_effects=True, vmem_limit_bytes=63 * 2**20),
        name="denoise",
    )(lat, cond, sched.T, w_ada, w_qkv, w_out, w_up, w_down, w_head, k_old, v_old)
    tokens = RING**3 * rows
    return lat_out, all_k.reshape(LAYERS, tokens, width), all_v.reshape(LAYERS, tokens, width)


def solution(mesh):
    slot_spec = P(("img", "cfg"), None, None)
    cache_spec = P(("img", "cfg"), None, None, None)
    rep_spec = P()

    def local_step(latent, cond_vec, sched_coef, w_ada, w_qkv, w_out, w_up, w_down, w_head, k_stale, v_stale):
        lat_out, k_new, v_new = denoise(
            latent[0], cond_vec[0], sched_coef, w_ada, w_qkv, w_out, w_up, w_down, w_head, k_stale[0], v_stale[0]
        )
        return lat_out[None], k_new[None], v_new[None]

    return jax.shard_map(
        local_step,
        mesh=mesh,
        in_specs=(P("img", "patch", None), slot_spec, rep_spec, rep_spec, rep_spec, rep_spec, rep_spec, rep_spec, rep_spec, cache_spec, cache_spec),
        out_specs=(P(("img", "cfg"), "patch", None), cache_spec, cache_spec),
        check_vma=False,
    )
```

```python
import functools

import jax
import jax.numpy as jnp
from jax import lax
from jax.experimental import pallas as pl
from jax.experimental.pallas import tpu as pltpu
from jax.sharding import PartitionSpec as P

RING = 4
AXES = ("z", "y", "x")
COLOR_ORDERS = (("x", "y", "z"), ("y", "z", "x"), ("z", "x", "y"))
HEAD_AXES = ("z", "y")
MESH = pl.DeviceIdType.MESH
F32 = jnp.float32
BF16 = jnp.bfloat16
HEAD = 128
TILE = 512
SUB = 256
WIDE = 2 * TILE
BUFFERS = 12
STEPS = 2
LAYERS = 2
Q, K, V = 0, 1, 2
KV = (K, V)


def dot(lhs, rhs):
    return jnp.dot(lhs, rhs, preferred_element_type=F32)


def scoped(name, action):
    def inside():
        with jax.named_scope(name):
            action()

    return inside


def torus_position():
    patch = lax.axis_index("patch")
    return {"z": lax.div(patch, RING * RING), "y": lax.rem(lax.div(patch, RING), RING), "x": lax.rem(patch, RING)}


def patch_at(pos):
    return (pos["z"] * RING + pos["y"]) * RING + pos["x"]


class Torus:
    def __init__(self):
        self.pos = torus_position()
        self.coord, self.patch = {}, {}
        for axis in AXES:
            for by in range(1, RING):
                coord = lax.rem(self.pos[axis] + by, RING)
                self.coord[axis, by] = coord
                self.patch[axis, by] = patch_at({**self.pos, axis: coord})


def remote(src, dst, send_sem, recv_sem, **device_id):
    return pltpu.make_async_remote_copy(
        src_ref=src, dst_ref=dst, send_sem=send_sem, recv_sem=recv_sem, device_id=device_id, device_id_type=MESH
    )


class Ring:
    def __init__(self, torus, axis, view, send_sem, recv_sem):
        me, succ, prev = torus.pos[axis], torus.coord[axis, 1], torus.coord[axis, RING - 1]
        ahead, behind = torus.patch[axis, 1], torus.patch[axis, RING - 1]
        self.sends = ((me, None, ahead), (me, None, behind), (prev, 0, ahead), (succ, 1, behind))
        self.parts = (view, send_sem, recv_sem)

    def copy(self, slot):
        view, send_sem, recv_sem = self.parts
        coord, half, patch = self.sends[slot]
        part = view(coord, half)
        return remote(part, part, send_sem(slot), recv_sem(slot), patch=patch)

    def first(self):
        for slot in (0, 1):
            self.copy(slot).start()

    def relay(self):
        for slot in (0, 1):
            self.copy(slot).wait_recv()
            self.copy(slot + 2).start()

    def settle(self):
        for slot in (2, 3):
            self.copy(slot).wait_recv()

    def drain(self):
        for slot in range(4):
            self.copy(slot).wait_send()


def full_rings(ref, color, torus, send_sem, recv_sem):
    width = ref.shape[4]
    cut = [0, width // 3 // SUB * SUB, width // 3 // SUB * SUB * 2, width]
    base, size = cut[color], cut[color + 1] - cut[color]
    order = COLOR_ORDERS[color]

    def stage(k):
        axis = order[k]

        def view(coord, half):
            index = []
            for name in AXES:
                index.append(coord if name == axis else slice(None) if name in order[:k] else torus.pos[name])
            columns = pl.ds(base, size) if half is None else pl.ds(base + half * (size // 2), size // 2)
            return ref.at[(*index, slice(None), columns)]

        return Ring(torus, axis, view, lambda slot: send_sem.at[k, slot], lambda slot: recv_sem.at[k, slot])

    return [stage(k) for k in range(3)]


def share_rings(ref, head_axis, color, torus, send_sem, recv_sem):
    size = ref.shape[4] // 2
    rest = [axis for axis in AXES if axis != head_axis]
    order = rest if color else rest[::-1]
    columns = pl.ds(color * size, size)

    def stage(k):
        axis = order[k]

        def view(coord, half):
            index = []
            for name in AXES:
                if name == head_axis:
                    index.append(slice(None) if half is None else pl.ds(half * (RING // 2), RING // 2))
                else:
                    index.append(coord if name == axis else slice(None) if name in order[:k] else torus.pos[name])
            return ref.at[(*index, slice(None), columns)]

        return Ring(torus, axis, view, lambda slot: send_sem.at[k, slot], lambda slot: recv_sem.at[k, slot])

    return [stage(k) for k in range(2)]


def denoise_kernel(
    lat, cond, sched, w_ada, w_qkv, w_out, w_up, w_down, w_head, k_old, v_old,
    lat_out, all_k, all_v, shared,
    wbuf, kbuf, vbuf, lat_own, cond_own, xs, r, h, act, out_own, out_peer, down_own, down_peer, sb, rb, o_sum, o_top, o_total, o_own, ob, mod,
    cond_peer, scores,
    w_sem, in_sem, kv_sem, cond_sem, mod_send, mod_recv, qkv_send, qkv_recv, o_send, o_recv, out_send, out_recv, down_send, down_recv,
    x_sem, share_put, share_send, share_recv, own_put, own_send, own_recv, full_send, full_recv,
):
    rows, width = lat.shape
    half = width // 2
    group = width // RING
    chunk = width // 8
    hidden = w_up.shape[2] // 2
    n_qkv = half // TILE
    n_out = width // WIDE
    n_up = hidden // TILE
    n_deep = hidden // half
    n_down = n_out * n_deep
    n_head = half // TILE
    n_block = 3 * n_qkv + n_out + n_up + n_down
    n_step = LAYERS * n_block + n_head
    n_ada = 3
    n_tiles = n_ada + STEPS * n_step
    n_buf = wbuf.shape[0]
    scale = HEAD**-0.5

    c = lax.axis_index("cfg")
    other = 1 - c
    mod_block = other
    torus = Torus()
    z, y, x = (torus.pos[axis] for axis in AXES)
    line = [torus.pos[axis] for axis in HEAD_AXES]
    line_core = [lax.div(at, 2) for at in line]
    line_odd = [lax.rem(at, 2) for at in line]

    def line_patch(b, at):
        return patch_at({**torus.pos, HEAD_AXES[b]: at})

    def line_rows(ref, b):
        return ref.at[tuple(slice(None) if axis == HEAD_AXES[b] else torus.pos[axis] for axis in AXES)]


    def put(src, dst, slot):
        pltpu.make_async_copy(src, dst, w_sem.at[slot]).start()

    def put_deep(ref, col, slot):
        col = pl.multiple_of(col, TILE)
        for k in range(2):
            put(ref.at[pl.ds(k * half, half), pl.ds(col, TILE)], wbuf.at[slot, :, pl.ds(k * TILE, TILE)], slot)

    def put_wide(ref, row, col, slot):
        row = pl.multiple_of(row, half)
        col = pl.multiple_of(col, WIDE)
        put(ref.at[pl.ds(row, half), pl.ds(col, WIDE)], wbuf.at[slot], slot)

    def issue_ada(i):
        col = pl.multiple_of(i * 2 * width + (y * RING + x) * chunk, chunk)
        for k in range(2):
            put(w_ada.at[mod_block, pl.ds(k * half, half), pl.ds(col, chunk)], wbuf.at[i, :, pl.ds(k * chunk, chunk)], i)

    def issue(n):
        slot = lax.rem(n, n_buf)
        inside = lax.rem(n - n_ada, n_step)
        layer = lax.div(inside, n_block)
        u = lax.rem(inside, n_block)
        live = n < n_tiles
        block = live & (inside < LAYERS * n_block)
        at_out, at_up, at_down = 3 * n_qkv, 3 * n_qkv + n_out, 3 * n_qkv + n_out + n_up

        @pl.when(block & (u < at_out))
        def _():
            put_deep(w_qkv.at[layer], lax.div(u, n_qkv) * width + c * half + lax.rem(u, n_qkv) * TILE, slot)

        @pl.when(block & (u >= at_out) & (u < at_up))
        def _():
            put_wide(w_out.at[layer], c * half, (u - at_out) * WIDE, slot)

        @pl.when(block & (u >= at_up) & (u < at_down))
        def _():
            put_deep(w_up.at[layer], c * hidden + (u - at_up) * TILE, slot)

        @pl.when(block & (u >= at_down))
        def _():
            d = u - at_down
            put_wide(w_down.at[layer], c * hidden + lax.rem(d, n_deep) * half, lax.div(d, n_deep) * WIDE, slot)

        @pl.when(live & (inside >= LAYERS * n_block))
        def _():
            put_deep(w_head, c * half + (inside - LAYERS * n_block) * TILE, slot)

    def tile_loop(base, count, body, hooks=()):
        def one(t, carry):
            n = base + t
            slot = lax.rem(n, n_buf)
            tile = wbuf.at[slot]
            pltpu.make_async_copy(tile, tile, w_sem.at[slot]).wait()
            body(t, tile)
            issue(n + n_buf)
            for at, when, hook in hooks:
                pl.when((t == at) & when)(scoped("hook", hook))
            return carry

        lax.fori_loop(0, count, one, 0)

    def deep_dot(tile):
        return dot(h[:, :half], tile[:, :TILE]) + dot(h[:, half:], tile[:, TILE:])

    def load_kv(old_k, old_v):
        pltpu.make_async_copy(old_k, kbuf, kv_sem.at[0]).start()
        pltpu.make_async_copy(old_v, vbuf, kv_sem.at[1]).start()

    def load_stale(b):
        columns = pl.ds(pl.multiple_of(line[b] * group, group), group)
        load_kv(k_old.at[b, :, :, :, :, columns], v_old.at[b, :, :, :, :, columns])

    def load_shared(b):
        load_kv(shared.at[b, 0], shared.at[b, 1])

    share = [
        [share_rings(shared.at[b, i], HEAD_AXES[b], color, torus, share_send.at[b, i, color], share_recv.at[b, i, color]) for i in range(2) for color in range(2)]
        for b in range(LAYERS)
    ]
    full = [
        {
            p: [full_rings(ref.at[b], color, torus, full_send.at[b, p - K, color], full_recv.at[b, p - K, color]) for color in (2, 1, 0)]
            for p, ref in ((K, all_k), (V, all_v))
        }
        for b in range(LAYERS)
    ]

    def first(rings, k):
        for ring in rings:
            if k:
                ring[k - 1].settle()
            ring[k].first()

    def relay(rings, k):
        for ring in rings:
            ring[k].relay()

    def settle(rings, k):
        for ring in rings:
            ring[k].settle()

    barrier = pltpu.get_barrier_semaphore()

    def announce(**device_id):
        pl.semaphore_signal(barrier, inc=1, device_id=device_id, device_id_type=MESH)

    announce(cfg=other)
    for by in range(1, RING):
        for axis in HEAD_AXES:
            for core in range(2):
                announce(patch=torus.patch[axis, by], cfg=core)
        announce(patch=torus.patch["x", by])
    cond_in = pltpu.make_async_copy(cond, cond_own, in_sem.at[0])
    cond_in.start()
    for i in range(n_ada):
        issue_ada(i)
    lat_in = pltpu.make_async_copy(lat, lat_own, in_sem.at[1])
    lat_in.start()
    cond_in.wait()
    with jax.named_scope("barrier"):
        pl.semaphore_wait(barrier, 1 + 5 * (RING - 1))

    cond_swap = remote(cond_own, cond_peer, cond_sem.at[0], cond_sem.at[1], cfg=other)
    cond_swap.start()
    lat_in.wait()
    xs[0] = lat_own[...].astype(F32)
    with jax.named_scope("cond_swap"):
        cond_swap.wait()
    mine, theirs = cond_own[...], cond_peer[...]
    both = jnp.concatenate([jnp.where(c == 0, mine, theirs), jnp.where(c == 0, theirs, mine)], axis=0)
    silu = (both * jax.nn.sigmoid(both)).astype(BF16)

    def mod_ring(i, axis):
        part, base = (mod.at[mod_block, i, y, x], 0) if axis == "y" else (mod.at[mod_block, i, :, x], RING - 1)
        return [
            remote(part, part, mod_send.at[i, base + by - 1], mod_recv.at[i, base + by - 1], patch=torus.patch[axis, by]) for by in range(1, RING)
        ]

    def mod_swap(i):
        return remote(mod.at[mod_block, i], mod.at[mod_block, i], mod_send.at[i, 2 * RING - 2], mod_recv.at[i, 2 * RING - 2], cfg=other)

    def mod_go(i, axis):
        for one in mod_ring(i, axis):
            one.start()

    def mod_wait(i, axis):
        for one in mod_ring(i, axis):
            one.wait_recv()

    for i in range(n_ada):
        with jax.named_scope("ada_wait"):
            filled = wbuf.at[i, :, pl.ds(0, 2 * chunk)]
            pltpu.make_async_copy(filled, filled, w_sem.at[i]).wait()
        if i == 0:
            for n in range(n_ada, n_buf):
                issue(jnp.int32(n))
            load_stale(0)
        tile = wbuf.at[i]
        mod[mod_block, i, y, x] = dot(silu[:, :half], tile[:, :chunk]) + dot(silu[:, half:], tile[:, chunk : 2 * chunk])
        mod_go(i, "y")
        issue(jnp.int32(n_buf + i))
    with jax.named_scope("mod_y"):
        for i in range(n_ada):
            mod_wait(i, "y")
            mod_go(i, "x")

    def mod_pass(i):
        mod_wait(i, "x")
        mod_swap(i).start()

    @pl.when(c == 1)
    def _():
        with jax.named_scope("mod_x"):
            mod_pass(0)

    @pl.when(c == 0)
    def _():
        with jax.named_scope("mod_swap"):
            mod_swap(0).wait_recv()

    def mod_rest():
        pl.when(c == 0)(lambda: mod_pass(0))
        for i in range(1, n_ada):
            mod_pass(i)
        pl.when(c == 1)(lambda: mod_swap(0).wait_recv())
        for i in range(1, n_ada):
            mod_swap(i).wait_recv()

    def mod_row(b, step, which, i, s):
        at = which % 2 * 8 + i
        both = mod[b, which // 2, at // RING, at % RING, s * STEPS : (s + 1) * STEPS, :]
        return jnp.where(step == 0, both[0:1], both[1:2])

    def normed(s):
        values = r[s * rows : (s + 1) * rows, :]
        centered = values - jnp.mean(values, -1, keepdims=True)
        return centered * lax.rsqrt(jnp.mean(centered * centered, -1, keepdims=True) + 1e-6)

    def modulate(b, step, shift, gain):
        for s in range(2):
            values = normed(s)
            for i in range(8):
                at = slice(i * chunk, (i + 1) * chunk)
                part = values[:, at] * (1.0 + mod_row(b, step, gain, i, s)) + mod_row(b, step, shift, i, s)
                h[s * rows : (s + 1) * rows, at] = part.astype(BF16)

    def add_gated(b, step, gate, own, peer):
        for s in range(2):
            for i in range(8):
                at = (slice(s * rows, (s + 1) * rows), slice(i * chunk, (i + 1) * chunk))
                r[at] = r[at] + mod_row(b, step, gate, i, s) * (own[at] + peer[at])

    def chunk_swap(own, peer, t, send_sem, recv_sem):
        columns = pl.ds(pl.multiple_of(t * WIDE, WIDE), WIDE)
        return remote(own.at[:, columns], peer.at[:, columns], send_sem.at[t], recv_sem.at[t], cfg=other)

    def qkv_copy(b, p, s, g):
        return remote(sb.at[s, g, p], rb.at[b, p, line[b]], qkv_send.at[p, s, g], qkv_recv.at[b, p, line[b]], patch=line_patch(b, 2 * c + g), cfg=s)

    def qkv_out(b, p, do_send):
        for s in range(2):
            for g in range(2):
                if do_send:

                    @pl.when((2 * c + g == line[b]) & (c == s))
                    def _():
                        rb[b, p, line[b]] = sb[s, g, p]

                @pl.when((2 * c + g != line[b]) | (c != s))
                def _():
                    if do_send:
                        qkv_copy(b, p, s, g).start()
                    else:
                        qkv_copy(b, p, s, g).wait_send()

    def qkv_in(b, p):
        for src in range(RING):

            @pl.when((line[b] != src) | (c != line_core[b]))
            def _():
                part = rb.at[b, p, src]
                remote(part, part, qkv_send.at[p, 0, 0], qkv_recv.at[b, p, src], cfg=other).wait_recv()

    def qkv_part(p, base, hooks=()):
        def body(t, tile):
            part = deep_dot(tile).astype(BF16)
            for k in range(TILE // SUB):
                col = t * TILE + k * SUB
                g = lax.div(col, group)
                columns = pl.ds(pl.multiple_of(col - g * group, SUB), SUB)
                for s in range(2):
                    sb[s, g, p, :, columns] = part[s * rows : (s + 1) * rows, k * SUB : (k + 1) * SUB]

        tile_loop(base + p * n_qkv, n_qkv, body, hooks)

    def own_copies(b, p):
        local, swap = [], []
        for g in range(2):
            columns = pl.ds(pl.multiple_of(c * half + g * group, group), group)
            place = (all_k if p == K else all_v).at[b, z, y, x, :, columns]
            local.append(pltpu.make_async_copy(sb.at[c, g, p], place, own_put.at[p - K, g]))
            swap.append(remote(sb.at[other, g, p], place, own_send.at[p - K, g], own_recv.at[p - K, g], cfg=other))
        return local + swap

    def own_start(b, p):
        for one in own_copies(b, p):
            one.start()

    def own_wait(b, p):
        for one in own_copies(b, p):
            one.wait()

    def share_copy(b, p):
        return pltpu.make_async_copy(rb.at[b, p], line_rows(shared.at[b, p - K], b), share_put.at[p - K])

    tokens_z = RING * RING * rows
    n_rows = RING * rows

    n_heads = group // HEAD

    def scored(queries, keys):
        return lax.dot_general(queries, keys, (((1,), (1,)), ((), ())), preferred_element_type=F32)

    def patch_of(shape, axis):
        index = lax.broadcasted_iota(jnp.int32, shape, axis)
        return lax.div(index, jnp.full_like(index, rows))

    def attend_cache(b, hooks):
        own_patch = line_patch(b, patch_of((n_rows, tokens_z), 0))
        key_patch = patch_of((n_rows, tokens_z), 1)

        together = 2

        def one(step, carry):
            heads = [step * together + j for j in range(together)]
            columns = [pl.ds(pl.multiple_of(head * HEAD, HEAD), HEAD) for head in heads]
            queries = [rb[b, Q, :, :, at].reshape(n_rows, HEAD) for at in columns]
            tops, totals, mixed = [None] * together, [None] * together, [None] * together
            for plane in range(RING):
                planes = slice(plane * tokens_z, (plane + 1) * tokens_z)
                hidden_keys = key_patch + plane * RING * RING == own_patch
                for j, at in enumerate(columns):
                    part = scored(queries[j], kbuf[plane, :, :, :, at].reshape(tokens_z, HEAD))
                    part = jnp.where(hidden_keys, -jnp.inf, part)
                    scores[j, :, planes] = part
                    best = jnp.max(part, -1, keepdims=True)
                    tops[j] = best if plane == 0 else jnp.maximum(tops[j], best)
            for plane in range(RING):
                planes = slice(plane * tokens_z, (plane + 1) * tokens_z)
                for j, at in enumerate(columns):
                    weights = jnp.exp((scores[j, :, planes] - tops[j]) * scale)
                    add = jnp.sum(weights, -1, keepdims=True)
                    more = dot(weights.astype(BF16), vbuf[plane, :, :, :, at].reshape(tokens_z, HEAD))
                    totals[j] = add if plane == 0 else totals[j] + add
                    mixed[j] = more if plane == 0 else mixed[j] + more
            for j, (head, at) in enumerate(zip(heads, columns)):
                o_sum[:, at] = mixed[j]
                o_top[head] = jnp.broadcast_to(tops[j], (n_rows, HEAD))
                o_total[head] = jnp.broadcast_to(totals[j], (n_rows, HEAD))
            for when_at, when, hook in hooks:
                pl.when((step == when_at // together) & when)(scoped("hook", hook))
            return carry

        for i in range(2):
            buf = (kbuf, vbuf)[i]
            pltpu.make_async_copy(buf, buf, kv_sem.at[i]).wait()
        lax.fori_loop(0, n_heads // together, one, 0)

    def attend_fresh(b):
        same = patch_of((n_rows, n_rows), 0) == patch_of((n_rows, n_rows), 1)
        for start in range(0, n_heads, 3):
            heads = range(start, min(start + 3, n_heads))
            columns = [slice(head * HEAD, (head + 1) * HEAD) for head in heads]
            parts = [scored(rb[b, Q, :, :, at].reshape(n_rows, HEAD), rb[b, K, :, :, at].reshape(n_rows, HEAD)) for at in columns]
            parts = [jnp.where(same, part, -jnp.inf) for part in parts]
            tops = [jnp.maximum(o_top[head], jnp.max(part, -1, keepdims=True)) for head, part in zip(heads, parts)]
            weights = [jnp.exp((part - top) * scale) for part, top in zip(parts, tops)]
            fresh = [dot(weight.astype(BF16), rb[b, V, :, :, at].reshape(n_rows, HEAD)) for weight, at in zip(weights, columns)]
            shrink = [jnp.exp((o_top[head] - top) * scale) for head, top in zip(heads, tops)]
            totals = [o_total[head] * less + jnp.sum(weight, -1, keepdims=True) for head, less, weight in zip(heads, shrink, weights)]
            for at, less, more, total in zip(columns, shrink, fresh, totals):
                o_own[:, :, at] = ((o_sum[:, at] * less + more) / total).astype(BF16).reshape(RING, rows, HEAD)

    def o_copy(b, dst):
        return remote(
            o_own.at[dst], ob.at[c, line_odd[b]], o_send.at[dst], o_recv.at[c, line_odd[b]], patch=line_patch(b, dst), cfg=line_core[b]
        )

    def o_out(b, do_send):
        for dst in range(RING):
            if do_send:

                @pl.when((line[b] == dst) & (c == line_core[b]))
                def _():
                    ob[c, line_odd[b]] = o_own[dst]

            @pl.when((line[b] != dst) | (c != line_core[b]))
            def _():
                if do_send:
                    o_copy(b, dst).start()
                else:
                    o_copy(b, dst).wait_send()

    def o_in(b):
        for s in range(2):
            for g in range(2):

                @pl.when((2 * c + g != line[b]) | (c != s))
                def _():
                    part = ob.at[s, g]
                    remote(part, part, o_send.at[0], o_recv.at[s, g], cfg=other).wait_recv()

    def block(step, b):
        base = n_ada + step * n_step + b * n_block
        begin = step == 0
        last = step == STEPS - 1

        def unless_first(action):
            if b:
                action()
            else:
                pl.when(step > 0)(action)

        def gather_own(p):
            own_wait(b, p)
            first(full[b][p], 0)

        def send_late():
            gather_own(V)
            for p in KV:
                qkv_out(b, p, True)

        if b == 0:
            for s in range(2):
                r[s * rows : (s + 1) * rows, :] = xs[step]
        with jax.named_scope("ln1"):
            modulate(b, step, 0, 1)

        @unless_first
        def _():
            for p in (Q, K, V):
                qkv_out(1 - b, p, False)

        with jax.named_scope("qkv_q"):
            qkv_part(Q, base)
        qkv_out(b, Q, True)
        with jax.named_scope("qkv_k"):
            qkv_part(K, base)
        pl.when(begin)(lambda: qkv_out(b, K, True))

        @pl.when(last)
        def _():
            own_start(b, K)

        with jax.named_scope("qkv_v"):
            qkv_part(V, base, ((n_qkv - 1, last, lambda: gather_own(K)),))

        pl.when(begin)(lambda: qkv_out(b, V, True))

        @pl.when(last)
        def _():
            own_start(b, V)
            if b:
                with jax.named_scope("full_1a"):
                    send_late()
                    first(full[0][V], 2)
                    relay(full[1][K], 0)
                    relay(full[1][V], 0)

        with jax.named_scope("q_in"):
            qkv_in(b, Q)

        @unless_first
        def _():
            o_out(1 - b, False)

        hooks = () if b else ((min(1, n_heads - 2), last, send_late), (max(n_heads - 2, 1), last, lambda: relay(full[0][K], 0)))
        with jax.named_scope("attend_cache"):
            attend_cache(b, hooks)
        if b == 0:
            pl.when(begin)(lambda: load_stale(1))

            @pl.when(last)
            def _():
                with jax.named_scope("full_1"):
                    relay(full[0][V], 0)

        with jax.named_scope("kv_in"):
            for p in KV:
                qkv_in(b, p)

        @pl.when(begin)
        def _():
            for p in KV:
                share_copy(b, p).start()

        with jax.named_scope("attend_fresh"):
            attend_fresh(b)

        @pl.when(begin)
        def _():
            for p in KV:
                share_copy(b, p).wait()

        o_out(b, True)

        @pl.when(begin)
        def _():
            first(share[b], 0)
            if b:
                relay(share[0], 1)
            else:
                with jax.named_scope("mod_rest"):
                    mod_rest()

        @pl.when(last)
        def _():
            with jax.named_scope("full_2"):
                if b == 0:
                    first(full[0][K], 1)
                else:
                    relay(full[0][K], 2)
                    first(full[1][K], 1)
                    first(full[1][V], 1)
                    relay(full[0][V], 2)

        with jax.named_scope("o_in"):
            o_in(b)

        def out_body(t, tile):
            columns = pl.ds(pl.multiple_of(t * WIDE, WIDE), WIDE)
            part = [ob[:, g].reshape(2 * rows, group) for g in range(2)]
            out_own[:, columns] = dot(part[0], tile[:group]) + dot(part[1], tile[group:])
            chunk_swap(out_own, out_peer, t, out_send, out_recv).start()

        @unless_first
        def _():
            for t in range(n_out):
                chunk_swap(out_own, out_peer, t, out_send, out_recv).wait_send()

        with jax.named_scope("out"):
            tile_loop(base + 3 * n_qkv, n_out, out_body)
        if b:
            pl.when(begin)(lambda: relay(share[1], 0))
        else:
            pl.when(last)(lambda: first(full[0][V], 1))

        with jax.named_scope("out_swap"):
            for t in range(n_out):
                chunk_swap(out_own, out_peer, t, out_send, out_recv).wait_recv()
        with jax.named_scope("ln2"):
            add_gated(b, step, 2, out_own, out_peer)
            modulate(b, step, 3, 4)

        def up_body(t, tile):
            act[:, pl.ds(pl.multiple_of(t * TILE, TILE), TILE)] = jax.nn.gelu(deep_dot(tile), approximate=True).astype(BF16)

        def refill():
            settle(share[1 - b], 1)
            load_shared(1 - b)

        if b:
            hooks = (
                (n_up // 6, begin, refill),
                (n_up * 5 // 12, begin, lambda: first(share[1], 1)),
            )
        else:
            hooks = (
                (1, begin, lambda: relay(share[0], 0)),
                (n_up * 2 // 3, begin, lambda: first(share[0], 1)),
                (1, last, refill),
                (n_up // 6, last, lambda: relay(full[0][K], 1)),
                (n_up * 3 // 4, last, lambda: relay(full[0][V], 1)),
            )
        with jax.named_scope("up"):
            tile_loop(base + 3 * n_qkv + n_out, n_up, up_body, hooks)

        def down_body(t, tile):
            n = lax.div(t, n_deep)
            deep = lax.rem(t, n_deep)
            columns = pl.ds(pl.multiple_of(n * WIDE, WIDE), WIDE)
            part = dot(act[:, pl.ds(pl.multiple_of(deep * half, half), half)], tile[...])

            @pl.when(deep == 0)
            def _():
                down_own[:, columns] = part

            @pl.when(deep != 0)
            def _():
                down_own[:, columns] = down_own[:, columns] + part

            @pl.when(deep == n_deep - 1)
            def _():
                chunk_swap(down_own, down_peer, n, down_send, down_recv).start()

        @unless_first
        def _():
            for t in range(n_out):
                chunk_swap(down_own, down_peer, t, down_send, down_recv).wait_send()

        if b:
            hooks = (
                (n_down * 7 // 12, begin, lambda: relay(share[1][:2], 1)),
                (n_down // 4, last, lambda: relay(full[1][K], 1)),
                (n_down // 2, last, lambda: relay(full[1][V], 1)),
            )
        else:
            hooks = ((n_down // 12, last, lambda: first(full[0][K], 2)),)
        with jax.named_scope("down"):
            tile_loop(base + 3 * n_qkv + n_out + n_up, n_down, down_body, hooks)
        with jax.named_scope("down_swap"):
            for t in range(n_out):
                chunk_swap(down_own, down_peer, t, down_send, down_recv).wait_recv()
        with jax.named_scope("gate2"):
            add_gated(b, step, 5, down_own, down_peer)

    def one_step(step, carry):
        for b in range(LAYERS):
            block(step, b)
        for s in range(2):
            h[s * rows : (s + 1) * rows, :] = normed(s).astype(BF16)
        later = lax.rem(step + 1, STEPS)

        def head_body(t, tile):
            eps = deep_dot(tile).astype(BF16).astype(F32)
            with_cond, without = eps[:rows], eps[rows:]
            guided = without + sched[step, 2] * (with_cond - without)
            columns = pl.ds(pl.multiple_of(c * half + t * TILE, TILE), TILE)
            xs[later, :, columns] = sched[step, 0] * xs[step, :, columns] + sched[step, 1] * guided

        @pl.when(step > 0)
        def _():
            x_half(xs, step, c, half, x_sem, other).wait_send()

        with jax.named_scope("head"):
            tile_loop(n_ada + step * n_step + LAYERS * n_block, n_head, head_body)
        swap = x_half(xs, later, c, half, x_sem, other)
        swap.start()
        with jax.named_scope("x_swap"):
            swap.wait_recv()

        @pl.when(step == 0)
        def _():
            with jax.named_scope("relay_share"):
                relay(share[1][2:], 1)

        return carry

    lax.fori_loop(0, STEPS, one_step, 0)
    lat_out[...] = xs[0]

    with jax.named_scope("tail_c1"):
        for p in KV:
            first(full[1][p], 2)
    with jax.named_scope("tail_c2k"):
        relay(full[1][K], 2)
    with jax.named_scope("tail_c2v"):
        relay(full[1][V], 2)
    with jax.named_scope("tail_end"):
        for b in range(LAYERS):
            for p in KV:
                settle(full[b][p], 2)
    x_half(xs, 0, c, half, x_sem, other).wait_send()
    for p in (Q, K, V):
        qkv_out(LAYERS - 1, p, False)
    o_out(LAYERS - 1, False)
    for t in range(n_out):
        chunk_swap(out_own, out_peer, t, out_send, out_recv).wait_send()
        chunk_swap(down_own, down_peer, t, down_send, down_recv).wait_send()
    for i in range(n_ada):
        for one in (*mod_ring(i, "y"), *mod_ring(i, "x"), mod_swap(i)):
            one.wait_send()
    for b in range(LAYERS):
        for ring in share[b] + full[b][K] + full[b][V]:
            for stage in ring:
                stage.drain()


def x_half(xs, at, c, half, x_sem, other):
    part = xs.at[at, :, pl.ds(pl.multiple_of(c * half, half), half)]
    return remote(part, part, x_sem.at[0], x_sem.at[1], cfg=other)


def denoise(lat, cond, sched, w_ada, w_qkv, w_out, w_up, w_down, w_head, k_old, v_old):
    rows, width = lat.shape
    group = width // RING
    hidden = w_up.shape[2] // 2
    torus = (RING, RING, RING)
    cache = jax.ShapeDtypeStruct((LAYERS, *torus, rows, width), BF16)
    k_old = k_old.reshape(cache.shape)
    v_old = v_old.reshape(cache.shape)
    w_out = w_out.reshape(LAYERS, width, width)
    n_out = width // WIDE
    anywhere = pl.BlockSpec(memory_space=pl.ANY)
    vmem = pl.BlockSpec(memory_space=pltpu.VMEM)
    dma = pltpu.SemaphoreType.DMA
    n_heads = group // HEAD
    n_ada = 3
    lat_out, all_k, all_v, _ = pl.pallas_call(
        denoise_kernel,
        out_shape=(
            jax.ShapeDtypeStruct((rows, width), F32),
            cache,
            cache,
            jax.ShapeDtypeStruct((LAYERS, 2, *torus, rows, group), BF16),
        ),
        in_specs=[anywhere, anywhere, pl.BlockSpec(memory_space=pltpu.SMEM)] + [anywhere] * 8,
        out_specs=[vmem, anywhere, anywhere, anywhere],
        scratch_shapes=[
            pltpu.VMEM((BUFFERS, width // 2, WIDE), BF16),
            pltpu.VMEM((*torus, rows, group), BF16),
            pltpu.VMEM((*torus, rows, group), BF16),
            pltpu.VMEM((rows, width), BF16),
            pltpu.VMEM((STEPS, width), F32),
            pltpu.VMEM((STEPS, rows, width), F32),
            pltpu.VMEM((2 * rows, width), F32),
            pltpu.VMEM((2 * rows, width), BF16),
            pltpu.VMEM((2 * rows, hidden), BF16),
            pltpu.VMEM((2 * rows, width), F32),
            pltpu.VMEM((2 * rows, width), F32),
            pltpu.VMEM((2 * rows, width), F32),
            pltpu.VMEM((2 * rows, width), F32),
            pltpu.VMEM((2, 2, 3, rows, group), BF16),
            pltpu.VMEM((LAYERS, 3, RING, rows, group), BF16),
            pltpu.VMEM((RING * rows, group), F32),
            pltpu.VMEM((n_heads, RING * rows, HEAD), F32),
            pltpu.VMEM((n_heads, RING * rows, HEAD), F32),
            pltpu.VMEM((RING, rows, group), BF16),
            pltpu.VMEM((2, 2, rows, group), BF16),
            pltpu.VMEM((LAYERS, n_ada, RING, RING, 2 * STEPS, width // 8), F32),
            pltpu.VMEM((STEPS, width), F32),
            pltpu.VMEM((2, RING * rows, RING**3 * rows), F32),
            dma((BUFFERS,)),
            dma((2,)),
            dma((2,)),
            dma((2,)),
            dma((n_ada, 2 * RING - 1)),
            dma((n_ada, 2 * RING - 1)),
            dma((3, 2, 2)),
            dma((LAYERS, 3, RING)),
            dma((RING,)),
            dma((2, 2)),
            dma((n_out,)),
            dma((n_out,)),
            dma((n_out,)),
            dma((n_out,)),
            dma((2,)),
            dma((2,)),
            dma((LAYERS, 2, 2, 2, 4)),
            dma((LAYERS, 2, 2, 2, 4)),
            dma((2, 2)),
            dma((2, 2)),
            dma((2, 2)),
            dma((LAYERS, 2, 3, 3, 4)),
            dma((LAYERS, 2, 3, 3, 4)),
        ],
        compiler_params=pltpu.CompilerParams(collective_id=0, has_side_effects=True, vmem_limit_bytes=63 * 2**20),
        name="denoise",
    )(lat, cond, sched.T, w_ada, w_qkv, w_out, w_up, w_down, w_head, k_old, v_old)
    tokens = RING**3 * rows
    return lat_out, all_k.reshape(LAYERS, tokens, width), all_v.reshape(LAYERS, tokens, width)


def solution(mesh):
    slot_spec = P(("img", "cfg"), None, None)
    cache_spec = P(("img", "cfg"), None, None, None)
    rep_spec = P()

    def local_step(latent, cond_vec, sched_coef, w_ada, w_qkv, w_out, w_up, w_down, w_head, k_stale, v_stale):
        lat_out, k_new, v_new = denoise(
            latent[0], cond_vec[0], sched_coef, w_ada, w_qkv, w_out, w_up, w_down, w_head, k_stale[0], v_stale[0]
        )
        return lat_out[None], k_new[None], v_new[None]

    return jax.shard_map(
        local_step,
        mesh=mesh,
        in_specs=(P("img", "patch", None), slot_spec, rep_spec, rep_spec, rep_spec, rep_spec, rep_spec, rep_spec, rep_spec, cache_spec, cache_spec),
        out_specs=(P(("img", "cfg"), "patch", None), cache_spec, cache_spec),
        check_vma=False,
    )
```

```python
import functools

import jax
import jax.numpy as jnp
from jax import lax
from jax.experimental import pallas as pl
from jax.experimental.pallas import tpu as pltpu
from jax.sharding import PartitionSpec as P

RING = 4
AXES = ("z", "y", "x")
COLOR_ORDERS = (("x", "y", "z"), ("y", "z", "x"), ("z", "x", "y"))
HEAD_AXES = ("z", "y")
MESH = pl.DeviceIdType.MESH
F32 = jnp.float32
BF16 = jnp.bfloat16
HEAD = 128
TILE = 512
SUB = 256
WIDE = 2 * TILE
BUFFERS = 12
STEPS = 2
LAYERS = 2
Q, K, V = 0, 1, 2
KV = (K, V)


def dot(lhs, rhs):
    return jnp.dot(lhs, rhs, preferred_element_type=F32)


def scoped(name, action):
    def inside():
        with jax.named_scope(name):
            action()

    return inside


def torus_position():
    patch = lax.axis_index("patch")
    return {"z": lax.div(patch, RING * RING), "y": lax.rem(lax.div(patch, RING), RING), "x": lax.rem(patch, RING)}


def patch_at(pos):
    return (pos["z"] * RING + pos["y"]) * RING + pos["x"]


class Torus:
    def __init__(self):
        self.pos = torus_position()
        self.coord, self.patch = {}, {}
        for axis in AXES:
            for by in range(1, RING):
                coord = lax.rem(self.pos[axis] + by, RING)
                self.coord[axis, by] = coord
                self.patch[axis, by] = patch_at({**self.pos, axis: coord})


def remote(src, dst, send_sem, recv_sem, **device_id):
    return pltpu.make_async_remote_copy(
        src_ref=src, dst_ref=dst, send_sem=send_sem, recv_sem=recv_sem, device_id=device_id, device_id_type=MESH
    )


class Ring:
    def __init__(self, torus, axis, view, send_sem, recv_sem):
        me, succ, prev = torus.pos[axis], torus.coord[axis, 1], torus.coord[axis, RING - 1]
        ahead, behind = torus.patch[axis, 1], torus.patch[axis, RING - 1]
        self.sends = ((me, None, ahead), (me, None, behind), (prev, 0, ahead), (succ, 1, behind))
        self.parts = (view, send_sem, recv_sem)

    def copy(self, slot):
        view, send_sem, recv_sem = self.parts
        coord, half, patch = self.sends[slot]
        part = view(coord, half)
        return remote(part, part, send_sem(slot), recv_sem(slot), patch=patch)

    def first(self):
        for slot in (0, 1):
            self.copy(slot).start()

    def relay(self):
        for slot in (0, 1):
            self.copy(slot).wait_recv()
            self.copy(slot + 2).start()

    def settle(self):
        for slot in (2, 3):
            self.copy(slot).wait_recv()

    def drain(self):
        for slot in range(4):
            self.copy(slot).wait_send()


def full_rings(ref, color, torus, send_sem, recv_sem):
    width = ref.shape[4]
    cut = [0, width // 3 // SUB * SUB, width // 3 // SUB * SUB * 2, width]
    base, size = cut[color], cut[color + 1] - cut[color]
    order = COLOR_ORDERS[color]

    def stage(k):
        axis = order[k]

        def view(coord, half):
            index = []
            for name in AXES:
                index.append(coord if name == axis else slice(None) if name in order[:k] else torus.pos[name])
            columns = pl.ds(base, size) if half is None else pl.ds(base + half * (size // 2), size // 2)
            return ref.at[(*index, slice(None), columns)]

        return Ring(torus, axis, view, lambda slot: send_sem.at[k, slot], lambda slot: recv_sem.at[k, slot])

    return [stage(k) for k in range(3)]


def share_rings(ref, head_axis, color, torus, send_sem, recv_sem):
    size = ref.shape[4] // 2
    rest = [axis for axis in AXES if axis != head_axis]
    order = rest if color else rest[::-1]
    columns = pl.ds(color * size, size)

    def stage(k):
        axis = order[k]

        def view(coord, half):
            index = []
            for name in AXES:
                if name == head_axis:
                    index.append(slice(None) if half is None else pl.ds(half * (RING // 2), RING // 2))
                else:
                    index.append(coord if name == axis else slice(None) if name in order[:k] else torus.pos[name])
            return ref.at[(*index, slice(None), columns)]

        return Ring(torus, axis, view, lambda slot: send_sem.at[k, slot], lambda slot: recv_sem.at[k, slot])

    return [stage(k) for k in range(2)]


def denoise_kernel(
    lat, cond, sched, w_ada, w_qkv, w_out, w_up, w_down, w_head, k_old, v_old,
    lat_out, all_k, all_v, shared,
    wbuf, kbuf, vbuf, lat_own, cond_own, xs, r, h, act, out_own, out_peer, down_own, down_peer, sb, rb, o_sum, o_top, o_total, o_own, ob, mod,
    cond_peer, scores,
    w_sem, in_sem, kv_sem, cond_sem, mod_send, mod_recv, qkv_send, qkv_recv, o_send, o_recv, out_send, out_recv, down_send, down_recv,
    x_sem, share_put, share_send, share_recv, own_put, own_send, own_recv, full_send, full_recv,
):
    rows, width = lat.shape
    half = width // 2
    group = width // RING
    chunk = width // 8
    hidden = w_up.shape[2] // 2
    n_qkv = half // TILE
    n_out = width // WIDE
    n_up = hidden // TILE
    n_deep = hidden // half
    n_down = n_out * n_deep
    n_head = half // TILE
    n_block = 3 * n_qkv + n_out + n_up + n_down
    n_step = LAYERS * n_block + n_head
    n_ada = 3
    n_tiles = n_ada + STEPS * n_step
    n_buf = wbuf.shape[0]
    scale = HEAD**-0.5

    c = lax.axis_index("cfg")
    other = 1 - c
    mod_block = other
    torus = Torus()
    z, y, x = (torus.pos[axis] for axis in AXES)
    line = [torus.pos[axis] for axis in HEAD_AXES]
    line_core = [lax.div(at, 2) for at in line]
    line_odd = [lax.rem(at, 2) for at in line]

    def line_patch(b, at):
        return patch_at({**torus.pos, HEAD_AXES[b]: at})

    def line_rows(ref, b):
        return ref.at[tuple(slice(None) if axis == HEAD_AXES[b] else torus.pos[axis] for axis in AXES)]


    def put(src, dst, slot):
        pltpu.make_async_copy(src, dst, w_sem.at[slot]).start()

    def put_deep(ref, col, slot):
        col = pl.multiple_of(col, TILE)
        for k in range(2):
            put(ref.at[pl.ds(k * half, half), pl.ds(col, TILE)], wbuf.at[slot, :, pl.ds(k * TILE, TILE)], slot)

    def put_wide(ref, row, col, slot):
        row = pl.multiple_of(row, half)
        col = pl.multiple_of(col, WIDE)
        put(ref.at[pl.ds(row, half), pl.ds(col, WIDE)], wbuf.at[slot], slot)

    def issue_ada(i):
        col = pl.multiple_of(i * 2 * width + (y * RING + x) * chunk, chunk)
        for k in range(2):
            put(w_ada.at[mod_block, pl.ds(k * half, half), pl.ds(col, chunk)], wbuf.at[i, :, pl.ds(k * chunk, chunk)], i)

    def issue(n):
        slot = lax.rem(n, n_buf)
        inside = lax.rem(n - n_ada, n_step)
        layer = lax.div(inside, n_block)
        u = lax.rem(inside, n_block)
        live = n < n_tiles
        block = live & (inside < LAYERS * n_block)
        at_out, at_up, at_down = 3 * n_qkv, 3 * n_qkv + n_out, 3 * n_qkv + n_out + n_up

        @pl.when(block & (u < at_out))
        def _():
            put_deep(w_qkv.at[layer], lax.div(u, n_qkv) * width + c * half + lax.rem(u, n_qkv) * TILE, slot)

        @pl.when(block & (u >= at_out) & (u < at_up))
        def _():
            put_wide(w_out.at[layer], c * half, (u - at_out) * WIDE, slot)

        @pl.when(block & (u >= at_up) & (u < at_down))
        def _():
            put_deep(w_up.at[layer], c * hidden + (u - at_up) * TILE, slot)

        @pl.when(block & (u >= at_down))
        def _():
            d = u - at_down
            put_wide(w_down.at[layer], c * hidden + lax.rem(d, n_deep) * half, lax.div(d, n_deep) * WIDE, slot)

        @pl.when(live & (inside >= LAYERS * n_block))
        def _():
            put_deep(w_head, c * half + (inside - LAYERS * n_block) * TILE, slot)

    def tile_loop(base, count, body, hooks=()):
        def one(t, carry):
            n = base + t
            slot = lax.rem(n, n_buf)
            tile = wbuf.at[slot]
            pltpu.make_async_copy(tile, tile, w_sem.at[slot]).wait()
            body(t, tile)
            issue(n + n_buf)
            for at, when, hook in hooks:
                pl.when((t == at) & when)(scoped("hook", hook))
            return carry

        lax.fori_loop(0, count, one, 0)

    def deep_dot(tile):
        return dot(h[:, :half], tile[:, :TILE]) + dot(h[:, half:], tile[:, TILE:])

    def load_kv(old_k, old_v):
        pltpu.make_async_copy(old_k, kbuf, kv_sem.at[0]).start()
        pltpu.make_async_copy(old_v, vbuf, kv_sem.at[1]).start()

    def load_stale(b):
        columns = pl.ds(pl.multiple_of(line[b] * group, group), group)
        load_kv(k_old.at[b, :, :, :, :, columns], v_old.at[b, :, :, :, :, columns])

    def load_shared(b):
        load_kv(shared.at[b, 0], shared.at[b, 1])

    share = [
        [share_rings(shared.at[b, i], HEAD_AXES[b], color, torus, share_send.at[b, i, color], share_recv.at[b, i, color]) for i in range(2) for color in range(2)]
        for b in range(LAYERS)
    ]
    full = [
        {
            p: [full_rings(ref.at[b], color, torus, full_send.at[b, p - K, color], full_recv.at[b, p - K, color]) for color in (2, 0, 1)]
            for p, ref in ((K, all_k), (V, all_v))
        }
        for b in range(LAYERS)
    ]

    def first(rings, k):
        for ring in rings:
            if k:
                ring[k - 1].settle()
            ring[k].first()

    def relay(rings, k):
        for ring in rings:
            ring[k].relay()

    def settle(rings, k):
        for ring in rings:
            ring[k].settle()

    barrier = pltpu.get_barrier_semaphore()

    def announce(**device_id):
        pl.semaphore_signal(barrier, inc=1, device_id=device_id, device_id_type=MESH)

    announce(cfg=other)
    for by in range(1, RING):
        for axis in HEAD_AXES:
            for core in range(2):
                announce(patch=torus.patch[axis, by], cfg=core)
        announce(patch=torus.patch["x", by])
    cond_in = pltpu.make_async_copy(cond, cond_own, in_sem.at[0])
    cond_in.start()
    for i in range(n_ada):
        issue_ada(i)
    lat_in = pltpu.make_async_copy(lat, lat_own, in_sem.at[1])
    lat_in.start()
    cond_in.wait()
    with jax.named_scope("barrier"):
        pl.semaphore_wait(barrier, 1 + 5 * (RING - 1))

    cond_swap = remote(cond_own, cond_peer, cond_sem.at[0], cond_sem.at[1], cfg=other)
    cond_swap.start()
    lat_in.wait()
    xs[0] = lat_own[...].astype(F32)
    with jax.named_scope("cond_swap"):
        cond_swap.wait()
    mine, theirs = cond_own[...], cond_peer[...]
    both = jnp.concatenate([jnp.where(c == 0, mine, theirs), jnp.where(c == 0, theirs, mine)], axis=0)
    silu = (both * jax.nn.sigmoid(both)).astype(BF16)

    def mod_ring(i, axis):
        part, base = (mod.at[mod_block, i, y, x], 0) if axis == "y" else (mod.at[mod_block, i, :, x], RING - 1)
        return [
            remote(part, part, mod_send.at[i, base + by - 1], mod_recv.at[i, base + by - 1], patch=torus.patch[axis, by]) for by in range(1, RING)
        ]

    def mod_swap(i):
        return remote(mod.at[mod_block, i], mod.at[mod_block, i], mod_send.at[i, 2 * RING - 2], mod_recv.at[i, 2 * RING - 2], cfg=other)

    def mod_go(i, axis):
        for one in mod_ring(i, axis):
            one.start()

    def mod_wait(i, axis):
        for one in mod_ring(i, axis):
            one.wait_recv()

    for i in range(n_ada):
        with jax.named_scope("ada_wait"):
            filled = wbuf.at[i, :, pl.ds(0, 2 * chunk)]
            pltpu.make_async_copy(filled, filled, w_sem.at[i]).wait()
        if i == 0:
            for n in range(n_ada, n_buf):
                issue(jnp.int32(n))
            load_stale(0)
        tile = wbuf.at[i]
        mod[mod_block, i, y, x] = dot(silu[:, :half], tile[:, :chunk]) + dot(silu[:, half:], tile[:, chunk : 2 * chunk])
        mod_go(i, "y")
        issue(jnp.int32(n_buf + i))
    with jax.named_scope("mod_y"):
        for i in range(n_ada):
            mod_wait(i, "y")
            mod_go(i, "x")

    def mod_pass(i):
        mod_wait(i, "x")
        mod_swap(i).start()

    @pl.when(c == 1)
    def _():
        with jax.named_scope("mod_x"):
            mod_pass(0)

    @pl.when(c == 0)
    def _():
        with jax.named_scope("mod_swap"):
            mod_swap(0).wait_recv()

    def mod_rest():
        pl.when(c == 0)(lambda: mod_pass(0))
        for i in range(1, n_ada):
            mod_pass(i)

    def mod_rest_in():
        pl.when(c == 1)(lambda: mod_swap(0).wait_recv())
        for i in range(1, n_ada):
            mod_swap(i).wait_recv()

    def mod_row(b, step, which, i, s):
        at = which % 2 * 8 + i
        both = mod[b, which // 2, at // RING, at % RING, s * STEPS : (s + 1) * STEPS, :]
        return jnp.where(step == 0, both[0:1], both[1:2])

    def normed(s):
        values = r[s * rows : (s + 1) * rows, :]
        centered = values - jnp.mean(values, -1, keepdims=True)
        return centered * lax.rsqrt(jnp.mean(centered * centered, -1, keepdims=True) + 1e-6)

    def modulate(b, step, shift, gain):
        for s in range(2):
            values = normed(s)
            for i in range(8):
                at = slice(i * chunk, (i + 1) * chunk)
                part = values[:, at] * (1.0 + mod_row(b, step, gain, i, s)) + mod_row(b, step, shift, i, s)
                h[s * rows : (s + 1) * rows, at] = part.astype(BF16)

    def add_gated(b, step, gate, own, peer):
        for s in range(2):
            for i in range(8):
                at = (slice(s * rows, (s + 1) * rows), slice(i * chunk, (i + 1) * chunk))
                r[at] = r[at] + mod_row(b, step, gate, i, s) * (own[at] + peer[at])

    def chunk_swap(own, peer, t, send_sem, recv_sem):
        columns = pl.ds(pl.multiple_of(t * WIDE, WIDE), WIDE)
        return remote(own.at[:, columns], peer.at[:, columns], send_sem.at[t], recv_sem.at[t], cfg=other)

    def qkv_copy(b, p, s, g):
        return remote(sb.at[s, g, p], rb.at[b, p, line[b]], qkv_send.at[p, s, g], qkv_recv.at[b, p, line[b]], patch=line_patch(b, 2 * c + g), cfg=s)

    def qkv_out(b, p, do_send):
        for s in range(2):
            for g in range(2):
                if do_send:

                    @pl.when((2 * c + g == line[b]) & (c == s))
                    def _():
                        rb[b, p, line[b]] = sb[s, g, p]

                @pl.when((2 * c + g != line[b]) | (c != s))
                def _():
                    if do_send:
                        qkv_copy(b, p, s, g).start()
                    else:
                        qkv_copy(b, p, s, g).wait_send()

    def qkv_in(b, p):
        for src in range(RING):

            @pl.when((line[b] != src) | (c != line_core[b]))
            def _():
                part = rb.at[b, p, src]
                remote(part, part, qkv_send.at[p, 0, 0], qkv_recv.at[b, p, src], cfg=other).wait_recv()

    def qkv_part(p, base, hooks=()):
        def body(t, tile):
            part = deep_dot(tile).astype(BF16)
            for k in range(TILE // SUB):
                col = t * TILE + k * SUB
                g = lax.div(col, group)
                columns = pl.ds(pl.multiple_of(col - g * group, SUB), SUB)
                for s in range(2):
                    sb[s, g, p, :, columns] = part[s * rows : (s + 1) * rows, k * SUB : (k + 1) * SUB]

        tile_loop(base + p * n_qkv, n_qkv, body, hooks)

    def own_copies(b, p):
        local, swap = [], []
        for g in range(2):
            columns = pl.ds(pl.multiple_of(c * half + g * group, group), group)
            place = (all_k if p == K else all_v).at[b, z, y, x, :, columns]
            local.append(pltpu.make_async_copy(sb.at[c, g, p], place, own_put.at[p - K, g]))
            swap.append(remote(sb.at[other, g, p], place, own_send.at[p - K, g], own_recv.at[p - K, g], cfg=other))
        return local + swap

    def own_start(b, p):
        for one in own_copies(b, p):
            one.start()

    def own_wait(b, p):
        for one in own_copies(b, p):
            one.wait()

    def share_copy(b, p):
        return pltpu.make_async_copy(rb.at[b, p], line_rows(shared.at[b, p - K], b), share_put.at[p - K])

    tokens_z = RING * RING * rows
    n_rows = RING * rows

    n_heads = group // HEAD

    def scored(queries, keys):
        return lax.dot_general(queries, keys, (((1,), (1,)), ((), ())), preferred_element_type=F32)

    def patch_of(shape, axis):
        index = lax.broadcasted_iota(jnp.int32, shape, axis)
        return lax.div(index, jnp.full_like(index, rows))

    def attend_cache(b, hooks):
        own_patch = line_patch(b, patch_of((n_rows, tokens_z), 0))
        key_patch = patch_of((n_rows, tokens_z), 1)

        together = 2

        def one(step, carry):
            heads = [step * together + j for j in range(together)]
            columns = [pl.ds(pl.multiple_of(head * HEAD, HEAD), HEAD) for head in heads]
            queries = [rb[b, Q, :, :, at].reshape(n_rows, HEAD) for at in columns]
            tops, totals, mixed = [None] * together, [None] * together, [None] * together
            for plane in range(RING):
                planes = slice(plane * tokens_z, (plane + 1) * tokens_z)
                hidden_keys = key_patch + plane * RING * RING == own_patch
                for j, at in enumerate(columns):
                    part = scored(queries[j], kbuf[plane, :, :, :, at].reshape(tokens_z, HEAD))
                    part = jnp.where(hidden_keys, -jnp.inf, part)
                    scores[j, :, planes] = part
                    best = jnp.max(part, -1, keepdims=True)
                    tops[j] = best if plane == 0 else jnp.maximum(tops[j], best)
            for plane in range(RING):
                planes = slice(plane * tokens_z, (plane + 1) * tokens_z)
                for j, at in enumerate(columns):
                    weights = jnp.exp((scores[j, :, planes] - tops[j]) * scale)
                    add = jnp.sum(weights, -1, keepdims=True)
                    more = dot(weights.astype(BF16), vbuf[plane, :, :, :, at].reshape(tokens_z, HEAD))
                    totals[j] = add if plane == 0 else totals[j] + add
                    mixed[j] = more if plane == 0 else mixed[j] + more
            for j, (head, at) in enumerate(zip(heads, columns)):
                o_sum[:, at] = mixed[j]
                o_top[head] = jnp.broadcast_to(tops[j], (n_rows, HEAD))
                o_total[head] = jnp.broadcast_to(totals[j], (n_rows, HEAD))
            for when_at, when, hook in hooks:
                pl.when((step == when_at // together) & when)(scoped("hook", hook))
            return carry

        for i in range(2):
            buf = (kbuf, vbuf)[i]
            pltpu.make_async_copy(buf, buf, kv_sem.at[i]).wait()
        lax.fori_loop(0, n_heads // together, one, 0)

    def attend_fresh(b):
        same = patch_of((n_rows, n_rows), 0) == patch_of((n_rows, n_rows), 1)
        for start in range(0, n_heads, 3):
            heads = range(start, min(start + 3, n_heads))
            columns = [slice(head * HEAD, (head + 1) * HEAD) for head in heads]
            parts = [scored(rb[b, Q, :, :, at].reshape(n_rows, HEAD), rb[b, K, :, :, at].reshape(n_rows, HEAD)) for at in columns]
            parts = [jnp.where(same, part, -jnp.inf) for part in parts]
            tops = [jnp.maximum(o_top[head], jnp.max(part, -1, keepdims=True)) for head, part in zip(heads, parts)]
            weights = [jnp.exp((part - top) * scale) for part, top in zip(parts, tops)]
            fresh = [dot(weight.astype(BF16), rb[b, V, :, :, at].reshape(n_rows, HEAD)) for weight, at in zip(weights, columns)]
            shrink = [jnp.exp((o_top[head] - top) * scale) for head, top in zip(heads, tops)]
            totals = [o_total[head] * less + jnp.sum(weight, -1, keepdims=True) for head, less, weight in zip(heads, shrink, weights)]
            for at, less, more, total in zip(columns, shrink, fresh, totals):
                o_own[:, :, at] = ((o_sum[:, at] * less + more) / total).astype(BF16).reshape(RING, rows, HEAD)

    def o_copy(b, dst):
        return remote(
            o_own.at[dst], ob.at[c, line_odd[b]], o_send.at[dst], o_recv.at[c, line_odd[b]], patch=line_patch(b, dst), cfg=line_core[b]
        )

    def o_out(b, do_send):
        for dst in range(RING):
            if do_send:

                @pl.when((line[b] == dst) & (c == line_core[b]))
                def _():
                    ob[c, line_odd[b]] = o_own[dst]

            @pl.when((line[b] != dst) | (c != line_core[b]))
            def _():
                if do_send:
                    o_copy(b, dst).start()
                else:
                    o_copy(b, dst).wait_send()

    def o_in(b):
        for s in range(2):
            for g in range(2):

                @pl.when((2 * c + g != line[b]) | (c != s))
                def _():
                    part = ob.at[s, g]
                    remote(part, part, o_send.at[0], o_recv.at[s, g], cfg=other).wait_recv()

    def block(step, b):
        base = n_ada + step * n_step + b * n_block
        begin = step == 0
        last = step == STEPS - 1

        def unless_first(action):
            if b:
                action()
            else:
                pl.when(step > 0)(action)

        def gather_own(p):
            own_wait(b, p)
            first(full[b][p], 0)

        def send_late():
            gather_own(V)
            for p in KV:
                qkv_out(b, p, True)

        if b == 0:
            for s in range(2):
                r[s * rows : (s + 1) * rows, :] = xs[step]
        with jax.named_scope("ln1"):
            modulate(b, step, 0, 1)

        @unless_first
        def _():
            for p in (Q, K, V):
                qkv_out(1 - b, p, False)

        with jax.named_scope("qkv_q"):
            qkv_part(Q, base)
        qkv_out(b, Q, True)
        with jax.named_scope("qkv_k"):
            qkv_part(K, base)
        pl.when(begin)(lambda: qkv_out(b, K, True))

        @pl.when(last)
        def _():
            own_start(b, K)

        with jax.named_scope("qkv_v"):
            qkv_part(V, base, ((n_qkv - 1, last, lambda: gather_own(K)),))

        pl.when(begin)(lambda: qkv_out(b, V, True))

        @pl.when(last)
        def _():
            own_start(b, V)
            if b:
                with jax.named_scope("full_1a"):
                    send_late()
                    first(full[0][V], 2)
                    relay(full[1][K], 0)
                    relay(full[1][V], 0)

        with jax.named_scope("q_in"):
            qkv_in(b, Q)

        @unless_first
        def _():
            o_out(1 - b, False)

        hooks = () if b else ((min(1, n_heads - 2), last, send_late), (max(n_heads - 2, 1), last, lambda: relay(full[0][K], 0)))
        with jax.named_scope("attend_cache"):
            attend_cache(b, hooks)
        if b == 0:
            pl.when(begin)(lambda: load_stale(1))

            @pl.when(last)
            def _():
                with jax.named_scope("full_1"):
                    relay(full[0][V], 0)
                    first(full[0][K][:2], 1)

        with jax.named_scope("kv_in"):
            for p in KV:
                qkv_in(b, p)

        @pl.when(begin)
        def _():
            for p in KV:
                share_copy(b, p).start()

        with jax.named_scope("attend_fresh"):
            attend_fresh(b)

        @pl.when(begin)
        def _():
            for p in KV:
                share_copy(b, p).wait()

        o_out(b, True)

        @pl.when(begin)
        def _():
            first(share[b], 0)
            if b:
                relay(share[0], 1)
            else:
                with jax.named_scope("mod_rest"):
                    mod_rest()

        @pl.when(last)
        def _():
            with jax.named_scope("full_2"):
                if b == 0:
                    first(full[0][K][2:], 1)
                    first(full[0][V], 1)
                else:
                    relay(full[0][K], 2)
                    first(full[1][K], 1)
                    first(full[1][V], 1)
                    relay(full[0][V], 2)

        with jax.named_scope("o_in"):
            o_in(b)

        def out_body(t, tile):
            columns = pl.ds(pl.multiple_of(t * WIDE, WIDE), WIDE)
            part = [ob[:, g].reshape(2 * rows, group) for g in range(2)]
            out_own[:, columns] = dot(part[0], tile[:group]) + dot(part[1], tile[group:])
            chunk_swap(out_own, out_peer, t, out_send, out_recv).start()

        @unless_first
        def _():
            for t in range(n_out):
                chunk_swap(out_own, out_peer, t, out_send, out_recv).wait_send()

        with jax.named_scope("out"):
            tile_loop(base + 3 * n_qkv, n_out, out_body)
        if b:
            pl.when(begin)(lambda: relay(share[1], 0))
        else:
            pl.when(begin)(mod_rest_in)

        with jax.named_scope("out_swap"):
            for t in range(n_out):
                chunk_swap(out_own, out_peer, t, out_send, out_recv).wait_recv()
        with jax.named_scope("ln2"):
            add_gated(b, step, 2, out_own, out_peer)
            modulate(b, step, 3, 4)

        def up_body(t, tile):
            act[:, pl.ds(pl.multiple_of(t * TILE, TILE), TILE)] = jax.nn.gelu(deep_dot(tile), approximate=True).astype(BF16)

        def refill():
            settle(share[1 - b], 1)
            load_shared(1 - b)

        if b:
            hooks = (
                (n_up - 2, begin, refill),
                (n_up - 1, begin, lambda: first(share[1], 1)),
            )
        else:
            hooks = (
                (1, begin, lambda: relay(share[0], 0)),
                (n_up * 2 // 3, begin, lambda: first(share[0], 1)),
                (0, last, lambda: relay(full[0][K][:2], 1)),
                (n_up // 6, last, lambda: relay(full[0][K][2:], 1)),
                (n_up // 3, last, lambda: relay(full[0][V][:2], 1)),
                (n_up * 5 // 12, last, lambda: relay(share[1][2:], 1)),
                (n_up * 2 // 3, last, lambda: first(full[0][K][:2], 2)),
                (n_up * 3 // 4, last, lambda: relay(full[0][V][2:], 1)),
            )
        with jax.named_scope("up"):
            tile_loop(base + 3 * n_qkv + n_out, n_up, up_body, hooks)

        def down_body(t, tile):
            n = lax.div(t, n_deep)
            deep = lax.rem(t, n_deep)
            columns = pl.ds(pl.multiple_of(n * WIDE, WIDE), WIDE)
            part = dot(act[:, pl.ds(pl.multiple_of(deep * half, half), half)], tile[...])

            @pl.when(deep == 0)
            def _():
                down_own[:, columns] = part

            @pl.when(deep != 0)
            def _():
                down_own[:, columns] = down_own[:, columns] + part

            @pl.when(deep == n_deep - 1)
            def _():
                chunk_swap(down_own, down_peer, n, down_send, down_recv).start()

        @unless_first
        def _():
            for t in range(n_out):
                chunk_swap(down_own, down_peer, t, down_send, down_recv).wait_send()

        if b:
            hooks = (
                (n_down // 4, last, lambda: relay(full[1][K], 1)),
                (n_down // 2, last, lambda: relay(full[1][V], 1)),
            )
        else:
            hooks = ((n_down // 12, last, lambda: first(full[0][K][2:], 2)), (n_down // 2, last, refill))
        with jax.named_scope("down"):
            tile_loop(base + 3 * n_qkv + n_out + n_up, n_down, down_body, hooks)
        with jax.named_scope("down_swap"):
            for t in range(n_out):
                chunk_swap(down_own, down_peer, t, down_send, down_recv).wait_recv()
        with jax.named_scope("gate2"):
            add_gated(b, step, 5, down_own, down_peer)

    def one_step(step, carry):
        for b in range(LAYERS):
            block(step, b)
        for s in range(2):
            h[s * rows : (s + 1) * rows, :] = normed(s).astype(BF16)
        later = lax.rem(step + 1, STEPS)

        def head_body(t, tile):
            eps = deep_dot(tile).astype(BF16).astype(F32)
            with_cond, without = eps[:rows], eps[rows:]
            guided = without + sched[step, 2] * (with_cond - without)
            columns = pl.ds(pl.multiple_of(c * half + t * TILE, TILE), TILE)
            xs[later, :, columns] = sched[step, 0] * xs[step, :, columns] + sched[step, 1] * guided

        @pl.when(step > 0)
        def _():
            x_half(xs, step, c, half, x_sem, other).wait_send()

        with jax.named_scope("head"):
            tile_loop(n_ada + step * n_step + LAYERS * n_block, n_head, head_body)
        swap = x_half(xs, later, c, half, x_sem, other)
        swap.start()
        with jax.named_scope("x_swap"):
            swap.wait_recv()

        @pl.when(step == 0)
        def _():
            with jax.named_scope("relay_share"):
                relay(share[1][:2], 1)

        return carry

    lax.fori_loop(0, STEPS, one_step, 0)
    lat_out[...] = xs[0]

    with jax.named_scope("tail_c1"):
        for p in KV:
            for at in (0, 2, 1):
                first(full[1][p][at : at + 1], 2)
    with jax.named_scope("tail_c2k"):
        relay(full[1][K], 2)
    with jax.named_scope("tail_c2v"):
        relay(full[1][V], 2)
    with jax.named_scope("tail_end"):
        for b in range(LAYERS):
            for p in KV:
                settle(full[b][p], 2)
    x_half(xs, 0, c, half, x_sem, other).wait_send()
    for p in (Q, K, V):
        qkv_out(LAYERS - 1, p, False)
    o_out(LAYERS - 1, False)
    for t in range(n_out):
        chunk_swap(out_own, out_peer, t, out_send, out_recv).wait_send()
        chunk_swap(down_own, down_peer, t, down_send, down_recv).wait_send()
    for i in range(n_ada):
        for one in (*mod_ring(i, "y"), *mod_ring(i, "x"), mod_swap(i)):
            one.wait_send()
    for b in range(LAYERS):
        for ring in share[b] + full[b][K] + full[b][V]:
            for stage in ring:
                stage.drain()


def x_half(xs, at, c, half, x_sem, other):
    part = xs.at[at, :, pl.ds(pl.multiple_of(c * half, half), half)]
    return remote(part, part, x_sem.at[0], x_sem.at[1], cfg=other)


def output_kernel(lat, all_k, all_v, lat_out, k_out, v_out, buf, lat_buf, in_sem, out_sem):
    n_buf = buf.shape[0]
    pieces = [(src.at[b, z], dst.at[b, z]) for src, dst in ((all_k, k_out), (all_v, v_out)) for b in range(LAYERS) for z in range(src.shape[1])]

    def come(i):
        return pltpu.make_async_copy(pieces[i][0], buf.at[i % n_buf], in_sem.at[i % n_buf])

    def go(i):
        return pltpu.make_async_copy(buf.at[i % n_buf], pieces[i][1], out_sem.at[i % n_buf])

    lat_in = pltpu.make_async_copy(lat, lat_buf, in_sem.at[n_buf])
    lat_go = pltpu.make_async_copy(lat_buf, lat_out, out_sem.at[n_buf])
    lat_in.start()
    for i in range(n_buf):
        come(i).start()
    lat_in.wait()
    lat_go.start()
    for i in range(len(pieces)):
        come(i).wait()
        go(i).start()
        late = i - n_buf // 2
        if late >= 0 and late + n_buf < len(pieces):
            go(late).wait()
            come(late + n_buf).start()
    for i in range(max(0, len(pieces) - n_buf), len(pieces)):
        go(i).wait()
    lat_go.wait()


def output_copies(lat, all_k, all_v):
    pieces = 16
    n_buf = 24
    tall = (LAYERS, pieces, all_k.size // (LAYERS * pieces * all_k.shape[-1]), all_k.shape[-1])
    anywhere = pl.BlockSpec(memory_space=pl.ANY)
    dma = pltpu.SemaphoreType.DMA
    return pl.pallas_call(
        output_kernel,
        out_shape=(jax.ShapeDtypeStruct(lat.shape, F32), jax.ShapeDtypeStruct(tall, BF16), jax.ShapeDtypeStruct(tall, BF16)),
        in_specs=[anywhere] * 3,
        out_specs=[anywhere] * 3,
        scratch_shapes=[pltpu.VMEM((n_buf, *tall[2:]), BF16), pltpu.VMEM(lat.shape, F32), dma((n_buf + 1,)), dma((n_buf + 1,))],
        compiler_params=pltpu.CompilerParams(vmem_limit_bytes=60 * 2**20),
        name="outputs",
    )(lat, all_k.reshape(tall), all_v.reshape(tall))


def denoise(lat, cond, sched, w_ada, w_qkv, w_out, w_up, w_down, w_head, k_old, v_old):
    rows, width = lat.shape
    group = width // RING
    hidden = w_up.shape[2] // 2
    torus = (RING, RING, RING)
    cache = jax.ShapeDtypeStruct((LAYERS, *torus, rows, width), BF16)
    k_old = k_old.reshape(cache.shape)
    v_old = v_old.reshape(cache.shape)
    w_out = w_out.reshape(LAYERS, width, width)
    n_out = width // WIDE
    anywhere = pl.BlockSpec(memory_space=pl.ANY)
    vmem = pl.BlockSpec(memory_space=pltpu.VMEM)
    dma = pltpu.SemaphoreType.DMA
    n_heads = group // HEAD
    n_ada = 3
    lat_out, all_k, all_v, _ = pl.pallas_call(
        denoise_kernel,
        out_shape=(
            jax.ShapeDtypeStruct((rows, width), F32),
            cache,
            cache,
            jax.ShapeDtypeStruct((LAYERS, 2, *torus, rows, group), BF16),
        ),
        in_specs=[anywhere, anywhere, pl.BlockSpec(memory_space=pltpu.SMEM)] + [anywhere] * 8,
        out_specs=[vmem, anywhere, anywhere, anywhere],
        scratch_shapes=[
            pltpu.VMEM((BUFFERS, width // 2, WIDE), BF16),
            pltpu.VMEM((*torus, rows, group), BF16),
            pltpu.VMEM((*torus, rows, group), BF16),
            pltpu.VMEM((rows, width), BF16),
            pltpu.VMEM((STEPS, width), F32),
            pltpu.VMEM((STEPS, rows, width), F32),
            pltpu.VMEM((2 * rows, width), F32),
            pltpu.VMEM((2 * rows, width), BF16),
            pltpu.VMEM((2 * rows, hidden), BF16),
            pltpu.VMEM((2 * rows, width), F32),
            pltpu.VMEM((2 * rows, width), F32),
            pltpu.VMEM((2 * rows, width), F32),
            pltpu.VMEM((2 * rows, width), F32),
            pltpu.VMEM((2, 2, 3, rows, group), BF16),
            pltpu.VMEM((LAYERS, 3, RING, rows, group), BF16),
            pltpu.VMEM((RING * rows, group), F32),
            pltpu.VMEM((n_heads, RING * rows, HEAD), F32),
            pltpu.VMEM((n_heads, RING * rows, HEAD), F32),
            pltpu.VMEM((RING, rows, group), BF16),
            pltpu.VMEM((2, 2, rows, group), BF16),
            pltpu.VMEM((LAYERS, n_ada, RING, RING, 2 * STEPS, width // 8), F32),
            pltpu.VMEM((STEPS, width), F32),
            pltpu.VMEM((2, RING * rows, RING**3 * rows), F32),
            dma((BUFFERS,)),
            dma((2,)),
            dma((2,)),
            dma((2,)),
            dma((n_ada, 2 * RING - 1)),
            dma((n_ada, 2 * RING - 1)),
            dma((3, 2, 2)),
            dma((LAYERS, 3, RING)),
            dma((RING,)),
            dma((2, 2)),
            dma((n_out,)),
            dma((n_out,)),
            dma((n_out,)),
            dma((n_out,)),
            dma((2,)),
            dma((2,)),
            dma((LAYERS, 2, 2, 2, 4)),
            dma((LAYERS, 2, 2, 2, 4)),
            dma((2, 2)),
            dma((2, 2)),
            dma((2, 2)),
            dma((LAYERS, 2, 3, 3, 4)),
            dma((LAYERS, 2, 3, 3, 4)),
        ],
        compiler_params=pltpu.CompilerParams(collective_id=0, has_side_effects=True, vmem_limit_bytes=63 * 2**20),
        name="denoise",
    )(lat, cond, sched.T, w_ada, w_qkv, w_out, w_up, w_down, w_head, k_old, v_old)
    tokens = RING**3 * rows
    lat_out, k_new, v_new = output_copies(lat_out, all_k, all_v)
    return lat_out, k_new.reshape(LAYERS, tokens, width), v_new.reshape(LAYERS, tokens, width)


def solution(mesh):
    slot_spec = P(("img", "cfg"), None, None)
    cache_spec = P(("img", "cfg"), None, None, None)
    rep_spec = P()

    def local_step(latent, cond_vec, sched_coef, w_ada, w_qkv, w_out, w_up, w_down, w_head, k_stale, v_stale):
        lat_out, k_new, v_new = denoise(
            latent[0], cond_vec[0], sched_coef, w_ada, w_qkv, w_out, w_up, w_down, w_head, k_stale[0], v_stale[0]
        )
        return lat_out[None], k_new[None], v_new[None]

    return jax.shard_map(
        local_step,
        mesh=mesh,
        in_specs=(P("img", "patch", None), slot_spec, rep_spec, rep_spec, rep_spec, rep_spec, rep_spec, rep_spec, rep_spec, cache_spec, cache_spec),
        out_specs=(P(("img", "cfg"), "patch", None), cache_spec, cache_spec),
        check_vma=False,
    )
```

```python
import functools

import jax
import jax.numpy as jnp
from jax import lax
from jax.experimental import pallas as pl
from jax.experimental.pallas import tpu as pltpu
from jax.sharding import PartitionSpec as P

RING = 4
AXES = ("z", "y", "x")
COLOR_ORDERS = (("x", "y", "z"), ("y", "z", "x"), ("z", "x", "y"))
HEAD_AXES = ("z", "y")
MESH = pl.DeviceIdType.MESH
F32 = jnp.float32
BF16 = jnp.bfloat16
HEAD = 128
TILE = 512
SUB = 256
WIDE = 2 * TILE
BUFFERS = 12
STEPS = 2
LAYERS = 2
Q, K, V = 0, 1, 2
KV = (K, V)


def dot(lhs, rhs):
    return jnp.dot(lhs, rhs, preferred_element_type=F32)


def scoped(name, action):
    def inside():
        with jax.named_scope(name):
            action()

    return inside


def torus_position():
    patch = lax.axis_index("patch")
    return {"z": lax.div(patch, RING * RING), "y": lax.rem(lax.div(patch, RING), RING), "x": lax.rem(patch, RING)}


def patch_at(pos):
    return (pos["z"] * RING + pos["y"]) * RING + pos["x"]


class Torus:
    def __init__(self):
        self.pos = torus_position()
        self.coord, self.patch = {}, {}
        for axis in AXES:
            for by in range(1, RING):
                coord = lax.rem(self.pos[axis] + by, RING)
                self.coord[axis, by] = coord
                self.patch[axis, by] = patch_at({**self.pos, axis: coord})


def remote(src, dst, send_sem, recv_sem, **device_id):
    return pltpu.make_async_remote_copy(
        src_ref=src, dst_ref=dst, send_sem=send_sem, recv_sem=recv_sem, device_id=device_id, device_id_type=MESH
    )


class Ring:
    def __init__(self, torus, axis, view, send_sem, recv_sem):
        me, succ, prev = torus.pos[axis], torus.coord[axis, 1], torus.coord[axis, RING - 1]
        ahead, behind = torus.patch[axis, 1], torus.patch[axis, RING - 1]
        self.sends = ((me, None, ahead), (me, None, behind), (prev, 0, ahead), (succ, 1, behind))
        self.parts = (view, send_sem, recv_sem)

    def copy(self, slot):
        view, send_sem, recv_sem = self.parts
        coord, half, patch = self.sends[slot]
        part = view(coord, half)
        return remote(part, part, send_sem(slot), recv_sem(slot), patch=patch)

    def first(self):
        for slot in (0, 1):
            self.copy(slot).start()

    def relay(self):
        for slot in (0, 1):
            self.copy(slot).wait_recv()
            self.copy(slot + 2).start()

    def settle(self):
        for slot in (2, 3):
            self.copy(slot).wait_recv()

    def drain(self):
        for slot in range(4):
            self.copy(slot).wait_send()


def full_rings(ref, color, torus, send_sem, recv_sem):
    width = ref.shape[4]
    cut = [0, width // 3 // SUB * SUB, width // 3 // SUB * SUB * 2, width]
    base, size = cut[color], cut[color + 1] - cut[color]
    order = COLOR_ORDERS[color]

    def stage(k):
        axis = order[k]

        def view(coord, half):
            index = []
            for name in AXES:
                index.append(coord if name == axis else slice(None) if name in order[:k] else torus.pos[name])
            columns = pl.ds(base, size) if half is None else pl.ds(base + half * (size // 2), size // 2)
            return ref.at[(*index, slice(None), columns)]

        return Ring(torus, axis, view, lambda slot: send_sem.at[k, slot], lambda slot: recv_sem.at[k, slot])

    return [stage(k) for k in range(3)]


def share_rings(ref, head_axis, color, torus, send_sem, recv_sem):
    size = ref.shape[4] // 2
    rest = [axis for axis in AXES if axis != head_axis]
    order = rest if color else rest[::-1]
    columns = pl.ds(color * size, size)

    def stage(k):
        axis = order[k]

        def view(coord, half):
            index = []
            for name in AXES:
                if name == head_axis:
                    index.append(slice(None) if half is None else pl.ds(half * (RING // 2), RING // 2))
                else:
                    index.append(coord if name == axis else slice(None) if name in order[:k] else torus.pos[name])
            return ref.at[(*index, slice(None), columns)]

        return Ring(torus, axis, view, lambda slot: send_sem.at[k, slot], lambda slot: recv_sem.at[k, slot])

    return [stage(k) for k in range(2)]


def denoise_kernel(
    lat, cond, sched, w_ada, w_qkv, w_out, w_up, w_down, w_head, k_old, v_old,
    lat_out, all_k, all_v, shared,
    wbuf, kbuf, vbuf, lat_own, cond_own, xs, r, h, act, out_own, out_peer, down_own, down_peer, sb, rb, o_sum, o_top, o_total, o_own, ob, mod,
    cond_peer, scores,
    w_sem, in_sem, kv_sem, cond_sem, mod_send, mod_recv, qkv_send, qkv_recv, o_send, o_recv, out_send, out_recv, down_send, down_recv,
    x_sem, share_put, share_send, share_recv, own_put, own_send, own_recv, full_send, full_recv,
):
    rows, width = lat.shape
    half = width // 2
    group = width // RING
    chunk = width // 8
    hidden = w_up.shape[2] // 2
    n_qkv = half // TILE
    n_out = width // WIDE
    n_up = hidden // TILE
    n_deep = hidden // half
    n_down = n_out * n_deep
    n_head = half // TILE
    n_block = 3 * n_qkv + n_out + n_up + n_down
    n_step = LAYERS * n_block + n_head
    n_ada = 3
    n_buf = wbuf.shape[0]
    scale = HEAD**-0.5

    c = lax.axis_index("cfg")
    other = 1 - c
    mod_block = other
    torus = Torus()
    z, y, x = (torus.pos[axis] for axis in AXES)
    line = [torus.pos[axis] for axis in HEAD_AXES]
    line_core = [lax.div(at, 2) for at in line]
    line_odd = [lax.rem(at, 2) for at in line]

    def line_patch(b, at):
        return patch_at({**torus.pos, HEAD_AXES[b]: at})

    def line_rows(ref, b):
        return ref.at[tuple(slice(None) if axis == HEAD_AXES[b] else torus.pos[axis] for axis in AXES)]


    def put(src, dst, slot):
        pltpu.make_async_copy(src, dst, w_sem.at[slot]).start()

    def put_deep(ref, col, slot):
        col = pl.multiple_of(col, TILE)
        for k in range(2):
            put(ref.at[pl.ds(k * half, half), pl.ds(col, TILE)], wbuf.at[slot, :, pl.ds(k * TILE, TILE)], slot)

    def put_wide(ref, row, col, slot):
        row = pl.multiple_of(row, half)
        col = pl.multiple_of(col, WIDE)
        put(ref.at[pl.ds(row, half), pl.ds(col, WIDE)], wbuf.at[slot], slot)

    def issue_ada(i):
        col = pl.multiple_of(i * 2 * width + (y * RING + x) * chunk, chunk)
        for k in range(2):
            put(w_ada.at[mod_block, pl.ds(k * half, half), pl.ds(col, chunk)], wbuf.at[i, :, pl.ds(k * chunk, chunk)], i)

    assert 3 * n_qkv + n_out == n_up == n_down == n_head + 3 * n_qkv == n_buf

    def qkv_tile(layer, j, slot):
        put_deep(w_qkv.at[layer], lax.div(j, n_qkv) * width + c * half + lax.rem(j, n_qkv) * TILE, slot)

    def out_tile(layer, j, slot):
        put_wide(w_out.at[layer], c * half, j * WIDE, slot)

    def up_tile(layer, j, slot):
        put_deep(w_up.at[layer], c * hidden + j * TILE, slot)

    def down_tile(layer, j, slot):
        put_wide(w_down.at[layer], c * hidden + lax.rem(j, n_deep) * half, lax.div(j, n_deep) * WIDE, slot)

    def head_tile(j, slot):
        put_deep(w_head, c * half + j * TILE, slot)

    def run_hooks(t, hooks):
        if not hooks:
            return
        tests = [(t == at) & when for at, when, _ in hooks]

        @pl.when(functools.reduce(jnp.logical_or, tests))
        def _():
            for test, (_, _, action) in zip(tests, hooks):
                pl.when(test)(scoped("hook", action))

    def tile_loop(base, count, body, ahead, hooks=()):
        def one(t, carry):
            slot = lax.rem(base + t, n_buf)
            tile = wbuf.at[slot]
            pltpu.make_async_copy(tile, tile, w_sem.at[slot]).wait()
            body(t, tile)
            ahead(t, slot)
            run_hooks(t, hooks)
            return carry

        lax.fori_loop(0, count, one, 0)

    def deep_dot(tile):
        return dot(h[:, :half], tile[:, :TILE]) + dot(h[:, half:], tile[:, TILE:])

    def load_kv(old_k, old_v):
        pltpu.make_async_copy(old_k, kbuf, kv_sem.at[0]).start()
        pltpu.make_async_copy(old_v, vbuf, kv_sem.at[1]).start()

    def load_stale(b):
        columns = pl.ds(pl.multiple_of(line[b] * group, group), group)
        load_kv(k_old.at[b, :, :, :, :, columns], v_old.at[b, :, :, :, :, columns])

    def load_shared(b):
        load_kv(shared.at[b, 0], shared.at[b, 1])

    share = [
        [share_rings(shared.at[b, i], HEAD_AXES[b], color, torus, share_send.at[b, i, color], share_recv.at[b, i, color]) for i in range(2) for color in range(2)]
        for b in range(LAYERS)
    ]
    full = [
        {
            p: [full_rings(ref.at[b], color, torus, full_send.at[b, p - K, color], full_recv.at[b, p - K, color]) for color in (2, 0, 1)]
            for p, ref in ((K, all_k), (V, all_v))
        }
        for b in range(LAYERS)
    ]

    def first(rings, k):
        for ring in rings:
            if k:
                ring[k - 1].settle()
            ring[k].first()

    def relay(rings, k):
        for ring in rings:
            ring[k].relay()

    def settle(rings, k):
        for ring in rings:
            ring[k].settle()

    barrier = pltpu.get_barrier_semaphore()

    def announce(**device_id):
        pl.semaphore_signal(barrier, inc=1, device_id=device_id, device_id_type=MESH)

    announce(cfg=other)
    for by in range(1, RING):
        for axis in HEAD_AXES:
            for core in range(2):
                announce(patch=torus.patch[axis, by], cfg=core)
        announce(patch=torus.patch["x", by])
    cond_in = pltpu.make_async_copy(cond, cond_own, in_sem.at[0])
    cond_in.start()
    for i in range(n_ada):
        issue_ada(i)
    lat_in = pltpu.make_async_copy(lat, lat_own, in_sem.at[1])
    lat_in.start()
    cond_in.wait()
    with jax.named_scope("barrier"):
        pl.semaphore_wait(barrier, 1 + 5 * (RING - 1))

    cond_swap = remote(cond_own, cond_peer, cond_sem.at[0], cond_sem.at[1], cfg=other)
    cond_swap.start()
    lat_in.wait()
    xs[0] = lat_own[...].astype(F32)
    with jax.named_scope("cond_swap"):
        cond_swap.wait()
    mine, theirs = cond_own[...], cond_peer[...]
    both = jnp.concatenate([jnp.where(c == 0, mine, theirs), jnp.where(c == 0, theirs, mine)], axis=0)
    silu = (both * jax.nn.sigmoid(both)).astype(BF16)

    def mod_ring(i, axis):
        part, base = (mod.at[mod_block, i, y, x], 0) if axis == "y" else (mod.at[mod_block, i, :, x], RING - 1)
        return [
            remote(part, part, mod_send.at[i, base + by - 1], mod_recv.at[i, base + by - 1], patch=torus.patch[axis, by]) for by in range(1, RING)
        ]

    def mod_swap(i):
        return remote(mod.at[mod_block, i], mod.at[mod_block, i], mod_send.at[i, 2 * RING - 2], mod_recv.at[i, 2 * RING - 2], cfg=other)

    def mod_go(i, axis):
        for one in mod_ring(i, axis):
            one.start()

    def mod_wait(i, axis):
        for one in mod_ring(i, axis):
            one.wait_recv()

    for i in range(n_ada):
        with jax.named_scope("ada_wait"):
            filled = wbuf.at[i, :, pl.ds(0, 2 * chunk)]
            pltpu.make_async_copy(filled, filled, w_sem.at[i]).wait()
        if i == 0:
            for n in range(n_ada, n_buf):
                qkv_tile(0, jnp.int32(n - n_ada), n)
            load_stale(0)
        tile = wbuf.at[i]
        mod[mod_block, i, y, x] = dot(silu[:, :half], tile[:, :chunk]) + dot(silu[:, half:], tile[:, chunk : 2 * chunk])
        mod_go(i, "y")
        out_tile(0, jnp.int32(i), i)
    with jax.named_scope("mod_y"):
        for i in range(n_ada):
            mod_wait(i, "y")
            mod_go(i, "x")

    def mod_pass(i):
        mod_wait(i, "x")
        mod_swap(i).start()

    @pl.when(c == 1)
    def _():
        with jax.named_scope("mod_x"):
            mod_pass(0)

    @pl.when(c == 0)
    def _():
        with jax.named_scope("mod_swap"):
            mod_swap(0).wait_recv()

    def mod_rest():
        pl.when(c == 0)(lambda: mod_pass(0))
        for i in range(1, n_ada):
            mod_pass(i)

    def mod_rest_in():
        pl.when(c == 1)(lambda: mod_swap(0).wait_recv())
        for i in range(1, n_ada):
            mod_swap(i).wait_recv()

    def mod_row(b, step, which, i, s):
        at = which % 2 * 8 + i
        both = mod[b, which // 2, at // RING, at % RING, s * STEPS : (s + 1) * STEPS, :]
        return jnp.where(step == 0, both[0:1], both[1:2])

    def normed(s):
        values = r[s * rows : (s + 1) * rows, :]
        centered = values - jnp.mean(values, -1, keepdims=True)
        return centered * lax.rsqrt(jnp.mean(centered * centered, -1, keepdims=True) + 1e-6)

    def modulate(b, step, shift, gain):
        for s in range(2):
            values = normed(s)
            for i in range(8):
                at = slice(i * chunk, (i + 1) * chunk)
                part = values[:, at] * (1.0 + mod_row(b, step, gain, i, s)) + mod_row(b, step, shift, i, s)
                h[s * rows : (s + 1) * rows, at] = part.astype(BF16)

    def add_gated(b, step, gate, own, peer):
        for s in range(2):
            for i in range(8):
                at = (slice(s * rows, (s + 1) * rows), slice(i * chunk, (i + 1) * chunk))
                r[at] = r[at] + mod_row(b, step, gate, i, s) * (own[at] + peer[at])

    def chunk_swap(own, peer, t, send_sem, recv_sem):
        columns = pl.ds(pl.multiple_of(t * WIDE, WIDE), WIDE)
        return remote(own.at[:, columns], peer.at[:, columns], send_sem.at[t], recv_sem.at[t], cfg=other)

    def qkv_copy(b, p, s, g):
        return remote(sb.at[s, g, p], rb.at[b, p, line[b]], qkv_send.at[p, s, g], qkv_recv.at[b, p, line[b]], patch=line_patch(b, 2 * c + g), cfg=s)

    def qkv_out(b, p, do_send):
        for s in range(2):
            for g in range(2):
                if do_send:

                    @pl.when((2 * c + g == line[b]) & (c == s))
                    def _():
                        rb[b, p, line[b]] = sb[s, g, p]

                @pl.when((2 * c + g != line[b]) | (c != s))
                def _():
                    if do_send:
                        qkv_copy(b, p, s, g).start()
                    else:
                        qkv_copy(b, p, s, g).wait_send()

    def qkv_in(b, p):
        for src in range(RING):

            @pl.when((line[b] != src) | (c != line_core[b]))
            def _():
                part = rb.at[b, p, src]
                remote(part, part, qkv_send.at[p, 0, 0], qkv_recv.at[b, p, src], cfg=other).wait_recv()

    def qkv_part(b, p, base, hooks=()):
        def body(t, tile):
            part = deep_dot(tile).astype(BF16)
            for k in range(TILE // SUB):
                col = t * TILE + k * SUB
                g = lax.div(col, group)
                columns = pl.ds(pl.multiple_of(col - g * group, SUB), SUB)
                for s in range(2):
                    sb[s, g, p, :, columns] = part[s * rows : (s + 1) * rows, k * SUB : (k + 1) * SUB]

        tile_loop(base + p * n_qkv, n_qkv, body, lambda t, slot: up_tile(b, p * n_qkv + t, slot), hooks)

    def own_copies(b, p):
        local, swap = [], []
        for g in range(2):
            columns = pl.ds(pl.multiple_of(c * half + g * group, group), group)
            place = (all_k if p == K else all_v).at[b, z, y, x, :, columns]
            local.append(pltpu.make_async_copy(sb.at[c, g, p], place, own_put.at[p - K, g]))
            swap.append(remote(sb.at[other, g, p], place, own_send.at[p - K, g], own_recv.at[p - K, g], cfg=other))
        return local + swap

    def own_start(b, p):
        for one in own_copies(b, p):
            one.start()

    def own_wait(b, p):
        for one in own_copies(b, p):
            one.wait()

    def share_copy(b, p):
        return pltpu.make_async_copy(rb.at[b, p], line_rows(shared.at[b, p - K], b), share_put.at[p - K])

    tokens_z = RING * RING * rows
    n_rows = RING * rows

    n_heads = group // HEAD

    def scored(queries, keys):
        return lax.dot_general(queries, keys, (((1,), (1,)), ((), ())), preferred_element_type=F32)

    def patch_of(shape, axis):
        index = lax.broadcasted_iota(jnp.int32, shape, axis)
        return lax.div(index, jnp.full_like(index, rows))

    def attend_cache(b, hooks):
        own_patch = line_patch(b, patch_of((n_rows, tokens_z), 0))
        key_patch = patch_of((n_rows, tokens_z), 1)

        together = 2

        def one(step, carry):
            heads = [step * together + j for j in range(together)]
            columns = [pl.ds(pl.multiple_of(head * HEAD, HEAD), HEAD) for head in heads]
            queries = [rb[b, Q, :, :, at].reshape(n_rows, HEAD) for at in columns]
            tops, totals, mixed = [None] * together, [None] * together, [None] * together
            for plane in range(RING):
                planes = slice(plane * tokens_z, (plane + 1) * tokens_z)
                hidden_keys = key_patch + plane * RING * RING == own_patch
                for j, at in enumerate(columns):
                    part = scored(queries[j], kbuf[plane, :, :, :, at].reshape(tokens_z, HEAD))
                    part = jnp.where(hidden_keys, -jnp.inf, part)
                    scores[j, :, planes] = part
                    best = jnp.max(part, -1, keepdims=True)
                    tops[j] = best if plane == 0 else jnp.maximum(tops[j], best)
            for plane in range(RING):
                planes = slice(plane * tokens_z, (plane + 1) * tokens_z)
                for j, at in enumerate(columns):
                    weights = jnp.exp((scores[j, :, planes] - tops[j]) * scale)
                    add = jnp.sum(weights, -1, keepdims=True)
                    more = dot(weights.astype(BF16), vbuf[plane, :, :, :, at].reshape(tokens_z, HEAD))
                    totals[j] = add if plane == 0 else totals[j] + add
                    mixed[j] = more if plane == 0 else mixed[j] + more
            for j, (head, at) in enumerate(zip(heads, columns)):
                o_sum[:, at] = mixed[j]
                o_top[head] = jnp.broadcast_to(tops[j], (n_rows, HEAD))
                o_total[head] = jnp.broadcast_to(totals[j], (n_rows, HEAD))
            run_hooks(step, [(when_at // together, when, hook) for when_at, when, hook in hooks])
            return carry

        for i in range(2):
            buf = (kbuf, vbuf)[i]
            pltpu.make_async_copy(buf, buf, kv_sem.at[i]).wait()
        lax.fori_loop(0, n_heads // together, one, 0)

    def attend_fresh(b):
        same = patch_of((n_rows, n_rows), 0) == patch_of((n_rows, n_rows), 1)
        for start in range(0, n_heads, 3):
            heads = range(start, min(start + 3, n_heads))
            columns = [slice(head * HEAD, (head + 1) * HEAD) for head in heads]
            parts = [scored(rb[b, Q, :, :, at].reshape(n_rows, HEAD), rb[b, K, :, :, at].reshape(n_rows, HEAD)) for at in columns]
            parts = [jnp.where(same, part, -jnp.inf) for part in parts]
            tops = [jnp.maximum(o_top[head], jnp.max(part, -1, keepdims=True)) for head, part in zip(heads, parts)]
            weights = [jnp.exp((part - top) * scale) for part, top in zip(parts, tops)]
            fresh = [dot(weight.astype(BF16), rb[b, V, :, :, at].reshape(n_rows, HEAD)) for weight, at in zip(weights, columns)]
            shrink = [jnp.exp((o_top[head] - top) * scale) for head, top in zip(heads, tops)]
            totals = [o_total[head] * less + jnp.sum(weight, -1, keepdims=True) for head, less, weight in zip(heads, shrink, weights)]
            for at, less, more, total in zip(columns, shrink, fresh, totals):
                o_own[:, :, at] = ((o_sum[:, at] * less + more) / total).astype(BF16).reshape(RING, rows, HEAD)

    def o_copy(b, dst):
        return remote(
            o_own.at[dst], ob.at[c, line_odd[b]], o_send.at[dst], o_recv.at[c, line_odd[b]], patch=line_patch(b, dst), cfg=line_core[b]
        )

    def o_out(b, do_send):
        for dst in range(RING):
            if do_send:

                @pl.when((line[b] == dst) & (c == line_core[b]))
                def _():
                    ob[c, line_odd[b]] = o_own[dst]

            @pl.when((line[b] != dst) | (c != line_core[b]))
            def _():
                if do_send:
                    o_copy(b, dst).start()
                else:
                    o_copy(b, dst).wait_send()

    def o_in(b):
        for s in range(2):
            for g in range(2):

                @pl.when((2 * c + g != line[b]) | (c != s))
                def _():
                    part = ob.at[s, g]
                    remote(part, part, o_send.at[0], o_recv.at[s, g], cfg=other).wait_recv()

    def block(step, b):
        base = n_ada + step * n_step + b * n_block
        begin = step == 0
        last = step == STEPS - 1

        def unless_first(action):
            if b:
                action()
            else:
                pl.when(step > 0)(action)

        def gather_own(p):
            own_wait(b, p)
            first(full[b][p], 0)

        def send_late():
            gather_own(V)
            for p in KV:
                qkv_out(b, p, True)

        if b == 0:
            for s in range(2):
                r[s * rows : (s + 1) * rows, :] = xs[step]
        with jax.named_scope("ln1"):
            modulate(b, step, 0, 1)

        @unless_first
        def _():
            for p in (Q, K, V):
                qkv_out(1 - b, p, False)

        with jax.named_scope("qkv_q"):
            qkv_part(b, Q, base)
        qkv_out(b, Q, True)
        with jax.named_scope("qkv_k"):
            qkv_part(b, K, base)
        pl.when(begin)(lambda: qkv_out(b, K, True))

        @pl.when(last)
        def _():
            own_start(b, K)

        with jax.named_scope("qkv_v"):
            qkv_part(b, V, base, ((n_qkv - 1, last, lambda: gather_own(K)),))

        pl.when(begin)(lambda: qkv_out(b, V, True))

        @pl.when(last)
        def _():
            own_start(b, V)
            if b:
                with jax.named_scope("full_1a"):
                    send_late()
                    first(full[0][V], 2)
                    relay(full[1][K], 0)
                    relay(full[1][V], 0)

        with jax.named_scope("q_in"):
            qkv_in(b, Q)

        @unless_first
        def _():
            o_out(1 - b, False)

        hooks = () if b else ((min(1, n_heads - 2), last, send_late), (max(n_heads - 2, 1), last, lambda: relay(full[0][K], 0)))
        with jax.named_scope("attend_cache"):
            attend_cache(b, hooks)
        if b == 0:
            pl.when(begin)(lambda: load_stale(1))

            @pl.when(last)
            def _():
                with jax.named_scope("full_1"):
                    relay(full[0][V], 0)
                    first(full[0][K][:2], 1)

        with jax.named_scope("kv_in"):
            for p in KV:
                qkv_in(b, p)

        @pl.when(begin)
        def _():
            for p in KV:
                share_copy(b, p).start()

        with jax.named_scope("attend_fresh"):
            attend_fresh(b)

        @pl.when(begin)
        def _():
            for p in KV:
                share_copy(b, p).wait()

        o_out(b, True)

        @pl.when(begin)
        def _():
            first(share[b], 0)
            if b:
                relay(share[0], 1)
            else:
                with jax.named_scope("mod_rest"):
                    mod_rest()

        @pl.when(last)
        def _():
            with jax.named_scope("full_2"):
                if b == 0:
                    first(full[0][K][2:], 1)
                    first(full[0][V], 1)
                else:
                    relay(full[0][K], 2)
                    first(full[1][K], 1)
                    first(full[1][V], 1)
                    relay(full[0][V], 2)

        with jax.named_scope("o_in"):
            o_in(b)

        def out_body(t, tile):
            columns = pl.ds(pl.multiple_of(t * WIDE, WIDE), WIDE)
            part = [ob[:, g].reshape(2 * rows, group) for g in range(2)]
            out_own[:, columns] = dot(part[0], tile[:group]) + dot(part[1], tile[group:])
            chunk_swap(out_own, out_peer, t, out_send, out_recv).start()

        @unless_first
        def _():
            for t in range(n_out):
                chunk_swap(out_own, out_peer, t, out_send, out_recv).wait_send()

        with jax.named_scope("out"):
            tile_loop(base + 3 * n_qkv, n_out, out_body, lambda t, slot: up_tile(b, 3 * n_qkv + t, slot))
        if b:
            pl.when(begin)(lambda: relay(share[1], 0))
        else:
            pl.when(begin)(mod_rest_in)

        with jax.named_scope("out_swap"):
            for t in range(n_out):
                chunk_swap(out_own, out_peer, t, out_send, out_recv).wait_recv()
        with jax.named_scope("ln2"):
            add_gated(b, step, 2, out_own, out_peer)
            modulate(b, step, 3, 4)

        def up_body(t, tile):
            act[:, pl.ds(pl.multiple_of(t * TILE, TILE), TILE)] = jax.nn.gelu(deep_dot(tile), approximate=True).astype(BF16)

        def refill():
            settle(share[1 - b], 1)
            load_shared(1 - b)

        if b:
            hooks = ()
        else:
            hooks = (
                (1, begin, lambda: relay(share[0], 0)),
                (n_up * 2 // 3, begin, lambda: first(share[0], 1)),
                (0, last, lambda: relay(full[0][K][:2], 1)),
                (n_up // 6, last, lambda: relay(full[0][K][2:], 1)),
                (n_up // 3, last, lambda: relay(full[0][V][:2], 1)),
                (n_up * 5 // 12, last, lambda: relay(share[1][2:], 1)),
                (n_up * 2 // 3, last, lambda: first(full[0][K][:2], 2)),
                (n_up * 3 // 4, last, lambda: relay(full[0][V][2:], 1)),
            )
        with jax.named_scope("up"):
            tile_loop(base + 3 * n_qkv + n_out, n_up, up_body, lambda t, slot: down_tile(b, t, slot), hooks)

        def down_body(t, tile):
            n = lax.div(t, n_deep)
            deep = lax.rem(t, n_deep)
            columns = pl.ds(pl.multiple_of(n * WIDE, WIDE), WIDE)
            part = dot(act[:, pl.ds(pl.multiple_of(deep * half, half), half)], tile[...])

            down_own[:, columns] = jnp.where(deep == 0, 0.0, down_own[:, columns]) + part

            @pl.when(deep == n_deep - 1)
            def _():
                chunk_swap(down_own, down_peer, n, down_send, down_recv).start()

        @unless_first
        def _():
            for t in range(n_out):
                chunk_swap(down_own, down_peer, t, down_send, down_recv).wait_send()

        if b:
            hooks = (
                (n_down // 6, begin, lambda: first(share[1], 1)),
                (n_down // 3, begin, refill),
                (n_down // 4, last, lambda: relay(full[1][K], 1)),
                (n_down // 2, last, lambda: relay(full[1][V], 1)),
            )
        else:
            hooks = ((n_down // 12, last, lambda: first(full[0][K][2:], 2)), (n_down // 2, last, refill))
        n_first = n_head if b else 3 * n_qkv

        def after_down(t, slot):
            @pl.when(t < n_first)
            def _():
                if b:
                    head_tile(t, slot)
                else:
                    qkv_tile(1, t, slot)

            @pl.when((t >= n_first) & begin if b else t >= n_first)
            def _():
                if b:
                    qkv_tile(0, t - n_first, slot)
                else:
                    out_tile(1, t - n_first, slot)

        with jax.named_scope("down"):
            tile_loop(base + 3 * n_qkv + n_out + n_up, n_down, down_body, after_down, hooks)
        with jax.named_scope("down_swap"):
            for t in range(n_out):
                chunk_swap(down_own, down_peer, t, down_send, down_recv).wait_recv()
        with jax.named_scope("gate2"):
            add_gated(b, step, 5, down_own, down_peer)

    def one_step(step, carry):
        for b in range(LAYERS):
            block(step, b)
        for s in range(2):
            h[s * rows : (s + 1) * rows, :] = normed(s).astype(BF16)
        later = lax.rem(step + 1, STEPS)

        def head_body(t, tile):
            eps = deep_dot(tile).astype(BF16).astype(F32)
            with_cond, without = eps[:rows], eps[rows:]
            guided = without + sched[step, 2] * (with_cond - without)
            columns = pl.ds(pl.multiple_of(c * half + t * TILE, TILE), TILE)
            xs[later, :, columns] = sched[step, 0] * xs[step, :, columns] + sched[step, 1] * guided

        @pl.when(step > 0)
        def _():
            x_half(xs, step, c, half, x_sem, other).wait_send()

        with jax.named_scope("head"):
            tile_loop(
                n_ada + step * n_step + LAYERS * n_block,
                n_head,
                head_body,
                lambda t, slot: pl.when(step == 0)(lambda: out_tile(0, t, slot)),
            )
        swap = x_half(xs, later, c, half, x_sem, other)
        swap.start()
        with jax.named_scope("x_swap"):
            swap.wait_recv()

        @pl.when(step == 0)
        def _():
            with jax.named_scope("relay_share"):
                relay(share[1][:2], 1)

        return carry

    lax.fori_loop(0, STEPS, one_step, 0)
    lat_out[...] = xs[0]

    with jax.named_scope("tail_c1"):
        for p in KV:
            for at in (0, 2, 1):
                first(full[1][p][at : at + 1], 2)
    with jax.named_scope("tail_c2k"):
        relay(full[1][K], 2)
    with jax.named_scope("tail_c2v"):
        relay(full[1][V], 2)
    with jax.named_scope("tail_end"):
        for b in range(LAYERS):
            for p in KV:
                settle(full[b][p], 2)
    x_half(xs, 0, c, half, x_sem, other).wait_send()
    for p in (Q, K, V):
        qkv_out(LAYERS - 1, p, False)
    o_out(LAYERS - 1, False)
    for t in range(n_out):
        chunk_swap(out_own, out_peer, t, out_send, out_recv).wait_send()
        chunk_swap(down_own, down_peer, t, down_send, down_recv).wait_send()
    for i in range(n_ada):
        for one in (*mod_ring(i, "y"), *mod_ring(i, "x"), mod_swap(i)):
            one.wait_send()
    for b in range(LAYERS):
        for ring in share[b] + full[b][K] + full[b][V]:
            for stage in ring:
                stage.drain()


def x_half(xs, at, c, half, x_sem, other):
    part = xs.at[at, :, pl.ds(pl.multiple_of(c * half, half), half)]
    return remote(part, part, x_sem.at[0], x_sem.at[1], cfg=other)


def output_kernel(lat, all_k, all_v, lat_out, k_out, v_out, buf, lat_buf, in_sem, out_sem):
    n_buf = buf.shape[0]
    pieces = [(src.at[b, z], dst.at[b, z]) for src, dst in ((all_k, k_out), (all_v, v_out)) for b in range(LAYERS) for z in range(src.shape[1])]

    def come(i):
        return pltpu.make_async_copy(pieces[i][0], buf.at[i % n_buf], in_sem.at[i % n_buf])

    def go(i):
        return pltpu.make_async_copy(buf.at[i % n_buf], pieces[i][1], out_sem.at[i % n_buf])

    lat_in = pltpu.make_async_copy(lat, lat_buf, in_sem.at[n_buf])
    lat_go = pltpu.make_async_copy(lat_buf, lat_out, out_sem.at[n_buf])
    lat_in.start()
    for i in range(n_buf):
        come(i).start()
    lat_in.wait()
    lat_go.start()
    for i in range(len(pieces)):
        come(i).wait()
        go(i).start()
        late = i - n_buf // 2
        if late >= 0 and late + n_buf < len(pieces):
            go(late).wait()
            come(late + n_buf).start()
    for i in range(max(0, len(pieces) - n_buf), len(pieces)):
        go(i).wait()
    lat_go.wait()


def output_copies(lat, all_k, all_v):
    pieces = 16
    n_buf = 24
    tall = (LAYERS, pieces, all_k.size // (LAYERS * pieces * all_k.shape[-1]), all_k.shape[-1])
    anywhere = pl.BlockSpec(memory_space=pl.ANY)
    dma = pltpu.SemaphoreType.DMA
    return pl.pallas_call(
        output_kernel,
        out_shape=(jax.ShapeDtypeStruct(lat.shape, F32), jax.ShapeDtypeStruct(tall, BF16), jax.ShapeDtypeStruct(tall, BF16)),
        in_specs=[anywhere] * 3,
        out_specs=[anywhere] * 3,
        scratch_shapes=[pltpu.VMEM((n_buf, *tall[2:]), BF16), pltpu.VMEM(lat.shape, F32), dma((n_buf + 1,)), dma((n_buf + 1,))],
        compiler_params=pltpu.CompilerParams(vmem_limit_bytes=60 * 2**20),
        name="outputs",
    )(lat, all_k.reshape(tall), all_v.reshape(tall))


def denoise(lat, cond, sched, w_ada, w_qkv, w_out, w_up, w_down, w_head, k_old, v_old):
    rows, width = lat.shape
    group = width // RING
    hidden = w_up.shape[2] // 2
    torus = (RING, RING, RING)
    cache = jax.ShapeDtypeStruct((LAYERS, *torus, rows, width), BF16)
    k_old = k_old.reshape(cache.shape)
    v_old = v_old.reshape(cache.shape)
    w_out = w_out.reshape(LAYERS, width, width)
    n_out = width // WIDE
    anywhere = pl.BlockSpec(memory_space=pl.ANY)
    vmem = pl.BlockSpec(memory_space=pltpu.VMEM)
    dma = pltpu.SemaphoreType.DMA
    n_heads = group // HEAD
    n_ada = 3
    lat_out, all_k, all_v, _ = pl.pallas_call(
        denoise_kernel,
        out_shape=(
            jax.ShapeDtypeStruct((rows, width), F32),
            cache,
            cache,
            jax.ShapeDtypeStruct((LAYERS, 2, *torus, rows, group), BF16),
        ),
        in_specs=[anywhere, anywhere, pl.BlockSpec(memory_space=pltpu.SMEM)] + [anywhere] * 8,
        out_specs=[vmem, anywhere, anywhere, anywhere],
        scratch_shapes=[
            pltpu.VMEM((BUFFERS, width // 2, WIDE), BF16),
            pltpu.VMEM((*torus, rows, group), BF16),
            pltpu.VMEM((*torus, rows, group), BF16),
            pltpu.VMEM((rows, width), BF16),
            pltpu.VMEM((STEPS, width), F32),
            pltpu.VMEM((STEPS, rows, width), F32),
            pltpu.VMEM((2 * rows, width), F32),
            pltpu.VMEM((2 * rows, width), BF16),
            pltpu.VMEM((2 * rows, hidden), BF16),
            pltpu.VMEM((2 * rows, width), F32),
            pltpu.VMEM((2 * rows, width), F32),
            pltpu.VMEM((2 * rows, width), F32),
            pltpu.VMEM((2 * rows, width), F32),
            pltpu.VMEM((2, 2, 3, rows, group), BF16),
            pltpu.VMEM((LAYERS, 3, RING, rows, group), BF16),
            pltpu.VMEM((RING * rows, group), F32),
            pltpu.VMEM((n_heads, RING * rows, HEAD), F32),
            pltpu.VMEM((n_heads, RING * rows, HEAD), F32),
            pltpu.VMEM((RING, rows, group), BF16),
            pltpu.VMEM((2, 2, rows, group), BF16),
            pltpu.VMEM((LAYERS, n_ada, RING, RING, 2 * STEPS, width // 8), F32),
            pltpu.VMEM((STEPS, width), F32),
            pltpu.VMEM((2, RING * rows, RING**3 * rows), F32),
            dma((BUFFERS,)),
            dma((2,)),
            dma((2,)),
            dma((2,)),
            dma((n_ada, 2 * RING - 1)),
            dma((n_ada, 2 * RING - 1)),
            dma((3, 2, 2)),
            dma((LAYERS, 3, RING)),
            dma((RING,)),
            dma((2, 2)),
            dma((n_out,)),
            dma((n_out,)),
            dma((n_out,)),
            dma((n_out,)),
            dma((2,)),
            dma((2,)),
            dma((LAYERS, 2, 2, 2, 4)),
            dma((LAYERS, 2, 2, 2, 4)),
            dma((2, 2)),
            dma((2, 2)),
            dma((2, 2)),
            dma((LAYERS, 2, 3, 3, 4)),
            dma((LAYERS, 2, 3, 3, 4)),
        ],
        compiler_params=pltpu.CompilerParams(collective_id=0, has_side_effects=True, vmem_limit_bytes=63 * 2**20),
        name="denoise",
    )(lat, cond, sched.T, w_ada, w_qkv, w_out, w_up, w_down, w_head, k_old, v_old)
    tokens = RING**3 * rows
    lat_out, k_new, v_new = output_copies(lat_out, all_k, all_v)
    return lat_out, k_new.reshape(LAYERS, tokens, width), v_new.reshape(LAYERS, tokens, width)


def solution(mesh):
    slot_spec = P(("img", "cfg"), None, None)
    cache_spec = P(("img", "cfg"), None, None, None)
    rep_spec = P()

    def local_step(latent, cond_vec, sched_coef, w_ada, w_qkv, w_out, w_up, w_down, w_head, k_stale, v_stale):
        lat_out, k_new, v_new = denoise(
            latent[0], cond_vec[0], sched_coef, w_ada, w_qkv, w_out, w_up, w_down, w_head, k_stale[0], v_stale[0]
        )
        return lat_out[None], k_new[None], v_new[None]

    return jax.shard_map(
        local_step,
        mesh=mesh,
        in_specs=(P("img", "patch", None), slot_spec, rep_spec, rep_spec, rep_spec, rep_spec, rep_spec, rep_spec, rep_spec, cache_spec, cache_spec),
        out_specs=(P(("img", "cfg"), "patch", None), cache_spec, cache_spec),
        check_vma=False,
    )
```

```python
import functools

import jax
import jax.numpy as jnp
from jax import lax
from jax.experimental import pallas as pl
from jax.experimental.pallas import tpu as pltpu
from jax.sharding import PartitionSpec as P

RING = 4
AXES = ("z", "y", "x")
COLOR_ORDERS = (("x", "y", "z"), ("y", "z", "x"), ("z", "x", "y"))
HEAD_AXES = ("z", "y")
MESH = pl.DeviceIdType.MESH
F32 = jnp.float32
BF16 = jnp.bfloat16
HEAD = 128
TILE = 512
SUB = 256
WIDE = 2 * TILE
BUFFERS = 12
STEPS = 2
LAYERS = 2
Q, K, V = 0, 1, 2
KV = (K, V)


def dot(lhs, rhs):
    return jnp.dot(lhs, rhs, preferred_element_type=F32)


def scoped(name, action):
    def inside():
        with jax.named_scope(name):
            action()

    return inside


def torus_position():
    patch = lax.axis_index("patch")
    return {"z": lax.div(patch, RING * RING), "y": lax.rem(lax.div(patch, RING), RING), "x": lax.rem(patch, RING)}


def patch_at(pos):
    return (pos["z"] * RING + pos["y"]) * RING + pos["x"]


class Torus:
    def __init__(self):
        self.pos = torus_position()
        self.coord, self.patch = {}, {}
        for axis in AXES:
            for by in range(1, RING):
                coord = lax.rem(self.pos[axis] + by, RING)
                self.coord[axis, by] = coord
                self.patch[axis, by] = patch_at({**self.pos, axis: coord})


def remote(src, dst, send_sem, recv_sem, **device_id):
    return pltpu.make_async_remote_copy(
        src_ref=src, dst_ref=dst, send_sem=send_sem, recv_sem=recv_sem, device_id=device_id, device_id_type=MESH
    )


class Ring:
    def __init__(self, torus, axis, view, send_sem, recv_sem):
        me, succ, prev = torus.pos[axis], torus.coord[axis, 1], torus.coord[axis, RING - 1]
        ahead, behind = torus.patch[axis, 1], torus.patch[axis, RING - 1]
        self.sends = ((me, None, ahead), (me, None, behind), (prev, 0, ahead), (succ, 1, behind))
        self.parts = (view, send_sem, recv_sem)

    def copy(self, slot):
        view, send_sem, recv_sem = self.parts
        coord, half, patch = self.sends[slot]
        part = view(coord, half)
        return remote(part, part, send_sem(slot), recv_sem(slot), patch=patch)

    def first(self):
        for slot in (0, 1):
            self.copy(slot).start()

    def relay(self):
        for slot in (0, 1):
            self.copy(slot).wait_recv()
            self.copy(slot + 2).start()

    def settle(self):
        for slot in (2, 3):
            self.copy(slot).wait_recv()

    def drain(self):
        for slot in range(4):
            self.copy(slot).wait_send()


def full_rings(ref, color, torus, send_sem, recv_sem):
    width = ref.shape[4]
    cut = [0, width // 3 // SUB * SUB, width // 3 // SUB * SUB * 2, width]
    base, size = cut[color], cut[color + 1] - cut[color]
    order = COLOR_ORDERS[color]

    def stage(k):
        axis = order[k]

        def view(coord, half):
            index = []
            for name in AXES:
                index.append(coord if name == axis else slice(None) if name in order[:k] else torus.pos[name])
            columns = pl.ds(base, size) if half is None else pl.ds(base + half * (size // 2), size // 2)
            return ref.at[(*index, slice(None), columns)]

        return Ring(torus, axis, view, lambda slot: send_sem.at[k, slot], lambda slot: recv_sem.at[k, slot])

    return [stage(k) for k in range(3)]


def share_rings(ref, head_axis, color, torus, send_sem, recv_sem):
    size = ref.shape[4] // 2
    rest = [axis for axis in AXES if axis != head_axis]
    order = rest if color else rest[::-1]
    columns = pl.ds(color * size, size)

    def stage(k):
        axis = order[k]

        def view(coord, half):
            index = []
            for name in AXES:
                if name == head_axis:
                    index.append(slice(None) if half is None else pl.ds(half * (RING // 2), RING // 2))
                else:
                    index.append(coord if name == axis else slice(None) if name in order[:k] else torus.pos[name])
            return ref.at[(*index, slice(None), columns)]

        return Ring(torus, axis, view, lambda slot: send_sem.at[k, slot], lambda slot: recv_sem.at[k, slot])

    return [stage(k) for k in range(2)]


def denoise_kernel(
    lat, cond, sched, w_ada, w_qkv, w_out, w_up, w_down, w_head, k_old, v_old,
    lat_out, all_k, all_v, shared,
    wbuf, kbuf, vbuf, lat_own, cond_own, xs, r, h, act, out_own, out_peer, down_own, down_peer, sb, rb, o_sum, o_top, o_total, o_own, ob, mod,
    cond_peer, scores,
    w_sem, in_sem, kv_sem, cond_sem, mod_send, mod_recv, qkv_send, qkv_recv, o_send, o_recv, out_send, out_recv, down_send, down_recv,
    x_sem, share_put, share_send, share_recv, own_put, own_send, own_recv, full_send, full_recv,
):
    rows, width = lat.shape
    half = width // 2
    group = width // RING
    chunk = width // 8
    hidden = w_up.shape[2] // 2
    n_qkv = half // TILE
    n_out = width // WIDE
    n_up = hidden // TILE
    n_deep = hidden // half
    n_down = n_out * n_deep
    n_head = half // TILE
    n_block = 3 * n_qkv + n_out + n_up + n_down
    n_step = LAYERS * n_block + n_head
    n_ada = 3
    n_buf = wbuf.shape[0]
    scale = HEAD**-0.5

    c = lax.axis_index("cfg")
    other = 1 - c
    mod_block = other
    torus = Torus()
    z, y, x = (torus.pos[axis] for axis in AXES)
    line = [torus.pos[axis] for axis in HEAD_AXES]
    line_core = [lax.div(at, 2) for at in line]
    line_odd = [lax.rem(at, 2) for at in line]

    def line_patch(b, at):
        return patch_at({**torus.pos, HEAD_AXES[b]: at})

    def line_rows(ref, b):
        return ref.at[tuple(slice(None) if axis == HEAD_AXES[b] else torus.pos[axis] for axis in AXES)]


    def put(src, dst, slot):
        pltpu.make_async_copy(src, dst, w_sem.at[slot]).start()

    def put_deep(ref, col, slot):
        col = pl.multiple_of(col, TILE)
        for k in range(2):
            put(ref.at[pl.ds(k * half, half), pl.ds(col, TILE)], wbuf.at[slot, :, pl.ds(k * TILE, TILE)], slot)

    def put_wide(ref, row, col, slot):
        row = pl.multiple_of(row, half)
        col = pl.multiple_of(col, WIDE)
        put(ref.at[pl.ds(row, half), pl.ds(col, WIDE)], wbuf.at[slot], slot)

    def issue_ada(i):
        col = pl.multiple_of(i * 2 * width + (y * RING + x) * chunk, chunk)
        for k in range(2):
            put(w_ada.at[mod_block, pl.ds(k * half, half), pl.ds(col, chunk)], wbuf.at[i, :, pl.ds(k * chunk, chunk)], i)

    assert 3 * n_qkv + n_out == n_up == n_down == n_head + 3 * n_qkv == n_buf

    def qkv_tile(layer, j, slot):
        put_deep(w_qkv.at[layer], lax.div(j, n_qkv) * width + c * half + lax.rem(j, n_qkv) * TILE, slot)

    def out_tile(layer, j, slot):
        put_wide(w_out.at[layer], c * half, j * WIDE, slot)

    def up_tile(layer, j, slot):
        put_deep(w_up.at[layer], c * hidden + j * TILE, slot)

    def down_tile(layer, j, slot):
        put_wide(w_down.at[layer], c * hidden + lax.rem(j, n_deep) * half, lax.div(j, n_deep) * WIDE, slot)

    def head_tile(j, slot):
        put_deep(w_head, c * half + j * TILE, slot)

    def run_hooks(t, hooks):
        if not hooks:
            return
        tests = [(t == at) & when for at, when, _ in hooks]

        @pl.when(functools.reduce(jnp.logical_or, tests))
        def _():
            for test, (_, _, action) in zip(tests, hooks):
                pl.when(test)(scoped("hook", action))

    def tile_loop(base, count, body, ahead, hooks=()):
        def one(t, carry):
            slot = lax.rem(base + t, n_buf)
            tile = wbuf.at[slot]
            pltpu.make_async_copy(tile, tile, w_sem.at[slot]).wait()
            body(t, tile)
            ahead(t, slot)
            run_hooks(t, hooks)
            return carry

        lax.fori_loop(0, count, one, 0)

    def deep_dot(tile):
        return dot(h[:, :half], tile[:, :TILE]) + dot(h[:, half:], tile[:, TILE:])

    def load_kv(old_k, old_v):
        pltpu.make_async_copy(old_k, kbuf, kv_sem.at[0]).start()
        pltpu.make_async_copy(old_v, vbuf, kv_sem.at[1]).start()

    def load_stale(b):
        columns = pl.ds(pl.multiple_of(line[b] * group, group), group)
        load_kv(k_old.at[b, :, :, :, :, columns], v_old.at[b, :, :, :, :, columns])

    def load_shared(b):
        load_kv(shared.at[b, 0], shared.at[b, 1])

    share = [
        [share_rings(shared.at[b, i], HEAD_AXES[b], color, torus, share_send.at[b, i, color], share_recv.at[b, i, color]) for i in range(2) for color in range(2)]
        for b in range(LAYERS)
    ]
    full = [
        {
            p: [full_rings(ref.at[b], color, torus, full_send.at[b, p - K, color], full_recv.at[b, p - K, color]) for color in (2, 0, 1)]
            for p, ref in ((K, all_k), (V, all_v))
        }
        for b in range(LAYERS)
    ]

    def first(rings, k):
        for ring in rings:
            if k:
                ring[k - 1].settle()
            ring[k].first()

    def relay(rings, k):
        for ring in rings:
            ring[k].relay()

    def settle(rings, k):
        for ring in rings:
            ring[k].settle()

    barrier = pltpu.get_barrier_semaphore()

    def announce(**device_id):
        pl.semaphore_signal(barrier, inc=1, device_id=device_id, device_id_type=MESH)

    announce(cfg=other)
    for by in range(1, RING):
        for axis in HEAD_AXES:
            for core in range(2):
                announce(patch=torus.patch[axis, by], cfg=core)
        announce(patch=torus.patch["x", by])
    cond_in = pltpu.make_async_copy(cond, cond_own, in_sem.at[0])
    cond_in.start()
    for i in range(n_ada):
        issue_ada(i)
    lat_in = pltpu.make_async_copy(lat, lat_own, in_sem.at[1])
    lat_in.start()
    cond_in.wait()
    with jax.named_scope("barrier"):
        pl.semaphore_wait(barrier, 1 + 5 * (RING - 1))

    cond_swap = remote(cond_own, cond_peer, cond_sem.at[0], cond_sem.at[1], cfg=other)
    cond_swap.start()
    lat_in.wait()
    xs[0] = lat_own[...].astype(F32)
    with jax.named_scope("cond_swap"):
        cond_swap.wait()
    mine, theirs = cond_own[...], cond_peer[...]
    both = jnp.concatenate([jnp.where(c == 0, mine, theirs), jnp.where(c == 0, theirs, mine)], axis=0)
    silu = (both * jax.nn.sigmoid(both)).astype(BF16)

    def mod_ring(i, axis):
        part, base = (mod.at[mod_block, i, y, x], 0) if axis == "y" else (mod.at[mod_block, i, :, x], RING - 1)
        return [
            remote(part, part, mod_send.at[i, base + by - 1], mod_recv.at[i, base + by - 1], patch=torus.patch[axis, by]) for by in range(1, RING)
        ]

    def mod_swap(i):
        return remote(mod.at[mod_block, i], mod.at[mod_block, i], mod_send.at[i, 2 * RING - 2], mod_recv.at[i, 2 * RING - 2], cfg=other)

    def mod_go(i, axis):
        for one in mod_ring(i, axis):
            one.start()

    def mod_wait(i, axis):
        for one in mod_ring(i, axis):
            one.wait_recv()

    for i in range(n_ada):
        with jax.named_scope("ada_wait"):
            filled = wbuf.at[i, :, pl.ds(0, 2 * chunk)]
            pltpu.make_async_copy(filled, filled, w_sem.at[i]).wait()
        if i == 0:
            for n in range(n_ada, n_buf):
                qkv_tile(0, jnp.int32(n - n_ada), n)
            load_stale(0)
        tile = wbuf.at[i]
        mod[mod_block, i, y, x] = dot(silu[:, :half], tile[:, :chunk]) + dot(silu[:, half:], tile[:, chunk : 2 * chunk])
        mod_go(i, "y")
        out_tile(0, jnp.int32(i), i)
    with jax.named_scope("mod_y"):
        for i in range(n_ada):
            mod_wait(i, "y")
            mod_go(i, "x")

    def mod_pass(i):
        mod_wait(i, "x")
        mod_swap(i).start()

    @pl.when(c == 1)
    def _():
        with jax.named_scope("mod_x"):
            mod_pass(0)

    @pl.when(c == 0)
    def _():
        with jax.named_scope("mod_swap"):
            mod_swap(0).wait_recv()

    def mod_rest():
        pl.when(c == 0)(lambda: mod_pass(0))
        for i in range(1, n_ada):
            mod_pass(i)

    def mod_rest_in():
        pl.when(c == 1)(lambda: mod_swap(0).wait_recv())
        for i in range(1, n_ada):
            mod_swap(i).wait_recv()

    def mod_row(b, step, which, i, s):
        at = which % 2 * 8 + i
        both = mod[b, which // 2, at // RING, at % RING, s * STEPS : (s + 1) * STEPS, :]
        return jnp.where(step == 0, both[0:1], both[1:2])

    def normed(s):
        values = r[s * rows : (s + 1) * rows, :]
        centered = values - jnp.mean(values, -1, keepdims=True)
        return centered * lax.rsqrt(jnp.mean(centered * centered, -1, keepdims=True) + 1e-6)

    def modulate(b, step, shift, gain):
        for s in range(2):
            values = normed(s)
            for i in range(8):
                at = slice(i * chunk, (i + 1) * chunk)
                part = values[:, at] * (1.0 + mod_row(b, step, gain, i, s)) + mod_row(b, step, shift, i, s)
                h[s * rows : (s + 1) * rows, at] = part.astype(BF16)

    def add_gated(b, step, gate, own, peer):
        for s in range(2):
            for i in range(8):
                at = (slice(s * rows, (s + 1) * rows), slice(i * chunk, (i + 1) * chunk))
                r[at] = r[at] + mod_row(b, step, gate, i, s) * (own[at] + peer[at])

    def chunk_swap(own, peer, t, send_sem, recv_sem):
        columns = pl.ds(pl.multiple_of(t * WIDE, WIDE), WIDE)
        return remote(own.at[:, columns], peer.at[:, columns], send_sem.at[t], recv_sem.at[t], cfg=other)

    def qkv_copy(b, p, s, g):
        return remote(sb.at[s, g, p], rb.at[b, p, line[b]], qkv_send.at[p, s, g], qkv_recv.at[b, p, line[b]], patch=line_patch(b, 2 * c + g), cfg=s)

    def qkv_out(b, p, do_send):
        for s in range(2):
            for g in range(2):
                if do_send:

                    @pl.when((2 * c + g == line[b]) & (c == s))
                    def _():
                        rb[b, p, line[b]] = sb[s, g, p]

                @pl.when((2 * c + g != line[b]) | (c != s))
                def _():
                    if do_send:
                        qkv_copy(b, p, s, g).start()
                    else:
                        qkv_copy(b, p, s, g).wait_send()

    def qkv_in(b, p):
        for src in range(RING):

            @pl.when((line[b] != src) | (c != line_core[b]))
            def _():
                part = rb.at[b, p, src]
                remote(part, part, qkv_send.at[p, 0, 0], qkv_recv.at[b, p, src], cfg=other).wait_recv()

    def qkv_part(b, p, base, hooks=()):
        def body(t, tile):
            part = deep_dot(tile).astype(BF16)
            for k in range(TILE // SUB):
                col = t * TILE + k * SUB
                g = lax.div(col, group)
                columns = pl.ds(pl.multiple_of(col - g * group, SUB), SUB)
                for s in range(2):
                    sb[s, g, p, :, columns] = part[s * rows : (s + 1) * rows, k * SUB : (k + 1) * SUB]

        tile_loop(base + p * n_qkv, n_qkv, body, lambda t, slot: up_tile(b, p * n_qkv + t, slot), hooks)

    def own_copies(b, p):
        local, swap = [], []
        for g in range(2):
            columns = pl.ds(pl.multiple_of(c * half + g * group, group), group)
            place = (all_k if p == K else all_v).at[b, z, y, x, :, columns]
            local.append(pltpu.make_async_copy(sb.at[c, g, p], place, own_put.at[p - K, g]))
            swap.append(remote(sb.at[other, g, p], place, own_send.at[p - K, g], own_recv.at[p - K, g], cfg=other))
        return local + swap

    def own_start(b, p):
        for one in own_copies(b, p):
            one.start()

    def own_wait(b, p):
        for one in own_copies(b, p):
            one.wait()

    def share_copy(b, p):
        return pltpu.make_async_copy(rb.at[b, p], line_rows(shared.at[b, p - K], b), share_put.at[p - K])

    tokens_z = RING * RING * rows
    n_rows = RING * rows

    n_heads = group // HEAD

    def scored(queries, keys):
        return lax.dot_general(queries, keys, (((1,), (1,)), ((), ())), preferred_element_type=F32)

    def patch_of(shape, axis):
        index = lax.broadcasted_iota(jnp.int32, shape, axis)
        return lax.div(index, jnp.full_like(index, rows))

    def attend_cache(b, hooks):
        own_patch = line_patch(b, patch_of((n_rows, tokens_z), 0))
        key_patch = patch_of((n_rows, tokens_z), 1)

        together = 2

        def one(step, carry):
            heads = [step * together + j for j in range(together)]
            columns = [pl.ds(pl.multiple_of(head * HEAD, HEAD), HEAD) for head in heads]
            queries = [rb[b, Q, :, :, at].reshape(n_rows, HEAD) for at in columns]
            tops, totals, mixed = [None] * together, [None] * together, [None] * together
            for plane in range(RING):
                planes = slice(plane * tokens_z, (plane + 1) * tokens_z)
                hidden_keys = key_patch + plane * RING * RING == own_patch
                for j, at in enumerate(columns):
                    part = scored(queries[j], kbuf[plane, :, :, :, at].reshape(tokens_z, HEAD))
                    part = jnp.where(hidden_keys, -jnp.inf, part)
                    scores[j, :, planes] = part
                    best = jnp.max(part, -1, keepdims=True)
                    tops[j] = best if plane == 0 else jnp.maximum(tops[j], best)
            for plane in range(RING):
                planes = slice(plane * tokens_z, (plane + 1) * tokens_z)
                for j, at in enumerate(columns):
                    weights = jnp.exp((scores[j, :, planes] - tops[j]) * scale)
                    add = jnp.sum(weights, -1, keepdims=True)
                    more = dot(weights.astype(BF16), vbuf[plane, :, :, :, at].reshape(tokens_z, HEAD))
                    totals[j] = add if plane == 0 else totals[j] + add
                    mixed[j] = more if plane == 0 else mixed[j] + more
            for j, (head, at) in enumerate(zip(heads, columns)):
                o_sum[:, at] = mixed[j]
                o_top[head] = jnp.broadcast_to(tops[j], (n_rows, HEAD))
                o_total[head] = jnp.broadcast_to(totals[j], (n_rows, HEAD))
            run_hooks(step, [(when_at // together, when, hook) for when_at, when, hook in hooks])
            return carry

        for i in range(2):
            buf = (kbuf, vbuf)[i]
            pltpu.make_async_copy(buf, buf, kv_sem.at[i]).wait()
        lax.fori_loop(0, n_heads // together, one, 0)

    def attend_fresh(b):
        same = patch_of((n_rows, n_rows), 0) == patch_of((n_rows, n_rows), 1)
        for start in range(0, n_heads, 3):
            heads = range(start, min(start + 3, n_heads))
            columns = [slice(head * HEAD, (head + 1) * HEAD) for head in heads]
            parts = [scored(rb[b, Q, :, :, at].reshape(n_rows, HEAD), rb[b, K, :, :, at].reshape(n_rows, HEAD)) for at in columns]
            parts = [jnp.where(same, part, -jnp.inf) for part in parts]
            tops = [jnp.maximum(o_top[head], jnp.max(part, -1, keepdims=True)) for head, part in zip(heads, parts)]
            weights = [jnp.exp((part - top) * scale) for part, top in zip(parts, tops)]
            fresh = [dot(weight.astype(BF16), rb[b, V, :, :, at].reshape(n_rows, HEAD)) for weight, at in zip(weights, columns)]
            shrink = [jnp.exp((o_top[head] - top) * scale) for head, top in zip(heads, tops)]
            totals = [o_total[head] * less + jnp.sum(weight, -1, keepdims=True) for head, less, weight in zip(heads, shrink, weights)]
            for at, less, more, total in zip(columns, shrink, fresh, totals):
                o_own[:, :, at] = ((o_sum[:, at] * less + more) / total).astype(BF16).reshape(RING, rows, HEAD)

    def o_copy(b, dst):
        return remote(
            o_own.at[dst], ob.at[c, line_odd[b]], o_send.at[dst], o_recv.at[c, line_odd[b]], patch=line_patch(b, dst), cfg=line_core[b]
        )

    def o_out(b, do_send):
        for dst in range(RING):
            if do_send:

                @pl.when((line[b] == dst) & (c == line_core[b]))
                def _():
                    ob[c, line_odd[b]] = o_own[dst]

            @pl.when((line[b] != dst) | (c != line_core[b]))
            def _():
                if do_send:
                    o_copy(b, dst).start()
                else:
                    o_copy(b, dst).wait_send()

    def o_in(b):
        for s in range(2):
            for g in range(2):

                @pl.when((2 * c + g != line[b]) | (c != s))
                def _():
                    part = ob.at[s, g]
                    remote(part, part, o_send.at[0], o_recv.at[s, g], cfg=other).wait_recv()

    def block(step, b):
        base = n_ada + step * n_step + b * n_block
        begin = step == 0
        last = step == STEPS - 1

        def unless_first(action):
            if b:
                action()
            else:
                pl.when(step > 0)(action)

        def gather_own(p):
            own_wait(b, p)
            first(full[b][p], 0)

        def send_late():
            gather_own(V)
            for p in KV:
                qkv_out(b, p, True)

        if b == 0:
            for s in range(2):
                r[s * rows : (s + 1) * rows, :] = xs[step]
        with jax.named_scope("ln1"):
            modulate(b, step, 0, 1)

        @unless_first
        def _():
            for p in (Q, K, V):
                qkv_out(1 - b, p, False)

        with jax.named_scope("qkv_q"):
            qkv_part(b, Q, base)
        qkv_out(b, Q, True)
        with jax.named_scope("qkv_k"):
            qkv_part(b, K, base)
        pl.when(begin)(lambda: qkv_out(b, K, True))

        @pl.when(last)
        def _():
            own_start(b, K)

        with jax.named_scope("qkv_v"):
            qkv_part(b, V, base, ((n_qkv - 1, last, lambda: gather_own(K)),))

        pl.when(begin)(lambda: qkv_out(b, V, True))

        @pl.when(last)
        def _():
            own_start(b, V)
            if b:
                with jax.named_scope("full_1a"):
                    send_late()
                    first(full[0][V], 2)
                    relay(full[1][K], 0)
                    relay(full[1][V], 0)
            else:
                send_late()

        with jax.named_scope("q_in"):
            qkv_in(b, Q)
        if b == 0:
            pl.when(last)(lambda: relay(full[0][K], 0))

        @unless_first
        def _():
            o_out(1 - b, False)

        hooks = () if b else ((n_heads // 2, last, lambda: relay(full[0][V], 0)),)
        with jax.named_scope("attend_cache"):
            attend_cache(b, hooks)
        if b == 0:
            pl.when(begin)(lambda: load_stale(1))

            @pl.when(last)
            def _():
                with jax.named_scope("full_1"):
                    first(full[0][K][:2], 1)

        with jax.named_scope("kv_in"):
            for p in KV:
                qkv_in(b, p)

        @pl.when(begin)
        def _():
            for p in KV:
                share_copy(b, p).start()

        with jax.named_scope("attend_fresh"):
            attend_fresh(b)

        @pl.when(begin)
        def _():
            for p in KV:
                share_copy(b, p).wait()

        o_out(b, True)

        @pl.when(begin)
        def _():
            first(share[b], 0)
            if b:
                relay(share[0], 1)
            else:
                with jax.named_scope("mod_rest"):
                    mod_rest()

        @pl.when(last)
        def _():
            with jax.named_scope("full_2"):
                if b == 0:
                    first(full[0][K][2:], 1)
                    first(full[0][V], 1)
                else:
                    relay(full[0][K], 2)
                    first(full[1][K], 1)
                    first(full[1][V], 1)
                    relay(full[0][V], 2)

        with jax.named_scope("o_in"):
            o_in(b)

        def out_body(t, tile):
            columns = pl.ds(pl.multiple_of(t * WIDE, WIDE), WIDE)
            part = [ob[:, g].reshape(2 * rows, group) for g in range(2)]
            out_own[:, columns] = dot(part[0], tile[:group]) + dot(part[1], tile[group:])
            chunk_swap(out_own, out_peer, t, out_send, out_recv).start()

        @unless_first
        def _():
            for t in range(n_out):
                chunk_swap(out_own, out_peer, t, out_send, out_recv).wait_send()

        with jax.named_scope("out"):
            tile_loop(base + 3 * n_qkv, n_out, out_body, lambda t, slot: up_tile(b, 3 * n_qkv + t, slot))
        if b:
            pl.when(begin)(lambda: relay(share[1], 0))
        else:
            pl.when(begin)(mod_rest_in)

        with jax.named_scope("out_swap"):
            for t in range(n_out):
                chunk_swap(out_own, out_peer, t, out_send, out_recv).wait_recv()
        with jax.named_scope("ln2"):
            add_gated(b, step, 2, out_own, out_peer)
            modulate(b, step, 3, 4)

        def up_body(t, tile):
            act[:, pl.ds(pl.multiple_of(t * TILE, TILE), TILE)] = jax.nn.gelu(deep_dot(tile), approximate=True).astype(BF16)

        def refill():
            settle(share[1 - b], 1)
            load_shared(1 - b)

        if b:
            hooks = ()
        else:
            hooks = (
                (1, begin, lambda: relay(share[0], 0)),
                (n_up * 2 // 3, begin, lambda: first(share[0], 1)),
                (0, last, lambda: relay(full[0][K][:2], 1)),
                (n_up // 6, last, lambda: relay(full[0][K][2:], 1)),
                (n_up // 3, last, lambda: relay(full[0][V][:2], 1)),
                (n_up * 5 // 12, last, lambda: relay(share[1][2:], 1)),
                (n_up * 2 // 3, last, lambda: first(full[0][K][:2], 2)),
                (n_up * 3 // 4, last, lambda: relay(full[0][V][2:], 1)),
            )
        with jax.named_scope("up"):
            tile_loop(base + 3 * n_qkv + n_out, n_up, up_body, lambda t, slot: down_tile(b, t, slot), hooks)

        def down_body(t, tile):
            n = lax.div(t, n_deep)
            deep = lax.rem(t, n_deep)
            columns = pl.ds(pl.multiple_of(n * WIDE, WIDE), WIDE)
            part = dot(act[:, pl.ds(pl.multiple_of(deep * half, half), half)], tile[...])

            down_own[:, columns] = jnp.where(deep == 0, 0.0, down_own[:, columns]) + part

            @pl.when(deep == n_deep - 1)
            def _():
                chunk_swap(down_own, down_peer, n, down_send, down_recv).start()

        @unless_first
        def _():
            for t in range(n_out):
                chunk_swap(down_own, down_peer, t, down_send, down_recv).wait_send()

        if b:
            hooks = (
                (n_down // 6, begin, lambda: first(share[1], 1)),
                (n_down // 3, begin, refill),
                (n_down // 4, last, lambda: relay(full[1][K], 1)),
                (n_down // 2, last, lambda: relay(full[1][V], 1)),
            )
        else:
            hooks = ((n_down // 12, last, lambda: first(full[0][K][2:], 2)), (n_down // 2, last, refill))
        n_first = n_head if b else 3 * n_qkv

        def after_down(t, slot):
            @pl.when(t < n_first)
            def _():
                if b:
                    head_tile(t, slot)
                else:
                    qkv_tile(1, t, slot)

            @pl.when((t >= n_first) & begin if b else t >= n_first)
            def _():
                if b:
                    qkv_tile(0, t - n_first, slot)
                else:
                    out_tile(1, t - n_first, slot)

        with jax.named_scope("down"):
            tile_loop(base + 3 * n_qkv + n_out + n_up, n_down, down_body, after_down, hooks)
        with jax.named_scope("down_swap"):
            for t in range(n_out):
                chunk_swap(down_own, down_peer, t, down_send, down_recv).wait_recv()
        with jax.named_scope("gate2"):
            add_gated(b, step, 5, down_own, down_peer)

    def one_step(step, carry):
        for b in range(LAYERS):
            block(step, b)
        for s in range(2):
            h[s * rows : (s + 1) * rows, :] = normed(s).astype(BF16)
        later = lax.rem(step + 1, STEPS)

        def head_body(t, tile):
            eps = deep_dot(tile).astype(BF16).astype(F32)
            with_cond, without = eps[:rows], eps[rows:]
            guided = without + sched[step, 2] * (with_cond - without)
            columns = pl.ds(pl.multiple_of(c * half + t * TILE, TILE), TILE)
            xs[later, :, columns] = sched[step, 0] * xs[step, :, columns] + sched[step, 1] * guided

        @pl.when(step > 0)
        def _():
            x_half(xs, step, c, half, x_sem, other).wait_send()

        with jax.named_scope("head"):
            tile_loop(
                n_ada + step * n_step + LAYERS * n_block,
                n_head,
                head_body,
                lambda t, slot: pl.when(step == 0)(lambda: out_tile(0, t, slot)),
            )
        swap = x_half(xs, later, c, half, x_sem, other)
        swap.start()
        with jax.named_scope("x_swap"):
            swap.wait_recv()

        @pl.when(step == 0)
        def _():
            with jax.named_scope("relay_share"):
                relay(share[1][:2], 1)

        return carry

    lax.fori_loop(0, STEPS, one_step, 0)
    lat_out[...] = xs[0]

    with jax.named_scope("tail_c1"):
        for p in KV:
            for at in (0, 2, 1):
                first(full[1][p][at : at + 1], 2)
    with jax.named_scope("tail_c2k"):
        relay(full[1][K], 2)
    with jax.named_scope("tail_c2v"):
        relay(full[1][V], 2)
    with jax.named_scope("tail_end"):
        for b in range(LAYERS):
            for p in KV:
                settle(full[b][p], 2)
    x_half(xs, 0, c, half, x_sem, other).wait_send()
    for p in (Q, K, V):
        qkv_out(LAYERS - 1, p, False)
    o_out(LAYERS - 1, False)
    for t in range(n_out):
        chunk_swap(out_own, out_peer, t, out_send, out_recv).wait_send()
        chunk_swap(down_own, down_peer, t, down_send, down_recv).wait_send()
    for i in range(n_ada):
        for one in (*mod_ring(i, "y"), *mod_ring(i, "x"), mod_swap(i)):
            one.wait_send()
    for b in range(LAYERS):
        for ring in share[b] + full[b][K] + full[b][V]:
            for stage in ring:
                stage.drain()


def x_half(xs, at, c, half, x_sem, other):
    part = xs.at[at, :, pl.ds(pl.multiple_of(c * half, half), half)]
    return remote(part, part, x_sem.at[0], x_sem.at[1], cfg=other)


def output_kernel(lat, all_k, all_v, lat_out, k_out, v_out, buf, lat_buf, in_sem, out_sem):
    n_buf = buf.shape[0]
    pieces = [(src.at[b, z], dst.at[b, z]) for src, dst in ((all_k, k_out), (all_v, v_out)) for b in range(LAYERS) for z in range(src.shape[1])]

    def come(i):
        return pltpu.make_async_copy(pieces[i][0], buf.at[i % n_buf], in_sem.at[i % n_buf])

    def go(i):
        return pltpu.make_async_copy(buf.at[i % n_buf], pieces[i][1], out_sem.at[i % n_buf])

    lat_in = pltpu.make_async_copy(lat, lat_buf, in_sem.at[n_buf])
    lat_go = pltpu.make_async_copy(lat_buf, lat_out, out_sem.at[n_buf])
    lat_in.start()
    for i in range(n_buf):
        come(i).start()
    lat_in.wait()
    lat_go.start()
    for i in range(len(pieces)):
        come(i).wait()
        go(i).start()
        late = i - n_buf // 2
        if late >= 0 and late + n_buf < len(pieces):
            go(late).wait()
            come(late + n_buf).start()
    for i in range(max(0, len(pieces) - n_buf), len(pieces)):
        go(i).wait()
    lat_go.wait()


def output_copies(lat, all_k, all_v):
    pieces = 16
    n_buf = 24
    tall = (LAYERS, pieces, all_k.size // (LAYERS * pieces * all_k.shape[-1]), all_k.shape[-1])
    anywhere = pl.BlockSpec(memory_space=pl.ANY)
    dma = pltpu.SemaphoreType.DMA
    return pl.pallas_call(
        output_kernel,
        out_shape=(jax.ShapeDtypeStruct(lat.shape, F32), jax.ShapeDtypeStruct(tall, BF16), jax.ShapeDtypeStruct(tall, BF16)),
        in_specs=[anywhere] * 3,
        out_specs=[anywhere] * 3,
        scratch_shapes=[pltpu.VMEM((n_buf, *tall[2:]), BF16), pltpu.VMEM(lat.shape, F32), dma((n_buf + 1,)), dma((n_buf + 1,))],
        compiler_params=pltpu.CompilerParams(vmem_limit_bytes=60 * 2**20),
        name="outputs",
    )(lat, all_k.reshape(tall), all_v.reshape(tall))


def denoise(lat, cond, sched, w_ada, w_qkv, w_out, w_up, w_down, w_head, k_old, v_old):
    rows, width = lat.shape
    group = width // RING
    hidden = w_up.shape[2] // 2
    torus = (RING, RING, RING)
    cache = jax.ShapeDtypeStruct((LAYERS, *torus, rows, width), BF16)
    k_old = k_old.reshape(cache.shape)
    v_old = v_old.reshape(cache.shape)
    w_out = w_out.reshape(LAYERS, width, width)
    n_out = width // WIDE
    anywhere = pl.BlockSpec(memory_space=pl.ANY)
    vmem = pl.BlockSpec(memory_space=pltpu.VMEM)
    dma = pltpu.SemaphoreType.DMA
    n_heads = group // HEAD
    n_ada = 3
    lat_out, all_k, all_v, _ = pl.pallas_call(
        denoise_kernel,
        out_shape=(
            jax.ShapeDtypeStruct((rows, width), F32),
            cache,
            cache,
            jax.ShapeDtypeStruct((LAYERS, 2, *torus, rows, group), BF16),
        ),
        in_specs=[anywhere, anywhere, pl.BlockSpec(memory_space=pltpu.SMEM)] + [anywhere] * 8,
        out_specs=[vmem, anywhere, anywhere, anywhere],
        scratch_shapes=[
            pltpu.VMEM((BUFFERS, width // 2, WIDE), BF16),
            pltpu.VMEM((*torus, rows, group), BF16),
            pltpu.VMEM((*torus, rows, group), BF16),
            pltpu.VMEM((rows, width), BF16),
            pltpu.VMEM((STEPS, width), F32),
            pltpu.VMEM((STEPS, rows, width), F32),
            pltpu.VMEM((2 * rows, width), F32),
            pltpu.VMEM((2 * rows, width), BF16),
            pltpu.VMEM((2 * rows, hidden), BF16),
            pltpu.VMEM((2 * rows, width), F32),
            pltpu.VMEM((2 * rows, width), F32),
            pltpu.VMEM((2 * rows, width), F32),
            pltpu.VMEM((2 * rows, width), F32),
            pltpu.VMEM((2, 2, 3, rows, group), BF16),
            pltpu.VMEM((LAYERS, 3, RING, rows, group), BF16),
            pltpu.VMEM((RING * rows, group), F32),
            pltpu.VMEM((n_heads, RING * rows, HEAD), F32),
            pltpu.VMEM((n_heads, RING * rows, HEAD), F32),
            pltpu.VMEM((RING, rows, group), BF16),
            pltpu.VMEM((2, 2, rows, group), BF16),
            pltpu.VMEM((LAYERS, n_ada, RING, RING, 2 * STEPS, width // 8), F32),
            pltpu.VMEM((STEPS, width), F32),
            pltpu.VMEM((2, RING * rows, RING**3 * rows), F32),
            dma((BUFFERS,)),
            dma((2,)),
            dma((2,)),
            dma((2,)),
            dma((n_ada, 2 * RING - 1)),
            dma((n_ada, 2 * RING - 1)),
            dma((3, 2, 2)),
            dma((LAYERS, 3, RING)),
            dma((RING,)),
            dma((2, 2)),
            dma((n_out,)),
            dma((n_out,)),
            dma((n_out,)),
            dma((n_out,)),
            dma((2,)),
            dma((2,)),
            dma((LAYERS, 2, 2, 2, 4)),
            dma((LAYERS, 2, 2, 2, 4)),
            dma((2, 2)),
            dma((2, 2)),
            dma((2, 2)),
            dma((LAYERS, 2, 3, 3, 4)),
            dma((LAYERS, 2, 3, 3, 4)),
        ],
        compiler_params=pltpu.CompilerParams(collective_id=0, has_side_effects=True, vmem_limit_bytes=63 * 2**20),
        name="denoise",
    )(lat, cond, sched.T, w_ada, w_qkv, w_out, w_up, w_down, w_head, k_old, v_old)
    tokens = RING**3 * rows
    lat_out, k_new, v_new = output_copies(lat_out, all_k, all_v)
    return lat_out, k_new.reshape(LAYERS, tokens, width), v_new.reshape(LAYERS, tokens, width)


def solution(mesh):
    slot_spec = P(("img", "cfg"), None, None)
    cache_spec = P(("img", "cfg"), None, None, None)
    rep_spec = P()

    def local_step(latent, cond_vec, sched_coef, w_ada, w_qkv, w_out, w_up, w_down, w_head, k_stale, v_stale):
        lat_out, k_new, v_new = denoise(
            latent[0], cond_vec[0], sched_coef, w_ada, w_qkv, w_out, w_up, w_down, w_head, k_stale[0], v_stale[0]
        )
        return lat_out[None], k_new[None], v_new[None]

    return jax.shard_map(
        local_step,
        mesh=mesh,
        in_specs=(P("img", "patch", None), slot_spec, rep_spec, rep_spec, rep_spec, rep_spec, rep_spec, rep_spec, rep_spec, cache_spec, cache_spec),
        out_specs=(P(("img", "cfg"), "patch", None), cache_spec, cache_spec),
        check_vma=False,
    )
```
